32 devices in a mesh: dp: 8 (over z, x), seq: 4 (over y, core).
Axes of the slice: x: 2, y: 2, z: 4, core: 2. Of those that a mesh axis runs over, the one named last changes fastest.
Arguments:
- tokens: bfloat16 [8192, 1280], P(('dp', 'seq')), may hold values from -6 to 6
- cotangent: bfloat16 [8192, 1280], P(('dp', 'seq')), may hold values from -6 to 6
- prefix_len: int32 [8], P('dp'), may hold values from 102 to 512
- gains_master: float32 [2, 1280], replicated, may hold values from 0.5 to 1.5
- gains_moment: float32 [2, 1280], replicated, may hold values from -192 to 192
- gains_square: float32 [2, 1280], replicated, may hold values from 256 to 2048
- qkv_master: float32 [1280, 1920], P('dp', 'seq'), may hold values from -0.15625 to 0.15625
- qkv_moment: float32 [1280, 1920], P('dp', 'seq'), may hold values from -96 to 96
- qkv_square: float32 [1280, 1920], P('dp', 'seq'), may hold values from 64 to 512
- out_master: float32 [1280, 1280], P('dp', 'seq'), may hold values from -2.5 to 2.5
- out_moment: float32 [1280, 1280], P('dp', 'seq'), may hold values from -12 to 12
- out_square: float32 [1280, 1280], P('dp', 'seq'), may hold values from 1 to 12
- gu_master: float32 [1280, 2, 3584], P('dp', None, 'seq'), may hold values from -0.15625 to 0.15625
- gu_moment: float32 [1280, 2, 3584], P('dp', None, 'seq'), may hold values from -64 to 64
- gu_square: float32 [1280, 2, 3584], P('dp', None, 'seq'), may hold values from 25 to 204
- down_master: float32 [3584, 1280], P('seq', 'dp'), may hold values from -0.09375 to 0.09375
- down_moment: float32 [3584, 1280], P('seq', 'dp'), may hold values from -96 to 96
- down_square: float32 [3584, 1280], P('seq', 'dp'), may hold values from 64 to 512
Outputs:
- layer_out: bfloat16 [8192, 1280], P(('dp', 'seq'))
- tokens_grad: float32 [8192, 1280], P(('dp', 'seq'))
- gains_grad: float32 [2, 1280], replicated
- qkv_grad: float32 [1280, 1920], P('dp', 'seq')
- out_grad: float32 [1280, 1280], P('dp', 'seq')
- gu_grad: float32 [1280, 2, 3584], P('dp', None, 'seq')
- down_grad: float32 [3584, 1280], P('seq', 'dp')
- gains_next: float32 [2, 1280], replicated
- gains_moment_next: float32 [2, 1280], replicated
- gains_square_next: float32 [2, 1280], replicated
- qkv_next: float32 [1280, 1920], P('dp', 'seq')
- qkv_moment_next: float32 [1280, 1920], P('dp', 'seq')
- qkv_square_next: float32 [1280, 1920], P('dp', 'seq')
- qkv_copy: bfloat16 [1280, 1920], P('dp', 'seq')
- out_next: float32 [1280, 1280], P('dp', 'seq')
- out_moment_next: float32 [1280, 1280], P('dp', 'seq')
- out_square_next: float32 [1280, 1280], P('dp', 'seq')
- out_copy: bfloat16 [1280, 1280], P('dp', 'seq')
- gu_next: float32 [1280, 2, 3584], P('dp', None, 'seq')
- gu_moment_next: float32 [1280, 2, 3584], P('dp', None, 'seq')
- gu_square_next: float32 [1280, 2, 3584], P('dp', None, 'seq')
- gu_copy: bfloat16 [1280, 2, 3584], P('dp', None, 'seq')
- down_next: float32 [3584, 1280], P('seq', 'dp')
- down_moment_next: float32 [3584, 1280], P('seq', 'dp')
- down_square_next: float32 [3584, 1280], P('seq', 'dp')
- down_copy: bfloat16 [3584, 1280], P('seq', 'dp')
The draws below stay inside these ranges and needn't reach their ends.
All inputs are finite; a program needn't handle non-finite values.
Results may differ from the reference program's by a relative error of at most 0.023.
Values may be sent and summed in bfloat16 or wider, within the bound.
A program may use at most 256 MiB of HBM per device.

```python
import math
import jax
import jax.numpy as jnp
from jax import lax

D = 1280
QUERY_HEADS = 20
KEY_VALUE_HEADS = 5
HEAD_SIZE = 64
FF = 3584
QUERY_WIDTH = 1280
QKV = 1920
LENGTH = 1024
SEQS = 8
TOKENS = 8192
N_DP = 8
N_SEQ = 4


def plant(array, key, low, top_value):
    index_at = [jax.random.randint(jax.random.fold_in(key, axis), (), 0, length) for axis, length in enumerate(array.shape)]
    longest = array.shape.index(max(array.shape))
    neighbour = index_at[:longest] + [(index_at[longest] + 1) % array.shape[longest]] + index_at[longest + 1:]
    return array.at[tuple(index_at)].set(low).at[tuple(neighbour)].set(top_value)


def block_scale(rng, dims, cuts, least, largest):
    gain = 1.0
    for axis_at, parts in cuts:
        steps = jax.random.uniform(jax.random.fold_in(jax.random.fold_in(rng, 6), axis_at), (parts,), jnp.float32, least / len(cuts), largest / len(cuts))
        gain = gain * jnp.repeat(jnp.exp(steps), dims[axis_at] // parts).reshape((-1,) + (1,) * (len(dims) - 1 - axis_at))
    return gain


def normal_values(rng, dims, width, limit, split=(), kind=jnp.bfloat16):
    drawn = width * jax.random.normal(rng, dims, jnp.float32)
    if split:
        drawn = drawn * block_scale(rng, dims, split, -0.22, 0.18)
    return jnp.clip(drawn, -limit, limit).astype(kind)


def setup_inputs(seed: int = 0) -> dict:
    arg_keys = jax.random.split(jax.random.key(seed), 19)
    tokens = normal_values(arg_keys[0], (TOKENS, D), 1.0, 6.0, ((0, 32),))
    cotangent = normal_values(arg_keys[1], (TOKENS, D), 1.0, 6.0, ((0, 32),))
    prefix_len = plant(jax.random.randint(arg_keys[2], (SEQS,), LENGTH // 10, LENGTH // 2 + 1), jax.random.fold_in(arg_keys[2], 1), LENGTH // 10, (LENGTH // 2 + 1) - 1).astype(jnp.int32)
    gains_master = jnp.clip(1.0 + 0.1 * jax.random.normal(arg_keys[3], (2, D), jnp.float32), 0.5, 1.5)
    gains_moment = normal_values(arg_keys[4], (2, D), (N_DP * N_SEQ), 192.0, (), jnp.float32)
    gains_square = jnp.clip(jnp.exp(jax.random.uniform(arg_keys[5], (2, D), jnp.float32, math.log(256.0), math.log(2048.0))), 256.0, 2048.0)
    qkv_master = normal_values(arg_keys[6], (D, QKV), D ** -0.5, 0.15625, ((0, 8), (1, 4)), jnp.float32)
    qkv_moment = normal_values(arg_keys[7], (D, QKV), (N_DP * N_SEQ // 2), 96.0, ((0, 8), (1, 4)), jnp.float32)
    qkv_square = jnp.clip(jnp.exp(math.log(512.0) - 2.0794415 * jax.random.uniform(arg_keys[8], (D, QKV), jnp.float32) ** block_scale(arg_keys[8], (D, QKV), ((0, 8), (1, 4)), -0.2, 0.2)), 64.0, 512.0)
    out_master = normal_values(arg_keys[9], (QUERY_WIDTH, D), (max(QUERY_WIDTH // 256, 1)) ** -0.5, 2.5, ((0, 8), (1, 4)), jnp.float32)
    out_moment = normal_values(arg_keys[10], (QUERY_WIDTH, D), (N_DP * N_SEQ // 12), 12.0, ((0, 8), (1, 4)), jnp.float32)
    out_square = jnp.clip(jnp.exp(math.log(12.0) - 2.4849066 * jax.random.uniform(arg_keys[11], (QUERY_WIDTH, D), jnp.float32) ** block_scale(arg_keys[11], (QUERY_WIDTH, D), ((0, 8), (1, 4)), -0.2, 0.2)), 1.0, 12.0)
    gu_master = normal_values(arg_keys[12], (D, 2, FF), D ** -0.5, 0.15625, ((0, 8), (2, 4)), jnp.float32)
    gu_moment = normal_values(arg_keys[13], (D, 2, FF), (N_DP * N_SEQ // 3), 64.0, ((0, 8), (2, 4)), jnp.float32)
    gu_square = jnp.clip(jnp.exp(math.log(204.0) - 2.099244 * jax.random.uniform(arg_keys[14], (D, 2, FF), jnp.float32) ** block_scale(arg_keys[14], (D, 2, FF), ((0, 8), (2, 4)), -0.2, 0.2)), 25.0, 204.0)
    down_master = normal_values(arg_keys[15], (FF, D), FF ** -0.5, 0.09375, ((0, 4), (1, 8)), jnp.float32)
    down_moment = normal_values(arg_keys[16], (FF, D), (N_DP * N_SEQ // 2), 96.0, ((0, 4), (1, 8)), jnp.float32)
    down_square = jnp.clip(jnp.exp(math.log(512.0) - 2.0794415 * jax.random.uniform(arg_keys[17], (FF, D), jnp.float32) ** block_scale(arg_keys[17], (FF, D), ((0, 4), (1, 8)), -0.2, 0.2)), 64.0, 512.0)
    return {"tokens": tokens, "cotangent": cotangent, "prefix_len": prefix_len, "gains_master": gains_master, "gains_moment": gains_moment, "gains_square": gains_square, "qkv_master": qkv_master, "qkv_moment": qkv_moment, "qkv_square": qkv_square, "out_master": out_master, "out_moment": out_moment, "out_square": out_square, "gu_master": gu_master, "gu_moment": gu_moment, "gu_square": gu_square, "down_master": down_master, "down_moment": down_moment, "down_square": down_square}


eps_norm = 1e-05
eps_adam = 1e-08
rope_base = 10000.0
beta_one = 0.5
beta_two = 0.5
weight_decay = 0.1
score_after_mask = -1e+30
gain_rate = 0.3

@jax.custom_vjp
def lower_bound(v):
    return lax.optimization_barrier(v.astype(jnp.bfloat16)).astype(jnp.float32)

@jax.custom_vjp
def low_back(v):
    return v

def low_keep(v):
    return (lower_bound(v), None)

def low_pass(kept, grad):
    return (grad,)

def back_keep(v):
    return (v, None)

def back_low(kept, grad):
    return (lower_bound(grad),)
lower_bound.defvjp(low_keep, low_pass)
low_back.defvjp(back_keep, back_low)

def matmul(left, right):
    return jnp.dot(left, right, precision=lax.Precision.HIGHEST, preferred_element_type=jnp.float32)

def normalize(values, gain_row):
    inv_rms = lax.rsqrt(lax.optimization_barrier(jnp.mean(values * values, axis=-1, keepdims=True)) + eps_norm)
    return values * inv_rms * gain_row

def rope_tables(positions, head_width):
    half_width = head_width // 2
    frequency = rope_base ** (-2.0 * jnp.arange(half_width, dtype=jnp.float32) / head_width)
    angles = positions.astype(jnp.float32)[:, None] * frequency[None, :]
    return (jnp.cos(angles), jnp.sin(angles))

def apply_rotary(vectors, cosine_rows, sine_rows):
    half_width = vectors.shape[-1] // 2
    lower_half = vectors[..., :half_width]
    upper_half = vectors[..., half_width:]
    cos_cols = cosine_rows[:, None, :]
    sin_cols = sine_rows[:, None, :]
    return jnp.concatenate([lower_half * cos_cols - upper_half * sin_cols, upper_half * cos_cols + lower_half * sin_cols], axis=-1)

def layer_one(values, gains, qkv_weight, out_weight, gu_weight, down_weight, prefix):
    token_length = values.shape[0]
    key_value_width = KEY_VALUE_HEADS * HEAD_SIZE
    attn_input = lower_bound(normalize(values, gains[0]))
    projected_input = low_back(matmul(attn_input, qkv_weight))
    positions = jnp.arange(token_length, dtype=jnp.int32)
    cosine_rows, sine_rows = rope_tables(positions, HEAD_SIZE)
    query_tensor = lower_bound(apply_rotary(projected_input[:, :QUERY_WIDTH].reshape(token_length, QUERY_HEADS, HEAD_SIZE), cosine_rows, sine_rows))
    key_tensor = lower_bound(apply_rotary(projected_input[:, QUERY_WIDTH:QUERY_WIDTH + key_value_width].reshape(token_length, KEY_VALUE_HEADS, HEAD_SIZE), cosine_rows, sine_rows))
    value_tensor = lower_bound(projected_input[:, QUERY_WIDTH + key_value_width:].reshape(token_length, KEY_VALUE_HEADS, HEAD_SIZE))
    grouped_heads = query_tensor.reshape(token_length, KEY_VALUE_HEADS, QUERY_HEADS // KEY_VALUE_HEADS, HEAD_SIZE)
    scores = jnp.einsum('tgrd,kgd->grtk', grouped_heads, key_tensor, precision=lax.Precision.HIGHEST) * HEAD_SIZE ** (-0.5)
    scores = low_back(scores)
    visible = (positions[None, :] <= positions[:, None]) | (positions[None, :] < prefix)
    scores = jnp.where(visible, scores, score_after_mask)
    probs = lower_bound(jax.nn.softmax(scores, axis=-1))
    mixed = jnp.einsum('grtk,kgd->tgrd', probs, value_tensor, precision=lax.Precision.HIGHEST).reshape(token_length, QUERY_WIDTH)
    mixed = lower_bound(low_back(mixed))
    resid = values + low_back(matmul(mixed, out_weight))
    mlp_input = lower_bound(normalize(resid, gains[1]))
    gateup = low_back(matmul(mlp_input, gu_weight.reshape(D, 2 * FF)))
    hidden = lower_bound(jax.nn.silu(gateup[:, :FF]) * gateup[:, FF:])
    return resid + low_back(matmul(hidden, down_weight))

def adam_update(master, moment, square, gradient, step_rate, decay):
    moment_next = beta_one * moment + (1.0 - beta_one) * gradient
    square_next = beta_two * square + (1.0 - beta_two) * gradient * gradient
    master_next = master - step_rate * (moment_next / (jnp.sqrt(square_next) + eps_adam) + decay * master)
    return (master_next, moment_next, square_next)

def reference(tokens, cotangent, prefix_len, gains_master, gains_moment, gains_square, qkv_master, qkv_moment, qkv_square, out_master, out_moment, out_square, gu_master, gu_moment, gu_square, down_master, down_moment, down_square):
    weights = (lower_bound(qkv_master), lower_bound(out_master), lower_bound(gu_master), lower_bound(down_master))
    inputs = tokens.astype(jnp.float32).reshape(SEQS, LENGTH, D)
    upstream = cotangent.astype(jnp.float32).reshape(SEQS, LENGTH, D)

    def forward(values, gains, qkv_weight, out_weight, gu_weight, down_weight):

        def one_sequence(item):
            return layer_one(item[0], gains, qkv_weight, out_weight, gu_weight, down_weight, item[1])
        return lax.map(jax.checkpoint(one_sequence), (values, prefix_len))
    outputs, pullback = jax.vjp(forward, inputs, gains_master, weights[0], weights[1], weights[2], weights[3])
    grads = pullback(upstream)
    rate_wide = 0.5 * D ** (-0.5)
    rate_out = 0.5 * max(QUERY_WIDTH // 256, 1) ** (-0.5)
    rate_down = 0.5 * FF ** (-0.5)
    gains_new = adam_update(gains_master, gains_moment, gains_square, grads[1], gain_rate, 0.0)
    qkv_new = adam_update(qkv_master, qkv_moment, qkv_square, grads[2], rate_wide, weight_decay)
    out_new = adam_update(out_master, out_moment, out_square, grads[3], rate_out, weight_decay)
    gu_new = adam_update(gu_master, gu_moment, gu_square, grads[4], rate_wide, weight_decay)
    down_new = adam_update(down_master, down_moment, down_square, grads[5], rate_down, weight_decay)
    return (outputs.reshape(TOKENS, D).astype(jnp.bfloat16), grads[0].reshape(TOKENS, D), grads[1], grads[2], grads[3], grads[4], grads[5], gains_new[0], gains_new[1], gains_new[2], qkv_new[0], qkv_new[1], qkv_new[2], qkv_new[0].astype(jnp.bfloat16), out_new[0], out_new[1], out_new[2], out_new[0].astype(jnp.bfloat16), gu_new[0], gu_new[1], gu_new[2], gu_new[0].astype(jnp.bfloat16), down_new[0], down_new[1], down_new[2], down_new[0].astype(jnp.bfloat16))
```

```python
import jax
import jax.numpy as jnp
from jax import lax
from jax.experimental import pallas as pl
from jax.experimental.pallas import tpu as pltpu
from jax.sharding import PartitionSpec as P

D = 1280
QUERY_HEADS = 20
KEY_VALUE_HEADS = 5
HEAD_SIZE = 64
FF = 3584
QUERY_WIDTH = 1280


eps_norm = 1e-05
eps_adam = 1e-08
rope_base = 10000.0
beta_one = 0.5
beta_two = 0.5
weight_decay = 0.1
score_after_mask = -1e30
gain_rate = 0.3
lines = 4
half_rows = 2


def normalize(values, gain_row):
    inv_rms = lax.rsqrt(jnp.mean(values * values, axis=-1, keepdims=True) + eps_norm)
    normed = values * inv_rms
    return (normed, inv_rms, normed * gain_row)


def norm_back(grad_out, normed, inv_rms, gain_row):
    scaled = grad_out * gain_row
    inner_mean = jnp.mean(scaled * normed, axis=-1, keepdims=True)
    return (jnp.sum(grad_out * normed, axis=0), inv_rms * (scaled - normed * inner_mean))


def rope_tables(positions, head_width):
    half_width = head_width // 2
    frequency = rope_base ** (-2.0 * jnp.arange(half_width, dtype=jnp.float32) / head_width)
    angles = positions.astype(jnp.float32)[:, None] * frequency[None, :]
    return (jnp.cos(angles), jnp.sin(angles))


def apply_rotary(vectors, cosine_rows, sine_rows):
    half_width = vectors.shape[-1] // 2
    lower_half = vectors[..., :half_width]
    upper_half = vectors[..., half_width:]
    cos_cols = cosine_rows[:, None, :]
    sin_cols = sine_rows[:, None, :]
    return jnp.concatenate(
        [
            lower_half * cos_cols - upper_half * sin_cols,
            upper_half * cos_cols + lower_half * sin_cols,
        ],
        axis=-1,
    )

bf16 = jnp.bfloat16
f32 = jnp.float32


def pick(values, index, axis):
    return lax.dynamic_index_in_dim(values, index, axis, keepdims=False)


def add(left, right, kind=jnp.bfloat16):
    return (left.astype(f32) + right.astype(f32)).astype(kind)


def after(values, *others):
    return lax.optimization_barrier((values,) + others)[0]


class Grid:
    def __init__(self):
        dp = lax.axis_index("dp")
        seq = lax.axis_index("seq")
        self.z, self.x, self.y, self.c = dp // 2, dp % 2, seq // 2, seq % 2

    def swap(self, values, axis, bit):
        count = lax.axis_size(axis)
        return lax.ppermute(values, axis, [(i, i ^ bit) for i in range(count)])

    def swap_x(self, values):
        return self.swap(values, "dp", 1)

    def swap_y(self, values):
        return self.swap(values, "seq", 2)

    def swap_c(self, values):
        return self.swap(values, "seq", 1)

    def send_z(self, values, steps):
        pairs = [(i, (i // 2 + steps) % lines * 2 + i % 2) for i in range(2 * lines)]
        return lax.ppermute(values, "dp", pairs)


def join_kernel(place, a_mine, b_mine, a_theirs, b_theirs, whole):
    z, x, y, c = place[0], place[1], place[2], place[3]
    rows = a_mine.shape[3]
    for line in range(lines):
        step = lax.rem(z - line + lines, lines)
        for side in range(2):
            x_step = lax.rem(x + side, 2)
            for half in range(half_rows):
                columns = []
                for owner in range(4):
                    y_step = lax.rem(y + owner // 2, 2)
                    if half == 0:
                        mine, theirs = a_mine[y_step, x_step, step], a_theirs[y_step, x_step, step]
                    else:
                        mine, theirs = b_mine[x_step, y_step, step], b_theirs[x_step, y_step, step]
                    columns.append(jnp.where(c == owner % 2, mine, theirs))
                at = ((line * 2 + side) * half_rows + half) * rows
                whole[at : at + rows, :] = jnp.concatenate(columns, axis=1)


def join(place, pieces):
    rows, width = pieces[0].shape[3:]
    vmem = pl.BlockSpec(memory_space=pltpu.VMEM)
    return pl.pallas_call(
        join_kernel,
        out_shape=jax.ShapeDtypeStruct((lines * 2 * half_rows * rows, 4 * width), bf16),
        in_specs=[pl.BlockSpec(memory_space=pltpu.SMEM)] + [vmem] * 4,
        out_specs=vmem,
        compiler_params=pltpu.CompilerParams(vmem_limit_bytes=40 * 2**20),
        name="join",
    )(place, *pieces)


def gather_lines(grid, shard):
    return [shard] + [grid.send_z(shard, steps) for steps in range(1, lines)]


def gather_attention(grid, stack):
    rows = stack[0].shape[0] // half_rows
    a_lines = jnp.stack([shard[:rows] for shard in stack])
    b_lines = jnp.stack([shard[rows:] for shard in stack])
    a_side = jnp.stack([a_lines, grid.swap_x(a_lines)])
    b_side = jnp.stack([b_lines, grid.swap_y(b_lines)])
    a_full = jnp.stack([a_side, grid.swap_y(a_side)])
    b_full = jnp.stack([b_side, grid.swap_x(b_side)])
    return a_full, b_full, grid.swap_c(a_full), grid.swap_c(b_full)


def gather_ffn(grid, shard, widths):
    rows = shard.shape[0]
    wholes = [jnp.zeros((2 * lines, rows, width), bf16) for width in widths]
    for steps, mine in enumerate(gather_lines(grid, shard)):
        line = (grid.z - steps + lines) % lines
        for block, side in ((mine, grid.x), (grid.swap_x(mine), 1 - grid.x)):
            at = 0
            for i, width in enumerate(widths):
                wholes[i] = lax.dynamic_update_slice(
                    wholes[i], block[None, :, at : at + width], (line * 2 + side, 0, 0)
                )
                at += width
    return [whole.reshape(2 * lines * rows, -1) for whole in wholes]


def reduce_lines(grid, sums, sums_exact):
    total = pick(sums_exact, grid.z, 0).astype(f32)
    for steps in range(1, lines):
        sent = pick(sums, (grid.z + steps) % lines, 0)
        total = total + grid.send_z(sent, steps).astype(f32)
    return total


def reduce_ffn(grid, gradient):
    rows = gradient.shape[0] // (2 * lines)
    blocks = gradient.reshape(lines, 2, rows, gradient.shape[1])
    theirs = pick(blocks, 1 - grid.x, 1)
    mine = pick(blocks, grid.x, 1)
    total = None
    for steps in (1, 2, 3, 0):
        line = (grid.z + steps) % lines
        both = pick(mine, line, 0).astype(f32) + grid.swap_x(pick(theirs, line, 0)).astype(f32)
        if steps:
            both = grid.send_z(both.astype(bf16), steps).astype(f32)
        total = both if total is None else total + both
    return total


def reduce_attention(grid, gradient):
    width = gradient.shape[2]
    rows = gradient.shape[1] // (2 * lines * half_rows)
    blocks = gradient.reshape(2, 2, lines, 2, half_rows, rows, width)
    chip = add(pick(blocks, grid.c, 1), grid.swap_c(pick(blocks, 1 - grid.c, 1)))
    a_part, b_part = chip[:, :, :, 0], chip[:, :, :, 1]
    a_part = add(pick(a_part, grid.y, 0), grid.swap_y(pick(a_part, 1 - grid.y, 0)))
    b_part = add(pick(b_part, grid.x, 2), grid.swap_x(pick(b_part, 1 - grid.x, 2)))
    a_part = add(pick(a_part, grid.x, 1), grid.swap_x(pick(a_part, 1 - grid.x, 1)))
    b_part = add(pick(b_part, grid.y, 0), grid.swap_y(pick(b_part, 1 - grid.y, 0)))
    sums = jnp.concatenate([a_part, b_part], axis=1)
    return reduce_lines(grid, sums, sums)


def gather_rows(grid, rows):
    pair = jnp.concatenate([rows, grid.swap_y(rows)], axis=0)
    return jnp.concatenate([pair, grid.swap_c(pair)], axis=0)


def reduce_rows(grid, partial):
    count = partial.shape[0] // 4
    chip = partial[: 2 * count].astype(f32) + grid.swap_c(partial[2 * count :]).astype(f32)
    return chip[:count] + grid.swap_y(chip[count:].astype(bf16)).astype(f32)


def reduce_all(grid, values):
    for axis, bit in (("seq", 1), ("seq", 2), ("dp", 1), ("dp", 2), ("dp", 4)):
        values = values + grid.swap(values, axis, bit)
    return values


class Plain:
    def gather_attention(self, shard):
        blocks = lax.all_gather(shard, ("dp", "seq"), axis=0)
        split = blocks.reshape(lax.axis_size("dp"), lax.axis_size("seq"), *shard.shape)
        return jnp.swapaxes(split, 1, 2).reshape(-1, lax.axis_size("seq") * shard.shape[1])

    def gather_ffn(self, shard, widths):
        whole = lax.all_gather(shard, "dp", axis=0, tiled=True)
        return [whole[:, : widths[0]], whole[:, widths[0] :]]

    def reduce_attention(self, gradient):
        owners, wide, width = gradient.shape
        blocks = gradient.reshape(owners, lax.axis_size("dp"), -1, width)
        blocks = jnp.swapaxes(blocks, 0, 1).reshape(-1, width)
        return lax.psum_scatter(blocks, ("dp", "seq"), scatter_dimension=0, tiled=True).astype(f32)


def visible_keys(query_positions, key_positions, prefix):
    return (key_positions[None, :] <= query_positions[:, None]) | (key_positions[None, :] < prefix)


def adam_update(master, moment, square, gradient, step_rate, decay):
    moment_next = beta_one * moment + (1.0 - beta_one) * gradient
    square_next = beta_two * square + (1.0 - beta_two) * gradient * gradient
    master_next = master - step_rate * (
        moment_next / (jnp.sqrt(square_next) + eps_adam) + decay * master
    )
    return (master_next, moment_next, square_next)


def on_device(
    tokens,
    cotangent,
    prefix_len,
    gains_master,
    gains_moment,
    gains_square,
    qkv_master,
    qkv_moment,
    qkv_square,
    out_master,
    out_moment,
    out_square,
    gu_master,
    gu_moment,
    gu_square,
    down_master,
    down_moment,
    down_square,
):
    seq_count = lax.axis_size("seq")
    dp_count = lax.axis_size("dp")
    seq_place = lax.axis_index("seq")
    near = dp_count == 2 * lines and seq_count == 4
    grid = Grid() if near else None
    plain = Plain()
    token_rows = tokens.shape[0]
    group = QUERY_HEADS // KEY_VALUE_HEADS
    kv_width = KEY_VALUE_HEADS * HEAD_SIZE
    quarter = FF // seq_count
    shard_rows = gu_master.shape[0]
    qkv_b = qkv_master.astype(bf16)
    out_b = out_master.astype(bf16)
    ffn_b = jnp.concatenate(
        [gu_master.astype(bf16).reshape(shard_rows, 2 * quarter), down_master.astype(bf16).T],
        axis=1,
    )
    widths = (2 * quarter, quarter)
    if near:
        place = jnp.stack([grid.z, grid.x, grid.y, grid.c]).astype(jnp.int32)
        qkv_lines = gather_lines(grid, qkv_b)
        out_lines = gather_lines(grid, after(out_b, *qkv_lines[1:]))
        qkv_full = join(place, gather_attention(grid, qkv_lines))
        out_full = join(place, gather_attention(grid, out_lines))
        gu_part, down_part = gather_ffn(grid, after(ffn_b, *out_lines[1:]), widths)
        cot_rows = gather_rows(grid, cotangent)
        order = (0, 2, 1, 3)
        key_places = [seq_place ^ step for step in order]
    else:
        qkv_full = plain.gather_attention(qkv_b)
        out_full = plain.gather_attention(out_b)
        gu_part, down_part = plain.gather_ffn(ffn_b, widths)
        cot_rows = lax.all_gather(cotangent, "seq", axis=0, tiled=True)
        key_places = list(range(seq_count))
    within = jnp.arange(token_rows, dtype=jnp.int32)
    positions = seq_place * token_rows + within
    key_positions = jnp.concatenate([spot * token_rows + within for spot in key_places])

    inputs = tokens.astype(f32)
    normed_attn, scale_attn, pre_attn = normalize(inputs, gains_master[0])
    attn_input = pre_attn.astype(bf16)
    projected = jnp.dot(attn_input, qkv_full, preferred_element_type=f32)
    cosine_rows, sine_rows = rope_tables(positions, HEAD_SIZE)
    queries = apply_rotary(
        projected[:, :QUERY_WIDTH].reshape(token_rows, QUERY_HEADS, HEAD_SIZE),
        cosine_rows,
        sine_rows,
    ).astype(bf16)
    keys_local = apply_rotary(
        projected[:, QUERY_WIDTH : QUERY_WIDTH + kv_width].reshape(
            token_rows, KEY_VALUE_HEADS, HEAD_SIZE
        ),
        cosine_rows,
        sine_rows,
    )
    kv_local = jnp.concatenate(
        [keys_local.reshape(token_rows, kv_width), projected[:, QUERY_WIDTH + kv_width :]], axis=1
    ).astype(bf16)
    if near:
        kv_rows = gather_rows(grid, kv_local)
    else:
        kv_rows = lax.all_gather(kv_local, "seq", axis=0, tiled=True)
    keys = kv_rows[:, :kv_width].reshape(-1, KEY_VALUE_HEADS, HEAD_SIZE)
    values = kv_rows[:, kv_width:].reshape(-1, KEY_VALUE_HEADS, HEAD_SIZE)
    grouped = queries.reshape(token_rows, KEY_VALUE_HEADS, group, HEAD_SIZE)
    visible = visible_keys(positions, key_positions, prefix_len[0])

    def scores_of():
        scores = jnp.einsum("tgrd,kgd->grtk", grouped, keys, preferred_element_type=f32)
        return jnp.where(visible, scores * HEAD_SIZE ** (-0.5), score_after_mask)

    scores = scores_of()
    row_max = jnp.max(scores, axis=-1)
    powers = jnp.exp(scores - row_max[..., None])
    row_total = jnp.sum(powers, axis=-1)
    weighted = jnp.einsum("grtk,kgd->tgrd", powers.astype(bf16), values, preferred_element_type=f32)
    mixed_exact = weighted / jnp.transpose(row_total, (2, 0, 1))[..., None]
    log_total = row_max + jnp.log(row_total)
    mixed = mixed_exact.reshape(token_rows, QUERY_WIDTH).astype(bf16)
    resid = inputs + jnp.dot(mixed, out_full, preferred_element_type=f32)
    normed_mlp, scale_mlp, pre_mlp = normalize(resid, gains_master[1])
    mlp_input = pre_mlp.astype(bf16)
    upstream = cotangent.astype(f32)
    if near:
        mlp_rows = gather_rows(grid, mlp_input)
    else:
        mlp_rows = lax.all_gather(mlp_input, "seq", axis=0, tiled=True)
    gateup = jnp.dot(mlp_rows, gu_part, preferred_element_type=f32)
    gate = gateup[:, :quarter]
    up_part = gateup[:, quarter:]
    sigmoid_gate = jax.nn.sigmoid(gate)
    silu_gate = gate * sigmoid_gate
    hidden = (silu_gate * up_part).astype(bf16)
    d_hidden = jnp.dot(cot_rows, down_part, preferred_element_type=f32)
    d_gate_b = (d_hidden * up_part * sigmoid_gate * (1.0 + gate * (1.0 - sigmoid_gate))).astype(bf16)
    d_up_b = (d_hidden * silu_gate).astype(bf16)
    d_gateup = jnp.concatenate([d_gate_b, d_up_b], axis=1)

    def contract(left, right, left_axis, right_axis):
        return lax.dot_general(
            left, right, (((left_axis,), (right_axis,)), ((), ())), preferred_element_type=f32
        )

    d_mlp_part = contract(d_gateup, gu_part, 1, 1).astype(bf16)
    branch_part = contract(hidden, down_part, 1, 1).astype(bf16)
    down_local = contract(cot_rows, hidden, 0, 0).astype(bf16)
    gu_local = contract(mlp_rows, d_gateup, 0, 0).astype(bf16)
    if near:
        d_mlp_input = reduce_rows(grid, d_mlp_part)
        branch_out = reduce_rows(grid, branch_part)
        down_owned = reduce_ffn(grid, down_local)
        gu_owned = reduce_ffn(grid, gu_local)
    else:

        def scatter(values, axis):
            return lax.psum_scatter(values, axis, scatter_dimension=0, tiled=True).astype(f32)

        d_mlp_input = scatter(d_mlp_part, "seq")
        branch_out = scatter(branch_part, "seq")
        down_owned = scatter(down_local, "dp")
        gu_owned = scatter(gu_local, "dp")
    layer_out = (resid + branch_out).astype(bf16)
    down_owned = down_owned.T
    gu_owned = gu_owned.reshape(shard_rows, 2, quarter)

    gain_mlp, d_normed = norm_back(d_mlp_input, normed_mlp, scale_mlp, gains_master[1])
    d_resid = upstream + d_normed
    d_branch = d_resid.astype(bf16)
    d_mixed = contract(d_branch, out_full, 1, 1).astype(bf16)
    out_local = jnp.moveaxis(
        contract(mixed, d_branch, 0, 0).astype(bf16).reshape(QUERY_WIDTH, seq_count, -1), 1, 0
    )
    if near:
        out_owned = reduce_attention(grid, out_local)
    else:
        out_owned = plain.reduce_attention(out_local)
    grouped_back = d_mixed.reshape(token_rows, KEY_VALUE_HEADS, group, HEAD_SIZE)
    row_delta = jnp.transpose(
        jnp.sum(grouped_back.astype(f32) * mixed_exact, axis=-1), (1, 2, 0)
    )
    probs = jnp.exp(scores_of() - log_total[..., None])
    d_probs = jnp.einsum("tgrd,kgd->grtk", grouped_back, values, preferred_element_type=f32)
    d_scores = (probs * (d_probs - row_delta[..., None])).astype(bf16)
    d_query_sum = jnp.einsum(
        "grtk,kgd->tgrd", d_scores, keys, preferred_element_type=f32
    ) * HEAD_SIZE ** (-0.5)
    d_key_rows = jnp.einsum(
        "grtk,tgrd->kgd", d_scores, grouped, preferred_element_type=f32
    ) * HEAD_SIZE ** (-0.5)
    d_value_rows = jnp.einsum(
        "grtk,tgrd->kgd", probs.astype(bf16), grouped_back, preferred_element_type=f32
    )
    d_pairs = jnp.concatenate(
        [d_key_rows.reshape(-1, kv_width), d_value_rows.reshape(-1, kv_width)], axis=1
    ).astype(bf16)
    if near:
        d_kv = reduce_rows(grid, d_pairs)
    else:
        d_kv = scatter(d_pairs, "seq")
    d_queries = apply_rotary(
        d_query_sum.reshape(token_rows, QUERY_HEADS, HEAD_SIZE), cosine_rows, -sine_rows
    ).reshape(token_rows, QUERY_WIDTH)
    d_keys = apply_rotary(
        d_kv[:, :kv_width].reshape(token_rows, KEY_VALUE_HEADS, HEAD_SIZE), cosine_rows, -sine_rows
    ).reshape(token_rows, kv_width)
    d_projected = jnp.concatenate([d_queries, d_keys, d_kv[:, kv_width:]], axis=1).astype(bf16)
    qkv_local = jnp.moveaxis(
        contract(attn_input, d_projected, 0, 0).astype(bf16).reshape(D, seq_count, -1), 1, 0
    )
    if near:
        qkv_owned = reduce_attention(grid, qkv_local)
    else:
        qkv_owned = plain.reduce_attention(qkv_local)
    d_attn_input = contract(d_projected, qkv_full, 1, 1)
    gain_attn, d_normed_attn = norm_back(d_attn_input, normed_attn, scale_attn, gains_master[0])
    tokens_grad = d_resid + d_normed_attn
    gains_local = jnp.stack([gain_attn, gain_mlp])
    if near:
        gains_grad = reduce_all(grid, gains_local)
    else:
        gains_grad = lax.psum(gains_local, ("dp", "seq"))
    owned = (qkv_owned, out_owned, gu_owned, down_owned)
    rate_wide = 0.5 * D ** (-0.5)
    rate_out = 0.5 * max(QUERY_WIDTH // 256, 1) ** (-0.5)
    rate_down = 0.5 * FF ** (-0.5)
    gains_new = adam_update(gains_master, gains_moment, gains_square, gains_grad, gain_rate, 0.0)
    qkv_new = adam_update(qkv_master, qkv_moment, qkv_square, owned[0], rate_wide, weight_decay)
    out_new = adam_update(out_master, out_moment, out_square, owned[1], rate_out, weight_decay)
    gu_new = adam_update(gu_master, gu_moment, gu_square, owned[2], rate_wide, weight_decay)
    down_new = adam_update(down_master, down_moment, down_square, owned[3], rate_down, weight_decay)
    return (
        layer_out,
        tokens_grad,
        gains_grad,
        owned[0],
        owned[1],
        owned[2],
        owned[3],
        gains_new[0],
        gains_new[1],
        gains_new[2],
        qkv_new[0],
        qkv_new[1],
        qkv_new[2],
        qkv_new[0].astype(jnp.bfloat16),
        out_new[0],
        out_new[1],
        out_new[2],
        out_new[0].astype(jnp.bfloat16),
        gu_new[0],
        gu_new[1],
        gu_new[2],
        gu_new[0].astype(jnp.bfloat16),
        down_new[0],
        down_new[1],
        down_new[2],
        down_new[0].astype(jnp.bfloat16),
    )


def solution(mesh):
    in_specs = (
        P(("dp", "seq"), None),
        P(("dp", "seq"), None),
        P("dp"),
        P(),
        P(),
        P(),
        P("dp", "seq"),
        P("dp", "seq"),
        P("dp", "seq"),
        P("dp", "seq"),
        P("dp", "seq"),
        P("dp", "seq"),
        P("dp", None, "seq"),
        P("dp", None, "seq"),
        P("dp", None, "seq"),
        P("seq", "dp"),
        P("seq", "dp"),
        P("seq", "dp"),
    )
    out_specs = (
        P(("dp", "seq"), None),
        P(("dp", "seq"), None),
        P(),
        P("dp", "seq"),
        P("dp", "seq"),
        P("dp", None, "seq"),
        P("seq", "dp"),
        P(),
        P(),
        P(),
        P("dp", "seq"),
        P("dp", "seq"),
        P("dp", "seq"),
        P("dp", "seq"),
        P("dp", "seq"),
        P("dp", "seq"),
        P("dp", "seq"),
        P("dp", "seq"),
        P("dp", None, "seq"),
        P("dp", None, "seq"),
        P("dp", None, "seq"),
        P("dp", None, "seq"),
        P("seq", "dp"),
        P("seq", "dp"),
        P("seq", "dp"),
        P("seq", "dp"),
    )
    return jax.shard_map(
        on_device, mesh=mesh, in_specs=in_specs, out_specs=out_specs, check_vma=False
    )
```

```python
import functools
import math

import jax
import jax.numpy as jnp
from jax import lax
from jax.experimental import pallas as pl
from jax.experimental.pallas import tpu as pltpu
from jax.sharding import PartitionSpec as P

D = 1280
QUERY_HEADS = 20
KEY_VALUE_HEADS = 5
HEAD_SIZE = 64
FF = 3584
QUERY_WIDTH = 1280
PAIR_WIDTH = KEY_VALUE_HEADS * HEAD_SIZE
QKV = QUERY_WIDTH + 2 * PAIR_WIDTH
GROUP = QUERY_HEADS // KEY_VALUE_HEADS


eps_norm = 1e-05
eps_adam = 1e-08
rope_base = 10000.0
beta_one = 0.5
beta_two = 0.5
weight_decay = 0.1
score_after_mask = -1e30
gain_rate = 0.3
lines = 4
half_rows = 2


bf16 = jnp.bfloat16
f32 = jnp.float32


def rope_tables(positions, head_width):
    half_width = head_width // 2
    frequency = rope_base ** (-2.0 * jnp.arange(half_width, dtype=jnp.float32) / head_width)
    angles = positions.astype(jnp.float32)[:, None] * frequency[None, :]
    return (jnp.cos(angles), jnp.sin(angles))


def pick(values, index, axis):
    return lax.dynamic_index_in_dim(values, index, axis, keepdims=False)


def add(left, right, kind=jnp.bfloat16):
    return (left.astype(f32) + right.astype(f32)).astype(kind)


def after(values, *others):
    return lax.optimization_barrier((values,) + others)[0]


class Grid:
    def __init__(self):
        dp = lax.axis_index("dp")
        seq = lax.axis_index("seq")
        self.z, self.x, self.y, self.c = dp // 2, dp % 2, seq // 2, seq % 2

    def swap(self, values, axis, bit):
        count = lax.axis_size(axis)
        return lax.ppermute(values, axis, [(i, i ^ bit) for i in range(count)])

    def swap_x(self, values):
        return self.swap(values, "dp", 1)

    def swap_y(self, values):
        return self.swap(values, "seq", 2)

    def swap_c(self, values):
        return self.swap(values, "seq", 1)

    def send_z(self, values, steps):
        pairs = [(i, (i // 2 + steps) % lines * 2 + i % 2) for i in range(2 * lines)]
        return lax.ppermute(values, "dp", pairs)


MESH = pl.DeviceIdType.MESH


def place_of():
    dp = lax.axis_index("dp")
    seq = lax.axis_index("seq")
    return dp // 2, lax.rem(dp, 2), seq // 2, lax.rem(seq, 2)


def greet(peers):
    barrier = pltpu.get_barrier_semaphore()
    for peer in peers:
        pl.semaphore_signal(barrier, inc=1, device_id=peer, device_id_type=MESH)
    pl.semaphore_wait(barrier, len(peers))


def spread_kernel(count, *refs):
    shards, wholes = refs[:count], refs[count : 2 * count]
    own_sem, sent, got = refs[2 * count :]
    z, x, y, c = place_of()
    mine, other = 2 * y + c, 2 * (1 - y) + c
    rows = shards[0].shape[0]
    half = rows // 2
    x_peer = (2 * z + 1 - x, mine)
    y_peer = (2 * z + x, other)
    c_peer = (2 * z + x, 2 * y + 1 - c)
    z_peers = [(2 * lax.rem(z + k, lines) + x, mine) for k in range(1, lines)]
    greet([x_peer, y_peer, c_peer] + z_peers)
    started = []
    arriving = {}

    def send(array, source, owner, block, peer, slot, part=None):
        view = wholes[array].at[owner, block]
        origin = view if source is None else source
        if part is not None:
            view = view.at[pl.ds(part * half, half)]
            origin = origin.at[pl.ds(part * half, half)]
        copy = pltpu.make_async_remote_copy(
            src_ref=origin,
            dst_ref=view,
            send_sem=sent.at[array, slot],
            recv_sem=got.at[array, slot],
            device_id=peer,
            device_id_type=MESH,
        )
        copy.start()
        started.append(copy)
        arriving[array, slot] = copy

    def arrive(array, slot):
        arriving[array, slot].wait_recv()

    local = []
    for array in range(count):
        copy = pltpu.make_async_copy(
            shards[array], wholes[array].at[mine, 2 * z + x], own_sem.at[array]
        )
        copy.start()
        local.append(copy)
        for k in (1, 3, 2):
            send(array, shards[array], mine, 2 * z + x, z_peers[k - 1], k)

    def first(array, k):
        line = lax.rem(z - k + lines, lines)
        if k:
            arrive(array, k)
        source = None if k else shards[array]
        send(array, source, mine, 2 * line + x, x_peer, 4 + k)
        send(array, source, mine, 2 * line + x, y_peer, 8 + k)
        send(array, source, mine, 2 * line + x, c_peer, 20 + k)

    def second(array, k):
        line = lax.rem(z - k + lines, lines)
        arrive(array, 4 + k)
        send(array, None, mine, 2 * line + 1 - x, y_peer, 12 + k, 0)
        arrive(array, 8 + k)
        send(array, None, other, 2 * line + x, x_peer, 16 + k, 1)
        send(array, None, mine, 2 * line + 1 - x, c_peer, 24 + k)
        send(array, None, other, 2 * line + x, c_peer, 28 + k)

    def third(array, k):
        line = lax.rem(z - k + lines, lines)
        arrive(array, 12 + k)
        arrive(array, 16 + k)
        send(array, None, other, 2 * line + 1 - x, c_peer, 32 + k)

    items = [(array, k) for array in range(count) for k in (0, 1, 3, 2)]
    for at in range(len(items) + 2):
        if at < len(items):
            first(*items[at])
        if 0 <= at - 1 < len(items):
            second(*items[at - 1])
        if 0 <= at - 2:
            third(*items[at - 2])
    for array in range(count):
        for slot in range(20, 36):
            arrive(array, slot)
    for copy in started:
        copy.wait_send()
    for copy in local:
        copy.wait()


def spread(shards):
    count = len(shards)
    anywhere = pl.BlockSpec(memory_space=pl.ANY)
    wholes = pl.pallas_call(
        functools.partial(spread_kernel, count),
        out_shape=[jax.ShapeDtypeStruct((4, 2 * lines) + s.shape, s.dtype) for s in shards],
        in_specs=[anywhere] * count,
        out_specs=[anywhere] * count,
        scratch_shapes=[
            pltpu.SemaphoreType.DMA((count,)),
            pltpu.SemaphoreType.DMA((count, 36)),
            pltpu.SemaphoreType.DMA((count, 36)),
        ],
        compiler_params=pltpu.CompilerParams(collective_id=0, has_side_effects=True),
        name="spread",
    )(*shards)
    return [whole.reshape(4, -1, whole.shape[3]) for whole in wholes]


def gather_lines(grid, shard):
    return [shard] + [grid.send_z(shard, steps) for steps in (1, 3, 2)]


def gather_ffn(grid, shard, widths):
    rows = shard.shape[0]
    wholes = [jnp.zeros((2 * lines, rows, width), bf16) for width in widths]
    for steps, mine in zip((0, 1, 3, 2), gather_lines(grid, shard)):
        line = (grid.z - steps + lines) % lines
        for block, side in ((mine, grid.x), (grid.swap_x(mine), 1 - grid.x)):
            at = 0
            for i, width in enumerate(widths):
                wholes[i] = lax.dynamic_update_slice(
                    wholes[i], block[None, :, at : at + width], (line * 2 + side, 0, 0)
                )
                at += width
    return [whole.reshape(2 * lines * rows, -1) for whole in wholes]


def reduce_lines(grid, sums, sums_exact):
    total = pick(sums_exact, grid.z, 0).astype(f32)
    for steps in range(1, lines):
        sent = pick(sums, (grid.z + steps) % lines, 0)
        total = total + grid.send_z(sent, steps).astype(f32)
    return total


def reduce_ffn(grid, gradient):
    rows = gradient.shape[0] // (2 * lines)
    blocks = gradient.reshape(lines, 2, rows, gradient.shape[1])
    theirs = pick(blocks, 1 - grid.x, 1)
    mine = pick(blocks, grid.x, 1)
    total = None
    for steps in (1, 2, 3, 0):
        line = (grid.z + steps) % lines
        both = pick(mine, line, 0).astype(f32) + grid.swap_x(pick(theirs, line, 0)).astype(f32)
        if steps:
            both = grid.send_z(both.astype(bf16), steps).astype(f32)
        total = both if total is None else total + both
    return total


def reduce_attention(grid, gradient):
    width = gradient.shape[2]
    rows = gradient.shape[1] // (2 * lines * half_rows)
    blocks = gradient.reshape(2, 2, lines, 2, half_rows, rows, width)
    chip = add(pick(blocks, grid.c, 1), grid.swap_c(pick(blocks, 1 - grid.c, 1)))
    a_part, b_part = chip[:, :, :, 0], chip[:, :, :, 1]
    a_part = add(pick(a_part, grid.y, 0), grid.swap_y(pick(a_part, 1 - grid.y, 0)))
    b_part = add(pick(b_part, grid.x, 2), grid.swap_x(pick(b_part, 1 - grid.x, 2)))
    a_part = add(pick(a_part, grid.x, 1), grid.swap_x(pick(a_part, 1 - grid.x, 1)))
    b_part = add(pick(b_part, grid.y, 0), grid.swap_y(pick(b_part, 1 - grid.y, 0)))
    sums = jnp.concatenate([a_part, b_part], axis=1)
    return reduce_lines(grid, sums, sums)


def gather_rows(grid, rows):
    pair = jnp.concatenate([rows, grid.swap_y(rows)], axis=0)
    return jnp.concatenate([pair, grid.swap_c(pair)], axis=0)


def reduce_rows(grid, partial):
    count = partial.shape[0] // 4
    chip = partial[: 2 * count].astype(f32) + grid.swap_c(partial[2 * count :]).astype(f32)
    return chip[:count] + grid.swap_y(chip[count:].astype(bf16)).astype(f32)


def reduce_all(grid, values):
    for axis, bit in (("seq", 1), ("seq", 2), ("dp", 1), ("dp", 2), ("dp", 4)):
        values = values + grid.swap(values, axis, bit)
    return values


class Plain:
    def gather_attention(self, shard):
        blocks = lax.all_gather(shard, ("dp", "seq"), axis=0)
        split = blocks.reshape(lax.axis_size("dp"), lax.axis_size("seq"), *shard.shape)
        return jnp.swapaxes(split, 0, 1).reshape(lax.axis_size("seq"), -1, shard.shape[1])

    def gather_ffn(self, shard, widths):
        whole = lax.all_gather(shard, "dp", axis=0, tiled=True)
        return [whole[:, : widths[0]], whole[:, widths[0] :]]

    def reduce_attention(self, gradient):
        owners, wide, width = gradient.shape
        blocks = gradient.reshape(owners, lax.axis_size("dp"), -1, width)
        blocks = jnp.swapaxes(blocks, 0, 1).reshape(-1, width)
        return lax.psum_scatter(blocks, ("dp", "seq"), scatter_dimension=0, tiled=True).astype(f32)


def spec(space=pltpu.VMEM):
    return pl.BlockSpec(memory_space=space)


def local_call(kernel, name, outs, *args, flops=0, smem=0):
    moved = sum(a.size * a.dtype.itemsize for a in args) + sum(
        math.prod(s) * jnp.dtype(k).itemsize for s, k in outs
    )
    return pl.pallas_call(
        kernel,
        out_shape=[jax.ShapeDtypeStruct(s, k) for s, k in outs],
        in_specs=[spec()] * (len(args) - smem) + [spec(pltpu.SMEM)] * smem,
        out_specs=[spec()] * len(outs),
        compiler_params=pltpu.CompilerParams(vmem_limit_bytes=60 * 2**20),
        cost_estimate=pl.CostEstimate(flops=flops, bytes_accessed=moved, transcendentals=0),
        name=name,
    )(*args)


def dot(left, right, left_axis=1, right_axis=0, **how):
    return lax.dot_general(
        left, right, (((left_axis,), (right_axis,)), ((), ())), preferred_element_type=f32, **how
    )


def rotate(chunk, cosine, sine):
    lane = lax.broadcasted_iota(jnp.int32, chunk.shape, 1)
    swapped = jnp.where(lane % 64 < 32, pltpu.roll(chunk, 96, 1), pltpu.roll(chunk, 32, 1))
    return chunk * cosine + swapped * sine


def project_kernel(tokens, gain, weight, cosine, sine, attn_input, queries, pairs):
    x = tokens[...].astype(f32)
    scale = lax.rsqrt(jnp.mean(x * x, axis=-1, keepdims=True) + eps_norm)
    normed = (x * scale * gain[...]).astype(bf16)
    attn_input[...] = normed
    projected = jnp.concatenate([dot(normed, weight[j]) for j in range(4)], axis=1)
    first = lax.broadcasted_iota(jnp.int32, (x.shape[0], 128), 1) < 64
    for chunk in range(QKV // 128):
        u = projected[:, chunk * 128 : chunk * 128 + 128]
        at = chunk * 128 - QUERY_WIDTH
        if at < 0:
            turned = rotate(u, cosine[...], sine[...]) * HEAD_SIZE ** (-0.5)
            queries[:, chunk * 128 : chunk * 128 + 128] = turned.astype(bf16)
        elif at + 128 <= PAIR_WIDTH:
            pairs[:, at : at + 128] = rotate(u, cosine[...], sine[...]).astype(bf16)
        elif at < PAIR_WIDTH:
            turned = jnp.where(first, rotate(u, cosine[...], sine[...]), u)
            pairs[:, at : at + 128] = turned.astype(bf16)
        else:
            pairs[:, at : at + 128] = u.astype(bf16)


def head(values, index):
    return values[:, index * HEAD_SIZE : (index + 1) * HEAD_SIZE]


def attend_kernel(
    queries, pairs, tokens, weight, gain, query_at, key_at, prefix, mixed, exact, logs, resid, mlp_input
):
    seen = (key_at[...] <= query_at[...]) | (key_at[...] < prefix[0])
    for group in range(KEY_VALUE_HEADS):
        keys = head(pairs, group)
        values = head(pairs, KEY_VALUE_HEADS + group)
        for member in range(GROUP):
            at = group * GROUP + member
            scores = jnp.where(seen, dot(head(queries, at), keys, 1, 1), score_after_mask)
            top = jnp.max(scores, axis=-1, keepdims=True)
            powers = jnp.exp(scores - top)
            total = jnp.sum(powers, axis=-1, keepdims=True)
            exact[:, at * 64 : at * 64 + 64] = dot(powers.astype(bf16), values) / total
            logs[:, at : at + 1] = top + jnp.log(total)
    mixed[...] = exact[...].astype(bf16)
    branch = jnp.concatenate([dot(mixed[...], weight[j]) for j in range(4)], axis=1)
    total = tokens[...].astype(f32) + branch
    resid[...] = total
    scale = lax.rsqrt(jnp.mean(total * total, axis=-1, keepdims=True) + eps_norm)
    mlp_input[...] = (total * scale * gain[...]).astype(bf16)


def back_norm(grad_out, source, gain):
    scale = lax.rsqrt(jnp.mean(source * source, axis=-1, keepdims=True) + eps_norm)
    normed = source * scale
    scaled = grad_out * gain
    inner = jnp.mean(scaled * normed, axis=-1, keepdims=True)
    return jnp.sum(grad_out * normed, axis=0, keepdims=True), scale * (scaled - normed * inner)


def branch_back_kernel(
    d_mlp, resid, cotangent, gain, weight, mixed, exact, d_resid, d_mixed, out_grad, gain_grad, deltas
):
    gain_sum, d_normed = back_norm(d_mlp[...], resid[...], gain[...])
    gain_grad[...] = gain_sum
    total = cotangent[...].astype(f32) + d_normed
    d_resid[...] = total
    width = weight.shape[2]
    d_branch = total.astype(bf16)
    back = None
    for j in range(4):
        part = d_branch[:, j * width : (j + 1) * width]
        out_grad[j] = dot(mixed[...], part, 0, 0).astype(bf16)
        term = dot(part, weight[j], 1, 1)
        back = term if back is None else back + term
    d_mixed[...] = back.astype(bf16)
    product = d_mixed[...].astype(f32) * exact[...]
    which = lax.broadcasted_iota(jnp.int32, (32, QUERY_WIDTH), 1) // HEAD_SIZE
    ones = (which == lax.broadcasted_iota(jnp.int32, (32, QUERY_WIDTH), 0)).astype(f32)
    deltas[...] = dot(ones, product, 1, 1, precision=lax.Precision.HIGHEST)


def attend_back_kernel(
    queries, pairs, d_mixed, logs, deltas, query_at, key_at, prefix, d_queries, d_pairs
):
    seen = (key_at[...] <= query_at[...]) | (key_at[...] < prefix[0])
    for group in range(KEY_VALUE_HEADS):
        keys = head(pairs, group)
        values = head(pairs, KEY_VALUE_HEADS + group)
        turned_keys = keys.T
        d_keys = d_values = None
        for member in range(GROUP):
            at = group * GROUP + member
            mine = head(queries, at)
            back = head(d_mixed, at)
            scores = jnp.where(seen, dot(keys, mine, 1, 1), score_after_mask)
            probs = jnp.exp(scores - logs[at : at + 1, :])
            d_probs = dot(values, back, 1, 1)
            d_scores = (probs * (d_probs - deltas[at : at + 1, :])).astype(bf16)
            turned = dot(turned_keys, d_scores) * HEAD_SIZE ** (-0.5)
            d_queries[:, at * 64 : at * 64 + 64] = turned.T
            key_term = dot(d_scores, mine)
            value_term = dot(probs.astype(bf16), back)
            d_keys = key_term if d_keys is None else d_keys + key_term
            d_values = value_term if d_values is None else d_values + value_term
        at = group * 64
        d_pairs[:, at : at + 64] = d_keys.astype(bf16)
        at += PAIR_WIDTH
        d_pairs[:, at : at + 64] = d_values.astype(bf16)


def project_back_kernel(
    d_queries, d_pairs, attn_input, tokens, d_resid, gain, weight, cosine, sine, tokens_grad, qkv_grad, gain_grad
):
    rows = tokens.shape[0]
    first = lax.broadcasted_iota(jnp.int32, (rows, 128), 1) < 64
    chunks = []
    for chunk in range(QKV // 128):
        at = chunk * 128 - QUERY_WIDTH
        if at < 0:
            chunks.append(rotate(d_queries[:, chunk * 128 : chunk * 128 + 128], cosine[...], -sine[...]))
            continue
        u = d_pairs[:, at : at + 128]
        if at + 128 <= PAIR_WIDTH:
            u = rotate(u, cosine[...], -sine[...])
        elif at < PAIR_WIDTH:
            u = jnp.where(first, rotate(u, cosine[...], -sine[...]), u)
        chunks.append(u)
    d_projected = jnp.concatenate([u.astype(bf16) for u in chunks], axis=1)
    width = weight.shape[2]
    back = None
    for j in range(4):
        part = d_projected[:, j * width : (j + 1) * width]
        qkv_grad[j] = dot(attn_input[...], part, 0, 0).astype(bf16)
        term = dot(part, weight[j], 1, 1)
        back = term if back is None else back + term
    gain_sum, d_normed = back_norm(back, tokens[...].astype(f32), gain[...])
    gain_grad[...] = gain_sum
    tokens_grad[...] = d_resid[...] + d_normed


def adam_update(master, moment, square, gradient, step_rate, decay):
    moment_next = beta_one * moment + (1.0 - beta_one) * gradient
    square_next = beta_two * square + (1.0 - beta_two) * gradient * gradient
    master_next = master - step_rate * (
        moment_next / (jnp.sqrt(square_next) + eps_adam) + decay * master
    )
    return (master_next, moment_next, square_next)


def on_device(
    tokens,
    cotangent,
    prefix_len,
    gains_master,
    gains_moment,
    gains_square,
    qkv_master,
    qkv_moment,
    qkv_square,
    out_master,
    out_moment,
    out_square,
    gu_master,
    gu_moment,
    gu_square,
    down_master,
    down_moment,
    down_square,
):
    seq_count = lax.axis_size("seq")
    dp_count = lax.axis_size("dp")
    seq_place = lax.axis_index("seq")
    near = dp_count == 2 * lines and seq_count == 4
    grid = Grid() if near else None
    plain = Plain()
    token_rows = tokens.shape[0]
    quarter = FF // seq_count
    shard_rows = gu_master.shape[0]
    qkv_b = qkv_master.astype(bf16)
    out_b = out_master.astype(bf16)
    ffn_b = jnp.concatenate(
        [gu_master.astype(bf16).reshape(shard_rows, 2 * quarter), down_master.astype(bf16).T],
        axis=1,
    )
    widths = (2 * quarter, quarter)
    if near:
        qkv_full, out_full = spread([qkv_b, out_b])
        gu_part, down_part = gather_ffn(grid, after(ffn_b, qkv_full), widths)
        cot_rows = gather_rows(grid, after(cotangent, qkv_full))
        order = (0, 2, 1, 3)
        key_places = [seq_place ^ step for step in order]
    else:
        qkv_full = plain.gather_attention(qkv_b)
        out_full = plain.gather_attention(out_b)
        gu_part, down_part = plain.gather_ffn(ffn_b, widths)
        cot_rows = lax.all_gather(cotangent, "seq", axis=0, tiled=True)
        key_places = list(range(seq_count))
    within = jnp.arange(token_rows, dtype=jnp.int32)
    positions = seq_place * token_rows + within
    key_positions = jnp.concatenate([spot * token_rows + within for spot in key_places])

    cosine_half, sine_half = rope_tables(positions, HEAD_SIZE)
    cosine = jnp.concatenate([cosine_half] * 4, axis=1)
    sine = jnp.concatenate([-sine_half, sine_half] * 2, axis=1)
    shape = (token_rows, D)
    attn_gain, mlp_gain = gains_master[0:1], gains_master[1:2]
    attn_input, queries, kv_local = local_call(
        project_kernel,
        "project",
        [(shape, bf16), (shape, bf16), ((token_rows, 2 * PAIR_WIDTH), bf16)],
        *(tokens, attn_gain, qkv_full, cosine, sine),
        flops=2 * token_rows * D * QKV,
    )
    if near:
        kv_rows = gather_rows(grid, kv_local)
    else:
        kv_rows = lax.all_gather(kv_local, "seq", axis=0, tiled=True)
    score_flops = 2 * token_rows * kv_rows.shape[0] * QUERY_WIDTH
    out_flops = 2 * token_rows * D * D
    mixed, mixed_exact, logs, resid, mlp_input = local_call(
        attend_kernel,
        "attend",
        [(shape, bf16), (shape, f32), ((token_rows, 128), f32), (shape, f32), (shape, bf16)],
        *(queries, kv_rows, tokens, out_full, mlp_gain),
        *(positions[:, None], key_positions[None, :], prefix_len),
        flops=2 * score_flops + out_flops,
        smem=1,
    )
    if near:
        mlp_rows = gather_rows(grid, mlp_input)
    else:
        mlp_rows = lax.all_gather(mlp_input, "seq", axis=0, tiled=True)
    gateup = jnp.dot(mlp_rows, gu_part, preferred_element_type=f32)
    gate = gateup[:, :quarter]
    up_part = gateup[:, quarter:]
    sigmoid_gate = jax.nn.sigmoid(gate)
    silu_gate = gate * sigmoid_gate
    hidden = (silu_gate * up_part).astype(bf16)
    d_hidden = jnp.dot(cot_rows, down_part, preferred_element_type=f32)
    d_gate_b = (d_hidden * up_part * sigmoid_gate * (1.0 + gate * (1.0 - sigmoid_gate))).astype(bf16)
    d_up_b = (d_hidden * silu_gate).astype(bf16)
    d_gateup = jnp.concatenate([d_gate_b, d_up_b], axis=1)

    def contract(left, right, left_axis, right_axis):
        return lax.dot_general(
            left, right, (((left_axis,), (right_axis,)), ((), ())), preferred_element_type=f32
        )

    d_mlp_part = contract(d_gateup, gu_part, 1, 1).astype(bf16)
    branch_part = contract(hidden, down_part, 1, 1).astype(bf16)
    down_local = contract(cot_rows, hidden, 0, 0).astype(bf16)
    gu_local = contract(mlp_rows, d_gateup, 0, 0).astype(bf16)
    if near:
        d_mlp_input = reduce_rows(grid, d_mlp_part)
        branch_out = reduce_rows(grid, branch_part)
        down_owned = reduce_ffn(grid, down_local)
        gu_owned = reduce_ffn(grid, gu_local)
    else:

        def scatter(values, axis):
            return lax.psum_scatter(values, axis, scatter_dimension=0, tiled=True).astype(f32)

        d_mlp_input = scatter(d_mlp_part, "seq")
        branch_out = scatter(branch_part, "seq")
        down_owned = scatter(down_local, "dp")
        gu_owned = scatter(gu_local, "dp")
    layer_out = (resid + branch_out).astype(bf16)
    down_owned = down_owned.T
    gu_owned = gu_owned.reshape(shard_rows, 2, quarter)

    pair_shape = (seq_count, D, out_full.shape[2])
    d_resid, d_mixed, out_local, gain_mlp, deltas = local_call(
        branch_back_kernel,
        "branch_back",
        [(shape, f32), (shape, bf16), (pair_shape, bf16), ((1, D), f32), ((32, token_rows), f32)],
        *(d_mlp_input, resid, cotangent, mlp_gain, out_full, mixed, mixed_exact),
        flops=2 * out_flops,
    )
    if near:
        out_owned = reduce_attention(grid, out_local)
    else:
        out_owned = plain.reduce_attention(out_local)
    d_queries, d_pairs = local_call(
        attend_back_kernel,
        "attend_back",
        [(shape, f32), (kv_rows.shape, bf16)],
        *(queries, kv_rows, d_mixed, logs.T, deltas),
        *(positions[None, :], key_positions[:, None], prefix_len),
        flops=5 * score_flops,
        smem=1,
    )
    if near:
        d_kv = reduce_rows(grid, d_pairs)
    else:
        d_kv = scatter(d_pairs, "seq")
    tokens_grad, qkv_local, gain_attn = local_call(
        project_back_kernel,
        "project_back",
        [(shape, f32), (qkv_full.shape, bf16), ((1, D), f32)],
        *(d_queries, d_kv, attn_input, tokens, d_resid, attn_gain, qkv_full, cosine, sine),
        flops=4 * token_rows * D * QKV,
    )
    if near:
        qkv_owned = reduce_attention(grid, qkv_local)
    else:
        qkv_owned = plain.reduce_attention(qkv_local)
    gains_local = jnp.concatenate([gain_attn, gain_mlp], axis=0)
    if near:
        gains_grad = reduce_all(grid, gains_local)
    else:
        gains_grad = lax.psum(gains_local, ("dp", "seq"))
    owned = (qkv_owned, out_owned, gu_owned, down_owned)
    rate_wide = 0.5 * D ** (-0.5)
    rate_out = 0.5 * max(QUERY_WIDTH // 256, 1) ** (-0.5)
    rate_down = 0.5 * FF ** (-0.5)
    gains_new = adam_update(gains_master, gains_moment, gains_square, gains_grad, gain_rate, 0.0)
    qkv_new = adam_update(qkv_master, qkv_moment, qkv_square, owned[0], rate_wide, weight_decay)
    out_new = adam_update(out_master, out_moment, out_square, owned[1], rate_out, weight_decay)
    gu_new = adam_update(gu_master, gu_moment, gu_square, owned[2], rate_wide, weight_decay)
    down_new = adam_update(down_master, down_moment, down_square, owned[3], rate_down, weight_decay)
    return (
        layer_out,
        tokens_grad,
        gains_grad,
        owned[0],
        owned[1],
        owned[2],
        owned[3],
        gains_new[0],
        gains_new[1],
        gains_new[2],
        qkv_new[0],
        qkv_new[1],
        qkv_new[2],
        qkv_new[0].astype(jnp.bfloat16),
        out_new[0],
        out_new[1],
        out_new[2],
        out_new[0].astype(jnp.bfloat16),
        gu_new[0],
        gu_new[1],
        gu_new[2],
        gu_new[0].astype(jnp.bfloat16),
        down_new[0],
        down_new[1],
        down_new[2],
        down_new[0].astype(jnp.bfloat16),
    )


def solution(mesh):
    in_specs = (
        P(("dp", "seq"), None),
        P(("dp", "seq"), None),
        P("dp"),
        P(),
        P(),
        P(),
        P("dp", "seq"),
        P("dp", "seq"),
        P("dp", "seq"),
        P("dp", "seq"),
        P("dp", "seq"),
        P("dp", "seq"),
        P("dp", None, "seq"),
        P("dp", None, "seq"),
        P("dp", None, "seq"),
        P("seq", "dp"),
        P("seq", "dp"),
        P("seq", "dp"),
    )
    out_specs = (
        P(("dp", "seq"), None),
        P(("dp", "seq"), None),
        P(),
        P("dp", "seq"),
        P("dp", "seq"),
        P("dp", None, "seq"),
        P("seq", "dp"),
        P(),
        P(),
        P(),
        P("dp", "seq"),
        P("dp", "seq"),
        P("dp", "seq"),
        P("dp", "seq"),
        P("dp", "seq"),
        P("dp", "seq"),
        P("dp", "seq"),
        P("dp", "seq"),
        P("dp", None, "seq"),
        P("dp", None, "seq"),
        P("dp", None, "seq"),
        P("dp", None, "seq"),
        P("seq", "dp"),
        P("seq", "dp"),
        P("seq", "dp"),
        P("seq", "dp"),
    )
    return jax.shard_map(
        on_device, mesh=mesh, in_specs=in_specs, out_specs=out_specs, check_vma=False
    )
```

```python
import functools
import math

import jax
import jax.numpy as jnp
from jax import lax
from jax.experimental import pallas as pl
from jax.experimental.pallas import tpu as pltpu
from jax.sharding import PartitionSpec as P

D = 1280
QUERY_HEADS = 20
KEY_VALUE_HEADS = 5
HEAD_SIZE = 64
FF = 3584
QUERY_WIDTH = 1280
PAIR_WIDTH = KEY_VALUE_HEADS * HEAD_SIZE
QKV = QUERY_WIDTH + 2 * PAIR_WIDTH
GROUP = QUERY_HEADS // KEY_VALUE_HEADS


eps_norm = 1e-05
eps_adam = 1e-08
rope_base = 10000.0
beta_one = 0.5
beta_two = 0.5
weight_decay = 0.1
score_after_mask = -1e30
gain_rate = 0.3
lines = 4
half_rows = 2


bf16 = jnp.bfloat16
f32 = jnp.float32


def rope_tables(positions, head_width):
    half_width = head_width // 2
    frequency = rope_base ** (-2.0 * jnp.arange(half_width, dtype=jnp.float32) / head_width)
    angles = positions.astype(jnp.float32)[:, None] * frequency[None, :]
    return (jnp.cos(angles), jnp.sin(angles))


def pick(values, index, axis):
    return lax.dynamic_index_in_dim(values, index, axis, keepdims=False)


def add(left, right, kind=jnp.bfloat16):
    return (left.astype(f32) + right.astype(f32)).astype(kind)


def after(values, *others):
    return lax.optimization_barrier((values,) + others)[0]


class Grid:
    def __init__(self):
        dp = lax.axis_index("dp")
        seq = lax.axis_index("seq")
        self.z, self.x, self.y, self.c = dp // 2, dp % 2, seq // 2, seq % 2

    def swap(self, values, axis, bit):
        count = lax.axis_size(axis)
        return lax.ppermute(values, axis, [(i, i ^ bit) for i in range(count)])

    def swap_x(self, values):
        return self.swap(values, "dp", 1)

    def swap_y(self, values):
        return self.swap(values, "seq", 2)

    def swap_c(self, values):
        return self.swap(values, "seq", 1)

    def send_z(self, values, steps):
        pairs = [(i, (i // 2 + steps) % lines * 2 + i % 2) for i in range(2 * lines)]
        return lax.ppermute(values, "dp", pairs)


MESH = pl.DeviceIdType.MESH


def place_of():
    dp = lax.axis_index("dp")
    seq = lax.axis_index("seq")
    return dp // 2, lax.rem(dp, 2), seq // 2, lax.rem(seq, 2)


def greet(peers):
    barrier = pltpu.get_barrier_semaphore()
    for peer in peers:
        pl.semaphore_signal(barrier, inc=1, device_id=peer, device_id_type=MESH)
    pl.semaphore_wait(barrier, len(peers))


def spread_kernel(count, *refs):
    shards, wholes = refs[:count], refs[count : 2 * count]
    own_sem, sent, got = refs[2 * count :]
    z, x, y, c = place_of()
    mine, other = 2 * y + c, 2 * (1 - y) + c
    rows = shards[0].shape[0]
    half = rows // 2
    x_peer = (2 * z + 1 - x, mine)
    y_peer = (2 * z + x, other)
    c_peer = (2 * z + x, 2 * y + 1 - c)
    z_peers = [(2 * lax.rem(z + k, lines) + x, mine) for k in range(1, lines)]
    greet([x_peer, y_peer, c_peer] + z_peers)
    started = []
    arriving = {}

    def send(array, source, owner, block, peer, slot, part=None):
        view = wholes[array].at[owner, block]
        origin = view if source is None else source
        if part is not None:
            view = view.at[pl.ds(part * half, half)]
            origin = origin.at[pl.ds(part * half, half)]
        copy = pltpu.make_async_remote_copy(
            src_ref=origin,
            dst_ref=view,
            send_sem=sent.at[array, slot],
            recv_sem=got.at[array, slot],
            device_id=peer,
            device_id_type=MESH,
        )
        copy.start()
        started.append(copy)
        arriving[array, slot] = copy

    def arrive(array, slot):
        arriving[array, slot].wait_recv()

    local = []
    for array in range(count):
        copy = pltpu.make_async_copy(
            shards[array], wholes[array].at[mine, 2 * z + x], own_sem.at[array]
        )
        copy.start()
        local.append(copy)
        for k in (1, 3, 2):
            send(array, shards[array], mine, 2 * z + x, z_peers[k - 1], k)

    def first(array, k):
        line = lax.rem(z - k + lines, lines)
        if k:
            arrive(array, k)
        source = None if k else shards[array]
        send(array, source, mine, 2 * line + x, x_peer, 4 + k)
        send(array, source, mine, 2 * line + x, y_peer, 8 + k)
        send(array, source, mine, 2 * line + x, c_peer, 20 + k)

    def second(array, k):
        line = lax.rem(z - k + lines, lines)
        arrive(array, 4 + k)
        send(array, None, mine, 2 * line + 1 - x, y_peer, 12 + k, 0)
        arrive(array, 8 + k)
        send(array, None, other, 2 * line + x, x_peer, 16 + k, 1)
        send(array, None, mine, 2 * line + 1 - x, c_peer, 24 + k)
        send(array, None, other, 2 * line + x, c_peer, 28 + k)

    def third(array, k):
        line = lax.rem(z - k + lines, lines)
        arrive(array, 12 + k)
        arrive(array, 16 + k)
        send(array, None, other, 2 * line + 1 - x, c_peer, 32 + k)

    items = [(array, k) for array in range(count) for k in (0, 1, 3, 2)]
    for at in range(len(items) + 2):
        if at < len(items):
            first(*items[at])
        if 0 <= at - 1 < len(items):
            second(*items[at - 1])
        if 0 <= at - 2:
            third(*items[at - 2])
    for array in range(count):
        for slot in range(20, 36):
            arrive(array, slot)
    for copy in started:
        copy.wait_send()
    for copy in local:
        copy.wait()


def spread(shards):
    count = len(shards)
    anywhere = pl.BlockSpec(memory_space=pl.ANY)
    wholes = pl.pallas_call(
        functools.partial(spread_kernel, count),
        out_shape=[jax.ShapeDtypeStruct((4, 2 * lines) + s.shape, s.dtype) for s in shards],
        in_specs=[anywhere] * count,
        out_specs=[anywhere] * count,
        scratch_shapes=[
            pltpu.SemaphoreType.DMA((count,)),
            pltpu.SemaphoreType.DMA((count, 36)),
            pltpu.SemaphoreType.DMA((count, 36)),
        ],
        compiler_params=pltpu.CompilerParams(collective_id=0, has_side_effects=True),
        name="spread",
    )(*shards)
    return [whole.reshape(4, -1, whole.shape[3]) for whole in wholes]


def gather_lines(grid, shard):
    return [shard] + [grid.send_z(shard, steps) for steps in (1, 3, 2)]


def gather_ffn(grid, shard, widths):
    rows = shard.shape[0]
    wholes = [jnp.zeros((2 * lines, rows, width), bf16) for width in widths]
    for steps, mine in zip((0, 1, 3, 2), gather_lines(grid, shard)):
        line = (grid.z - steps + lines) % lines
        for block, side in ((mine, grid.x), (grid.swap_x(mine), 1 - grid.x)):
            at = 0
            for i, width in enumerate(widths):
                wholes[i] = lax.dynamic_update_slice(
                    wholes[i], block[None, :, at : at + width], (line * 2 + side, 0, 0)
                )
                at += width
    return [whole.reshape(2 * lines * rows, -1) for whole in wholes]


def gather_rows(grid, rows):
    pair = jnp.concatenate([rows, grid.swap_y(rows)], axis=0)
    return jnp.concatenate([pair, grid.swap_c(pair)], axis=0)


class Plain:
    def gather_attention(self, shard):
        blocks = lax.all_gather(shard, ("dp", "seq"), axis=0)
        split = blocks.reshape(lax.axis_size("dp"), lax.axis_size("seq"), *shard.shape)
        return jnp.swapaxes(split, 0, 1).reshape(lax.axis_size("seq"), -1, shard.shape[1])

    def gather_ffn(self, shard, widths):
        whole = lax.all_gather(shard, "dp", axis=0, tiled=True)
        return [whole[:, : widths[0]], whole[:, widths[0] :]]

    def reduce_attention(self, gradient):
        owners, wide, width = gradient.shape
        blocks = gradient.reshape(owners, lax.axis_size("dp"), -1, width)
        blocks = jnp.swapaxes(blocks, 0, 1).reshape(-1, width)
        return lax.psum_scatter(blocks, ("dp", "seq"), scatter_dimension=0, tiled=True).astype(f32)


def spec(space=pltpu.VMEM):
    return pl.BlockSpec(memory_space=space)


def local_call(kernel, name, outs, *args, flops=0, smem=0):
    moved = sum(a.size * a.dtype.itemsize for a in args) + sum(
        math.prod(s) * jnp.dtype(k).itemsize for s, k in outs
    )
    return pl.pallas_call(
        kernel,
        out_shape=[jax.ShapeDtypeStruct(s, k) for s, k in outs],
        in_specs=[spec()] * (len(args) - smem) + [spec(pltpu.SMEM)] * smem,
        out_specs=[spec()] * len(outs),
        compiler_params=pltpu.CompilerParams(vmem_limit_bytes=60 * 2**20),
        cost_estimate=pl.CostEstimate(flops=flops, bytes_accessed=moved, transcendentals=0),
        name=name,
    )(*args)


def dot(left, right, left_axis=1, right_axis=0, **how):
    return lax.dot_general(
        left, right, (((left_axis,), (right_axis,)), ((), ())), preferred_element_type=f32, **how
    )


def rotate(chunk, cosine, sine):
    lane = lax.broadcasted_iota(jnp.int32, chunk.shape, 1)
    swapped = jnp.where(lane % 64 < 32, pltpu.roll(chunk, 96, 1), pltpu.roll(chunk, 32, 1))
    return chunk * cosine + swapped * sine


def project_kernel(tokens, gain, weight, cosine, sine, attn_input, queries, pairs):
    x = tokens[...].astype(f32)
    scale = lax.rsqrt(jnp.mean(x * x, axis=-1, keepdims=True) + eps_norm)
    normed = (x * scale * gain[...]).astype(bf16)
    attn_input[...] = normed
    projected = jnp.concatenate([dot(normed, weight[j]) for j in range(4)], axis=1)
    first = lax.broadcasted_iota(jnp.int32, (x.shape[0], 128), 1) < 64
    for chunk in range(QKV // 128):
        u = projected[:, chunk * 128 : chunk * 128 + 128]
        at = chunk * 128 - QUERY_WIDTH
        if at < 0:
            turned = rotate(u, cosine[...], sine[...]) * HEAD_SIZE ** (-0.5)
            queries[:, chunk * 128 : chunk * 128 + 128] = turned.astype(bf16)
        elif at + 128 <= PAIR_WIDTH:
            pairs[:, at : at + 128] = rotate(u, cosine[...], sine[...]).astype(bf16)
        elif at < PAIR_WIDTH:
            turned = jnp.where(first, rotate(u, cosine[...], sine[...]), u)
            pairs[:, at : at + 128] = turned.astype(bf16)
        else:
            pairs[:, at : at + 128] = u.astype(bf16)


def head(values, index):
    return values[:, index * HEAD_SIZE : (index + 1) * HEAD_SIZE]


def attend_kernel(
    queries, pairs, tokens, weight, gain, query_at, key_at, prefix, mixed, exact, logs, resid, mlp_input
):
    seen = (key_at[...] <= query_at[...]) | (key_at[...] < prefix[0])
    for group in range(KEY_VALUE_HEADS):
        keys = head(pairs, group)
        values = head(pairs, KEY_VALUE_HEADS + group)
        for member in range(GROUP):
            at = group * GROUP + member
            scores = jnp.where(seen, dot(head(queries, at), keys, 1, 1), score_after_mask)
            top = jnp.max(scores, axis=-1, keepdims=True)
            powers = jnp.exp(scores - top)
            total = jnp.sum(powers, axis=-1, keepdims=True)
            exact[:, at * 64 : at * 64 + 64] = dot(powers.astype(bf16), values) / total
            logs[:, at : at + 1] = top + jnp.log(total)
    mixed[...] = exact[...].astype(bf16)
    branch = jnp.concatenate([dot(mixed[...], weight[j]) for j in range(4)], axis=1)
    total = tokens[...].astype(f32) + branch
    resid[...] = total
    scale = lax.rsqrt(jnp.mean(total * total, axis=-1, keepdims=True) + eps_norm)
    mlp_input[...] = (total * scale * gain[...]).astype(bf16)


def back_norm(grad_out, source, gain):
    scale = lax.rsqrt(jnp.mean(source * source, axis=-1, keepdims=True) + eps_norm)
    normed = source * scale
    scaled = grad_out * gain
    inner = jnp.mean(scaled * normed, axis=-1, keepdims=True)
    return jnp.sum(grad_out * normed, axis=0, keepdims=True), scale * (scaled - normed * inner)


def branch_back(
    d_mlp, resid, cotangent, gain, weight, mixed, exact, d_resid, d_mixed, out_grad, gain_grad, deltas
):
    gain_sum, d_normed = back_norm(d_mlp, resid[...], gain[...])
    gain_grad[...] = gain_sum
    total = cotangent[...].astype(f32) + d_normed
    d_resid[...] = total
    width = weight.shape[2]
    d_branch = total.astype(bf16)
    back = None
    for j in range(4):
        part = d_branch[:, j * width : (j + 1) * width]
        out_grad[j] = dot(mixed[...], part, 0, 0).astype(bf16)
        term = dot(part, weight[j], 1, 1)
        back = term if back is None else back + term
    d_mixed[...] = back.astype(bf16)
    product = d_mixed[...].astype(f32) * exact[...]
    which = lax.broadcasted_iota(jnp.int32, (32, QUERY_WIDTH), 1) // HEAD_SIZE
    ones = (which == lax.broadcasted_iota(jnp.int32, (32, QUERY_WIDTH), 0)).astype(f32)
    deltas[...] = dot(ones, product, 1, 1, precision=lax.Precision.HIGHEST)


def branch_back_kernel(d_mlp, *refs):
    branch_back(d_mlp[...], *refs)


def attend_back_group(group, seen, queries, pairs, d_mixed, logs, deltas, d_queries, d_pairs):
    keys = head(pairs, group)
    values = head(pairs, KEY_VALUE_HEADS + group)
    turned_keys = keys.T
    d_keys = d_values = None
    for member in range(GROUP):
        at = group * GROUP + member
        mine = head(queries, at)
        back = head(d_mixed, at)
        scores = jnp.where(seen, dot(keys, mine, 1, 1), score_after_mask)
        probs = jnp.exp(scores - logs[at : at + 1, :])
        d_probs = dot(values, back, 1, 1)
        d_scores = (probs * (d_probs - deltas[at : at + 1, :])).astype(bf16)
        turned = dot(turned_keys, d_scores) * HEAD_SIZE ** (-0.5)
        d_queries[:, at * 64 : at * 64 + 64] = turned.T
        key_term = dot(d_scores, mine)
        value_term = dot(probs.astype(bf16), back)
        d_keys = key_term if d_keys is None else d_keys + key_term
        d_values = value_term if d_values is None else d_values + value_term
    at = group * 64
    d_pairs[:, at : at + 64] = d_keys.astype(bf16)
    at += PAIR_WIDTH
    d_pairs[:, at : at + 64] = d_values.astype(bf16)


def attend_back_kernel(
    queries, pairs, d_mixed, logs, deltas, query_at, key_at, prefix, d_queries, d_pairs
):
    seen = (key_at[...] <= query_at[...]) | (key_at[...] < prefix[0])
    for group in range(KEY_VALUE_HEADS):
        attend_back_group(group, seen, queries, pairs, d_mixed, logs, deltas, d_queries, d_pairs)


def unproject(d_queries, d_pairs, cosine, sine):
    rows = d_queries.shape[0]
    first = lax.broadcasted_iota(jnp.int32, (rows, 128), 1) < 64
    chunks = []
    for chunk in range(QKV // 128):
        at = chunk * 128 - QUERY_WIDTH
        if at < 0:
            chunks.append(rotate(d_queries[:, chunk * 128 : chunk * 128 + 128], cosine[...], -sine[...]))
            continue
        u = d_pairs[:, at : at + 128]
        if at + 128 <= PAIR_WIDTH:
            u = rotate(u, cosine[...], -sine[...])
        elif at < PAIR_WIDTH:
            u = jnp.where(first, rotate(u, cosine[...], -sine[...]), u)
        chunks.append(u)
    return jnp.concatenate([u.astype(bf16) for u in chunks], axis=1)


def project_back_kernel(
    d_queries, d_pairs, attn_input, tokens, d_resid, gain, weight, cosine, sine, tokens_grad, qkv_grad, gain_grad
):
    d_projected = unproject(d_queries, d_pairs, cosine, sine)
    width = weight.shape[2]
    back = None
    for j in range(4):
        part = d_projected[:, j * width : (j + 1) * width]
        qkv_grad[j] = dot(attn_input[...], part, 0, 0).astype(bf16)
        term = dot(part, weight[j], 1, 1)
        back = term if back is None else back + term
    gain_sum, d_normed = back_norm(back, tokens[...].astype(f32), gain[...])
    gain_grad[...] = gain_sum
    tokens_grad[...] = d_resid[...] + d_normed


class Links:
    def __init__(self, sent, got):
        self.sent, self.got, self.copies = sent, got, []

    def send(self, source, target, peer):
        slot = len(self.copies)
        copy = pltpu.make_async_remote_copy(
            src_ref=source,
            dst_ref=target,
            send_sem=self.sent.at[slot],
            recv_sem=self.got.at[slot],
            device_id=peer,
            device_id_type=MESH,
        )
        copy.start()
        self.copies.append(copy)
        return copy

    def finish(self):
        for copy in self.copies:
            copy.wait_send()


class Moves:
    def __init__(self, sems):
        self.sems, self.copies, self.seen = sems, [], set()

    def start(self, source, target):
        slot = len(self.copies)
        copy = pltpu.make_async_copy(source, target, self.sems.at[slot])
        copy.start()
        self.copies.append(copy)
        return slot

    def wait(self, *slots):
        for slot in slots:
            if slot not in self.seen:
                self.seen.add(slot)
                self.copies[slot].wait()

    def finish(self):
        self.wait(*range(len(self.copies)))


class Peers:
    def __init__(self):
        z, x, y, c = place_of()
        self.z, self.x, self.y, self.c = z, x, y, c
        dp, seq = 2 * z + x, 2 * y + c
        self.by_x = (2 * z + 1 - x, seq)
        self.by_y = (dp, 2 * (1 - y) + c)
        self.by_c = (dp, 2 * y + 1 - c)
        self.by_z = {k: (2 * self.line(k) + x, seq) for k in range(1, lines)}

    def line(self, steps):
        return lax.rem(self.z + steps, lines)

    def greet(self):
        greet([self.by_x, self.by_y, self.by_c] + [self.by_z[k] for k in range(1, lines)])


STEPS = (1, 3, 2, 0)


class RowSum:
    def __init__(self, peers, links, partial, arrived, passed, last):
        self.peers, self.links, self.partial = peers, links, partial
        self.arrived, self.passed, self.last = arrived, passed, last
        self.rows = partial.shape[0] // 4
        rows = self.rows
        self.far = links.send(
            partial.at[pl.ds(3 * rows, rows)], arrived.at[pl.ds(rows, rows)], peers.by_c
        )
        self.near = links.send(
            partial.at[pl.ds(2 * rows, rows)], arrived.at[pl.ds(0, rows)], peers.by_c
        )

    def cross(self, across):
        rows = self.rows
        self.far.wait_recv()
        total = across[...].astype(f32) + self.arrived[rows:, :].astype(f32)
        self.passed[...] = total.astype(bf16)
        self.over = self.links.send(self.passed, self.last, self.peers.by_y)

    def total(self, own):
        self.near.wait_recv()
        self.over.wait_recv()
        return (
            own[...].astype(f32)
            + self.arrived[: self.rows, :].astype(f32)
            + self.last[...].astype(f32)
        )


class BlockSum:
    def __init__(self, peers, links, moves, gradient, own, x_in, z_out, z_in):
        self.peers, self.links, self.moves = peers, links, moves
        self.gradient, self.own, self.x_in, self.z_out, self.z_in = gradient, own, x_in, z_out, z_in
        self.arriving, self.slots, self.final, self.kept = {}, {}, {}, None
        for at, k in enumerate(STEPS):
            block = 2 * peers.line(k) + peers.x
            self.slots[k] = [moves.start(gradient.at[block], own.at[at])]

    def taken(self, arrived):
        for at, k in enumerate(STEPS):
            self.slots[k].append(self.moves.start(arrived.at[self.peers.line(k)], self.x_in.at[at]))

    def open(self, k):
        at = STEPS.index(k)
        theirs = 2 * self.peers.line(k) + 1 - self.peers.x
        self.arriving[k] = self.links.send(
            self.gradient.at[theirs], self.x_in.at[at], self.peers.by_x
        )

    def sum_x(self, k):
        at = STEPS.index(k)
        self.moves.wait(*self.slots[k])
        if k in self.arriving:
            self.arriving[k].wait_recv()
        return self.own[at].astype(f32) + self.x_in[at].astype(f32)

    def step(self, k):
        at = STEPS.index(k)
        total = self.sum_x(k)
        if k:
            self.z_out[at] = total.astype(bf16)
            self.final[k] = self.links.send(self.z_out.at[at], self.z_in.at[at], self.peers.by_z[k])
        else:
            self.kept = total

    def total(self):
        total = self.kept
        for at, k in enumerate(STEPS[:-1]):
            self.final[k].wait_recv()
            total = total + self.z_in[at].astype(f32)
        return total


class OwnerSum:
    def __init__(self, peers, links, buffers, own):
        self.peers, self.links, self.own = peers, links, own
        (self.c_in, self.sums, self.y_in, self.x_in, self.x_out, self.y_out) = buffers[:6]
        (self.x_last, self.y_last, self.keep, self.z_out, self.z_in) = buffers[6:]
        self.half = self.sums.shape[3] // 2
        self.over, self.one, self.two, self.final = {}, {}, {}, {}

    def hand(self, source, y_side):
        self.over[y_side] = self.links.send(source, self.c_in.at[y_side], self.peers.by_c)

    def chip(self, y_side):
        self.over[y_side].wait_recv()
        for line in range(lines):
            for side in range(2):
                self.sums[y_side, line, side] = (
                    self.own(y_side, line, side).astype(f32)
                    + self.c_in[y_side, line, side].astype(f32)
                ).astype(bf16)

    def open(self, k):
        p, half = self.peers, self.half
        line, at = p.line(k), STEPS.index(k)
        self.one[k] = (
            self.links.send(
                self.sums.at[1 - p.y, line, :, pl.ds(0, half)], self.y_in.at[at], p.by_y
            ),
            self.links.send(
                self.sums.at[:, line, 1 - p.x, pl.ds(half, half)], self.x_in.at[at], p.by_x
            ),
        )

    def pass_on(self, k):
        p, half = self.peers, self.half
        line, at = p.line(k), STEPS.index(k)
        by_y, by_x = self.one[k]

        def add_up(mine, arrived):
            return mine.astype(f32) + arrived.astype(f32)

        by_y.wait_recv()
        theirs = add_up(self.sums[p.y, line, 1 - p.x, pl.ds(0, half)], self.y_in[at, 1 - p.x])
        self.x_out[at] = theirs.astype(bf16)
        first = self.links.send(self.x_out.at[at], self.x_last.at[at], p.by_x)
        mine = add_up(self.sums[p.y, line, p.x, pl.ds(0, half)], self.y_in[at, p.x])
        self.keep[at, 0:half] = mine
        by_x.wait_recv()
        theirs = add_up(self.sums[1 - p.y, line, p.x, pl.ds(half, half)], self.x_in[at, 1 - p.y])
        self.y_out[at] = theirs.astype(bf16)
        second = self.links.send(self.y_out.at[at], self.y_last.at[at], p.by_y)
        mine = add_up(self.sums[p.y, line, p.x, pl.ds(half, half)], self.x_in[at, p.y])
        self.keep[at, half : 2 * half] = mine
        self.two[k] = first, second

    def close(self, k):
        at, half = STEPS.index(k), self.half
        for copy in self.two[k]:
            copy.wait_recv()
        self.keep[at, 0:half] = self.keep[at, 0:half] + self.x_last[at].astype(f32)
        self.keep[at, half : 2 * half] = self.keep[at, half : 2 * half] + self.y_last[at].astype(f32)
        if k:
            self.z_out[at] = self.keep[at].astype(bf16)
            self.final[k] = self.links.send(self.z_out.at[at], self.z_in.at[at], self.peers.by_z[k])

    def total(self):
        total = self.keep[STEPS.index(0)]
        for at, k in enumerate(STEPS[:-1]):
            self.final[k].wait_recv()
            total = total + self.z_in[at].astype(f32)
        return total


def owner_buffers(rows, width):
    half = rows // 2
    return [
        pltpu.VMEM(shape, kind)
        for shape, kind in (
            ((2, lines, 2, rows, width), bf16),
            ((2, lines, 2, rows, width), bf16),
            ((lines, 2, half, width), bf16),
            ((lines, 2, half, width), bf16),
            ((lines, half, width), bf16),
            ((lines, half, width), bf16),
            ((lines, half, width), bf16),
            ((lines, half, width), bf16),
            ((lines, rows, width), f32),
            ((lines, rows, width), bf16),
            ((lines, rows, width), bf16),
        )
    ]


def back_one_kernel(
    d_mlp_part, branch_part, down, down_taken, gate, up, resid_far, cotangent_far, weight_far, mixed_far, exact_far,
    queries_far, pairs_far, gain, logs, query_at, key_at, prefix,
    layer_out, d_resid, out_grad_far, gain_grad, d_queries, d_kv, down_sum, gate_sum, up_lines,
    d_mlp_own, branch_own, resid, cotangent, weight, mixed, exact, queries, pairs,
    rows_in, rows_out, rows_last, branch_in, branch_out, branch_last, pair_in, pair_out, pair_last,
    d_mixed, deltas, d_pairs, out_grad, own_blocks, x_in, z_out, z_in, local_sem, sent, got,
):
    peers = Peers()
    links, moves = Links(sent, got), Moves(local_sem)
    rows = resid.shape[0]
    own_d_mlp = moves.start(d_mlp_part.at[pl.ds(0, 2 * rows)], d_mlp_own)
    own_branch = moves.start(branch_part.at[pl.ds(0, 2 * rows)], branch_own)
    ready = {}
    for name, source, target in (
        ("resid", resid_far, resid),
        ("cotangent", cotangent_far, cotangent),
        ("weight", weight_far, weight),
        ("mixed", mixed_far, mixed),
        ("exact", exact_far, exact),
        ("queries", queries_far, queries),
        ("pairs", pairs_far, pairs),
    ):
        ready[name] = moves.start(source, target)
    peers.greet()
    d_mlp_sum = RowSum(peers, links, d_mlp_part, rows_in, rows_out, rows_last)
    sums = [
        BlockSum(peers, links, moves, gradient, *(b.at[i] for b in (own_blocks, x_in, z_out, z_in)))
        for i, gradient in enumerate((down, gate, up))
    ]
    sums[0].taken(down_taken)
    for block in sums[1:]:
        for k in STEPS:
            block.open(k)
    branch_sum = RowSum(peers, links, branch_part, branch_in, branch_out, branch_last)
    pending = [(i, k) for i in (1, 2) for k in STEPS]

    def pump(count):
        for _ in range(count):
            if pending:
                i, k = pending.pop(0)
                if i == 1:
                    sums[i].step(k)
                    continue
                at = STEPS.index(k)
                z_out[2, at] = sums[i].sum_x(k).astype(bf16)
                moves.start(z_out.at[2, at], up_lines.at[at])

    moves.wait(own_d_mlp, own_branch)
    d_mlp_sum.cross(d_mlp_own.at[pl.ds(rows, rows)])
    branch_sum.cross(branch_own.at[pl.ds(rows, rows)])
    for k in STEPS:
        sums[0].step(k)
    pump(2)
    moves.wait(*(ready[n] for n in ("resid", "cotangent", "weight", "mixed", "exact")))
    d_mlp = d_mlp_sum.total(d_mlp_own.at[pl.ds(0, rows)])
    branch_back(
        d_mlp, resid, cotangent, gain, weight, mixed, exact, d_resid, d_mixed, out_grad, gain_grad, deltas
    )
    flush = moves.start(out_grad, out_grad_far)
    pump(2)
    moves.wait(ready["queries"], ready["pairs"])
    seen = (key_at[...] <= query_at[...]) | (key_at[...] < prefix[0])
    for group in range(KEY_VALUE_HEADS):
        attend_back_group(group, seen, queries, pairs, d_mixed, logs, deltas, d_queries, d_pairs)
        if group in (0, 2, 4):
            pump(1)
    pair_sum = RowSum(peers, links, d_pairs, pair_in, pair_out, pair_last)
    pair_sum.cross(d_pairs.at[pl.ds(rows, rows)])
    layer_out[...] = (
        resid[...] + branch_sum.total(branch_own.at[pl.ds(0, rows)]).astype(bf16).astype(f32)
    ).astype(bf16)
    pump(8)
    d_kv[...] = pair_sum.total(d_pairs.at[pl.ds(0, rows)])
    down_sum[...] = sums[0].total()
    gate_sum[...] = sums[1].total()
    links.finish()
    moves.finish()


def back_two_kernel(
    up_lines, out_grad, weight_far, d_queries, d_kv, attn_input, tokens, d_resid, gain, cosine, sine, gain_mlp,
    tokens_grad, gains_sum, up_sum, out_sum, qkv_sum,
    weight, out_own, qkv_grad, up_own, z_in,
    gain_own, gain_c, gain_one, gain_y, gain_two, gain_x, gain_z, local_sem, sent, got, *buffers,
):
    peers = Peers()
    links, moves = Links(sent, got), Moves(local_sem)
    own_out = [moves.start(out_grad.at[2 * side + peers.c], out_own.at[side]) for side in range(2)]
    own_up = moves.start(up_lines.at[STEPS.index(0)], up_own)
    weight_in = moves.start(weight_far, weight)
    out_total = OwnerSum(peers, links, buffers[:11], lambda s, line, side: out_own[s, line, side])
    qkv_total = OwnerSum(
        peers, links, buffers[11:], lambda s, line, side: qkv_grad[2 * s + peers.c, line, side]
    )
    peers.greet()
    for side in range(2):
        out_total.hand(out_grad.at[2 * side + 1 - peers.c], side)
    up_copies = [
        links.send(up_lines.at[at], z_in.at[at], peers.by_z[k]) for at, k in enumerate(STEPS[:-1])
    ]
    d_projected = unproject(d_queries, d_kv, cosine, sine)
    moves.wait(*own_out)
    width = weight.shape[2]
    for j in range(4):
        part = d_projected[:, j * width : (j + 1) * width]
        outer = dot(attn_input[...], part, 0, 0).astype(bf16)
        qkv_grad[j] = outer.reshape(qkv_grad.shape[1:])
        if j % 2:
            qkv_total.hand(qkv_grad.at[j - peers.c], j // 2)
        else:
            out_total.chip(j // 2)
        if j == 2:
            for k in STEPS:
                out_total.open(k)
    for side in range(2):
        qkv_total.chip(side)
    for k in STEPS:
        qkv_total.open(k)
    moves.wait(weight_in)
    back = None
    for j in range(4):
        part = d_projected[:, j * width : (j + 1) * width]
        term = dot(part, weight[j], 1, 1)
        back = term if back is None else back + term
    gain_sum, d_normed = back_norm(back, tokens[...].astype(f32), gain[...])
    gain_own[...] = jnp.concatenate([gain_sum, gain_mlp[...]], axis=0)
    gain_copy = links.send(gain_own, gain_c, peers.by_c)
    for k in STEPS:
        out_total.pass_on(k)
    tokens_grad[...] = d_resid[...] + d_normed
    gain_copy.wait_recv()
    gain_one[...] = gain_own[...] + gain_c[...]
    gain_copy = links.send(gain_one, gain_y, peers.by_y)
    for k in STEPS:
        qkv_total.pass_on(k)
    gain_copy.wait_recv()
    gain_two[...] = gain_one[...] + gain_y[...]
    gain_copy = links.send(gain_two, gain_x, peers.by_x)
    for k in STEPS:
        out_total.close(k)
    gain_copy.wait_recv()
    gain_z[peers.z] = gain_two[...] + gain_x[...]
    gain_copies = [
        links.send(gain_z.at[peers.z], gain_z.at[peers.z], peers.by_z[k]) for k in range(1, lines)
    ]
    for k in STEPS:
        qkv_total.close(k)
    moves.wait(own_up)
    up_total = up_own[...].astype(f32)
    for at, copy in enumerate(up_copies):
        copy.wait_recv()
        up_total = up_total + z_in[at].astype(f32)
    up_sum[...] = up_total
    out_sum[...] = out_total.total()
    for copy in gain_copies:
        copy.wait_recv()
    gains_sum[...] = ((gain_z[0] + gain_z[1]) + gain_z[2]) + gain_z[3]
    qkv_sum[...] = qkv_total.total()
    links.finish()
    moves.finish()


def remote_call(kernel, name, number, outs, scratch, *args, local=16, remote=64, smem=0, flops=0):
    places = {False: spec(), True: spec(pl.ANY)}
    return pl.pallas_call(
        kernel,
        out_shape=[jax.ShapeDtypeStruct(s, k) for s, k, _ in outs],
        in_specs=[places[far] for _, far in args[: len(args) - smem]] + [spec(pltpu.SMEM)] * smem,
        out_specs=[places[far] for _, _, far in outs],
        scratch_shapes=scratch[0]
        + [
            pltpu.SemaphoreType.DMA((local,)),
            pltpu.SemaphoreType.DMA((remote,)),
            pltpu.SemaphoreType.DMA((remote,)),
        ]
        + scratch[1],
        compiler_params=pltpu.CompilerParams(
            collective_id=number, has_side_effects=True, vmem_limit_bytes=62 * 2**20
        ),
        cost_estimate=pl.CostEstimate(flops=flops, bytes_accessed=2**24, transcendentals=0),
        name=name,
    )(*(array for array, _ in args))


def vmem_like(array):
    return pltpu.VMEM(array.shape, array.dtype)


def adam_update(master, moment, square, gradient, step_rate, decay):
    moment_next = beta_one * moment + (1.0 - beta_one) * gradient
    square_next = beta_two * square + (1.0 - beta_two) * gradient * gradient
    master_next = master - step_rate * (
        moment_next / (jnp.sqrt(square_next) + eps_adam) + decay * master
    )
    return (master_next, moment_next, square_next)


def on_device(
    tokens,
    cotangent,
    prefix_len,
    gains_master,
    gains_moment,
    gains_square,
    qkv_master,
    qkv_moment,
    qkv_square,
    out_master,
    out_moment,
    out_square,
    gu_master,
    gu_moment,
    gu_square,
    down_master,
    down_moment,
    down_square,
):
    seq_count = lax.axis_size("seq")
    dp_count = lax.axis_size("dp")
    seq_place = lax.axis_index("seq")
    near = dp_count == 2 * lines and seq_count == 4
    grid = Grid() if near else None
    plain = Plain()
    token_rows = tokens.shape[0]
    quarter = FF // seq_count
    shard_rows = gu_master.shape[0]
    qkv_b = qkv_master.astype(bf16)
    out_b = out_master.astype(bf16)
    ffn_b = jnp.concatenate(
        [gu_master.astype(bf16).reshape(shard_rows, 2 * quarter), down_master.astype(bf16).T],
        axis=1,
    )
    widths = (2 * quarter, quarter)
    if near:
        qkv_full, out_full = spread([qkv_b, out_b])
        gu_part, down_part = gather_ffn(grid, after(ffn_b, qkv_full), widths)
        cot_rows = gather_rows(grid, after(cotangent, qkv_full))
        order = (0, 2, 1, 3)
        key_places = [seq_place ^ step for step in order]
    else:
        qkv_full = plain.gather_attention(qkv_b)
        out_full = plain.gather_attention(out_b)
        gu_part, down_part = plain.gather_ffn(ffn_b, widths)
        cot_rows = lax.all_gather(cotangent, "seq", axis=0, tiled=True)
        key_places = list(range(seq_count))
    within = jnp.arange(token_rows, dtype=jnp.int32)
    positions = seq_place * token_rows + within
    key_positions = jnp.concatenate([spot * token_rows + within for spot in key_places])

    cosine_half, sine_half = rope_tables(positions, HEAD_SIZE)
    cosine = jnp.concatenate([cosine_half] * 4, axis=1)
    sine = jnp.concatenate([-sine_half, sine_half] * 2, axis=1)
    shape = (token_rows, D)
    attn_gain, mlp_gain = gains_master[0:1], gains_master[1:2]
    attn_input, queries, kv_local = local_call(
        project_kernel,
        "project",
        [(shape, bf16), (shape, bf16), ((token_rows, 2 * PAIR_WIDTH), bf16)],
        *(tokens, attn_gain, qkv_full, cosine, sine),
        flops=2 * token_rows * D * QKV,
    )
    if near:
        kv_rows = gather_rows(grid, kv_local)
    else:
        kv_rows = lax.all_gather(kv_local, "seq", axis=0, tiled=True)
    score_flops = 2 * token_rows * kv_rows.shape[0] * QUERY_WIDTH
    out_flops = 2 * token_rows * D * D
    mixed, mixed_exact, logs, resid, mlp_input = local_call(
        attend_kernel,
        "attend",
        [(shape, bf16), (shape, f32), ((token_rows, 128), f32), (shape, f32), (shape, bf16)],
        *(queries, kv_rows, tokens, out_full, mlp_gain),
        *(positions[:, None], key_positions[None, :], prefix_len),
        flops=2 * score_flops + out_flops,
        smem=1,
    )
    if near:
        mlp_rows = gather_rows(grid, mlp_input)
    else:
        mlp_rows = lax.all_gather(mlp_input, "seq", axis=0, tiled=True)
    gateup = jnp.dot(mlp_rows, gu_part, preferred_element_type=f32)
    gate = gateup[:, :quarter]
    up_part = gateup[:, quarter:]
    sigmoid_gate = jax.nn.sigmoid(gate)
    silu_gate = gate * sigmoid_gate
    hidden = (silu_gate * up_part).astype(bf16)
    d_hidden = jnp.dot(cot_rows, down_part, preferred_element_type=f32)
    d_gate_b = (d_hidden * up_part * sigmoid_gate * (1.0 + gate * (1.0 - sigmoid_gate))).astype(bf16)
    d_up_b = (d_hidden * silu_gate).astype(bf16)
    d_gateup = jnp.concatenate([d_gate_b, d_up_b], axis=1)

    def contract(left, right, left_axis, right_axis):
        return lax.dot_general(
            left, right, (((left_axis,), (right_axis,)), ((), ())), preferred_element_type=f32
        )

    down_local = contract(cot_rows, hidden, 0, 0).astype(bf16)
    pair_shape = (seq_count, D, out_full.shape[2])
    if near:
        blocks = (2 * lines, shard_rows, quarter)
        lined = (3, lines, shard_rows, quarter)
        down_local = down_local.reshape(blocks)
        down_theirs = pick(down_local.reshape(lines, 2, shard_rows, quarter), 1 - grid.x, 1)
        down_taken = grid.swap_x(down_theirs)
        d_gateup, d_gate_b, d_up_b, hidden = lax.optimization_barrier(
            (d_gateup, d_gate_b, d_up_b, hidden, down_theirs)
        )[:4]
        d_mlp_part = contract(d_gateup, gu_part, 1, 1).astype(bf16)
        branch_part = contract(hidden, down_part, 1, 1).astype(bf16)
        gate_local = contract(mlp_rows, d_gate_b, 0, 0).astype(bf16)
        up_local = contract(mlp_rows, d_up_b, 0, 0).astype(bf16)
        gate_local, up_local = gate_local.reshape(blocks), up_local.reshape(blocks)
        pair = (token_rows, 2 * PAIR_WIDTH)
        rows_of = [((2 * token_rows, D), bf16), (shape, bf16), (shape, bf16)]
        pairs_of = [((2 * token_rows, 2 * PAIR_WIDTH), bf16), (pair, bf16), (pair, bf16)]
        far = [resid, cotangent, out_full, mixed, mixed_exact, queries, kv_rows]
        layer_out, d_resid, out_local, gain_mlp, d_queries, d_kv, down_owned, gate_owned, up_lines = remote_call(
            back_one_kernel,
            "back_one",
            1,
            [
                (shape, bf16, False),
                (shape, f32, False),
                (pair_shape, bf16, True),
                ((1, D), f32, False),
                (shape, f32, False),
                (pair, f32, False),
                ((shard_rows, quarter), f32, False),
                ((shard_rows, quarter), f32, False),
                (lined[1:], bf16, True),
            ],
            (
                [pltpu.VMEM((2 * token_rows, D), bf16)] * 2
                + [vmem_like(a) for a in far]
                + [pltpu.VMEM(*s) for s in rows_of + rows_of + pairs_of]
                + [
                    pltpu.VMEM(shape, bf16),
                    pltpu.VMEM((32, token_rows), f32),
                    pltpu.VMEM(kv_rows.shape, bf16),
                    pltpu.VMEM(pair_shape, bf16),
                ]
                + [pltpu.VMEM(lined, bf16)] * 4,
                [],
            ),
            *((a, True) for a in (d_mlp_part, branch_part)),
            *((a, True) for a in (down_local, down_taken, gate_local, up_local, *far)),
            *((a, False) for a in (mlp_gain, logs.T, positions[None, :], key_positions[:, None])),
            (prefix_len, False),
            local=40,
            smem=1,
            flops=5 * score_flops + 2 * out_flops,
        )
        line_shape = (seq_count, lines, 2, shard_rows)
        qkv_width, out_width = qkv_full.shape[2], out_full.shape[2]
        tokens_grad, gains_grad, up_owned, out_owned, qkv_owned = remote_call(
            back_two_kernel,
            "back_two",
            2,
            [
                (shape, f32, False),
                ((2, D), f32, False),
                ((shard_rows, quarter), f32, False),
                ((shard_rows, out_width), f32, False),
                ((shard_rows, qkv_width), f32, False),
            ],
            (
                [
                    vmem_like(qkv_full),
                    pltpu.VMEM((2,) + line_shape[1:] + (out_width,), bf16),
                    pltpu.VMEM(line_shape + (qkv_width,), bf16),
                ]
                + [pltpu.VMEM(blocks[1:], bf16), pltpu.VMEM((3,) + blocks[1:], bf16)]
                + [pltpu.VMEM((2, D), f32)] * 6
                + [pltpu.VMEM((lines, 2, D), f32)],
                owner_buffers(shard_rows, out_width) + owner_buffers(shard_rows, qkv_width),
            ),
            *((a, True) for a in (up_lines, out_local.reshape(line_shape + (-1,)), qkv_full)),
            *((a, False) for a in (d_queries, d_kv, attn_input, tokens, d_resid, attn_gain)),
            *((a, False) for a in (cosine, sine, gain_mlp)),
            flops=4 * token_rows * D * QKV,
        )
        gu_owned = jnp.stack([gate_owned, up_owned], axis=1)
    else:
        d_mlp_part = contract(d_gateup, gu_part, 1, 1).astype(bf16)
        branch_part = contract(hidden, down_part, 1, 1).astype(bf16)
        gu_local = contract(mlp_rows, d_gateup, 0, 0).astype(bf16)

        def scatter(values, axis):
            return lax.psum_scatter(values, axis, scatter_dimension=0, tiled=True).astype(f32)

        d_mlp_input = scatter(d_mlp_part, "seq")
        layer_out = (resid + scatter(branch_part, "seq")).astype(bf16)
        down_owned = scatter(down_local, "dp")
        gu_owned = scatter(gu_local, "dp").reshape(shard_rows, 2, quarter)
        d_resid, d_mixed, out_local, gain_mlp, deltas = local_call(
            branch_back_kernel,
            "branch_back",
            [(shape, f32), (shape, bf16), (pair_shape, bf16), ((1, D), f32), ((32, token_rows), f32)],
            *(d_mlp_input, resid, cotangent, mlp_gain, out_full, mixed, mixed_exact),
            flops=2 * out_flops,
        )
        out_owned = plain.reduce_attention(out_local)
        d_queries, d_pairs = local_call(
            attend_back_kernel,
            "attend_back",
            [(shape, f32), (kv_rows.shape, bf16)],
            *(queries, kv_rows, d_mixed, logs.T, deltas),
            *(positions[None, :], key_positions[:, None], prefix_len),
            flops=5 * score_flops,
            smem=1,
        )
        d_kv = scatter(d_pairs, "seq")
        tokens_grad, qkv_local, gain_attn = local_call(
            project_back_kernel,
            "project_back",
            [(shape, f32), (qkv_full.shape, bf16), ((1, D), f32)],
            *(d_queries, d_kv, attn_input, tokens, d_resid, attn_gain, qkv_full, cosine, sine),
            flops=4 * token_rows * D * QKV,
        )
        qkv_owned = plain.reduce_attention(qkv_local)
        gains_grad = lax.psum(jnp.concatenate([gain_attn, gain_mlp], axis=0), ("dp", "seq"))
    down_owned = down_owned.T
    owned = (qkv_owned, out_owned, gu_owned, down_owned)
    rate_wide = 0.5 * D ** (-0.5)
    rate_out = 0.5 * max(QUERY_WIDTH // 256, 1) ** (-0.5)
    rate_down = 0.5 * FF ** (-0.5)
    gains_new = adam_update(gains_master, gains_moment, gains_square, gains_grad, gain_rate, 0.0)
    qkv_new = adam_update(qkv_master, qkv_moment, qkv_square, owned[0], rate_wide, weight_decay)
    out_new = adam_update(out_master, out_moment, out_square, owned[1], rate_out, weight_decay)
    gu_new = adam_update(gu_master, gu_moment, gu_square, owned[2], rate_wide, weight_decay)
    down_new = adam_update(down_master, down_moment, down_square, owned[3], rate_down, weight_decay)
    return (
        layer_out,
        tokens_grad,
        gains_grad,
        owned[0],
        owned[1],
        owned[2],
        owned[3],
        gains_new[0],
        gains_new[1],
        gains_new[2],
        qkv_new[0],
        qkv_new[1],
        qkv_new[2],
        qkv_new[0].astype(jnp.bfloat16),
        out_new[0],
        out_new[1],
        out_new[2],
        out_new[0].astype(jnp.bfloat16),
        gu_new[0],
        gu_new[1],
        gu_new[2],
        gu_new[0].astype(jnp.bfloat16),
        down_new[0],
        down_new[1],
        down_new[2],
        down_new[0].astype(jnp.bfloat16),
    )


def solution(mesh):
    in_specs = (
        P(("dp", "seq"), None),
        P(("dp", "seq"), None),
        P("dp"),
        P(),
        P(),
        P(),
        P("dp", "seq"),
        P("dp", "seq"),
        P("dp", "seq"),
        P("dp", "seq"),
        P("dp", "seq"),
        P("dp", "seq"),
        P("dp", None, "seq"),
        P("dp", None, "seq"),
        P("dp", None, "seq"),
        P("seq", "dp"),
        P("seq", "dp"),
        P("seq", "dp"),
    )
    out_specs = (
        P(("dp", "seq"), None),
        P(("dp", "seq"), None),
        P(),
        P("dp", "seq"),
        P("dp", "seq"),
        P("dp", None, "seq"),
        P("seq", "dp"),
        P(),
        P(),
        P(),
        P("dp", "seq"),
        P("dp", "seq"),
        P("dp", "seq"),
        P("dp", "seq"),
        P("dp", "seq"),
        P("dp", "seq"),
        P("dp", "seq"),
        P("dp", "seq"),
        P("dp", None, "seq"),
        P("dp", None, "seq"),
        P("dp", None, "seq"),
        P("dp", None, "seq"),
        P("seq", "dp"),
        P("seq", "dp"),
        P("seq", "dp"),
        P("seq", "dp"),
    )
    return jax.shard_map(
        on_device, mesh=mesh, in_specs=in_specs, out_specs=out_specs, check_vma=False
    )
```

```python
import functools
import math

import jax
import jax.numpy as jnp
from jax import lax
from jax.experimental import pallas as pl
from jax.experimental.pallas import tpu as pltpu
from jax.sharding import PartitionSpec as P

D = 1280
QUERY_HEADS = 20
KEY_VALUE_HEADS = 5
HEAD_SIZE = 64
FF = 3584
QUERY_WIDTH = 1280
PAIR_WIDTH = KEY_VALUE_HEADS * HEAD_SIZE
QKV = QUERY_WIDTH + 2 * PAIR_WIDTH
GROUP = QUERY_HEADS // KEY_VALUE_HEADS


eps_norm = 1e-05
eps_adam = 1e-08
rope_base = 10000.0
beta_one = 0.5
beta_two = 0.5
weight_decay = 0.1
score_after_mask = -1e30
gain_rate = 0.3
lines = 4
half_rows = 2


bf16 = jnp.bfloat16
f32 = jnp.float32


def rope_tables(positions, head_width):
    half_width = head_width // 2
    frequency = rope_base ** (-2.0 * jnp.arange(half_width, dtype=jnp.float32) / head_width)
    angles = positions.astype(jnp.float32)[:, None] * frequency[None, :]
    return (jnp.cos(angles), jnp.sin(angles))


def pick(values, index, axis):
    return lax.dynamic_index_in_dim(values, index, axis, keepdims=False)


def add(left, right, kind=jnp.bfloat16):
    return (left.astype(f32) + right.astype(f32)).astype(kind)


def after(values, *others):
    return lax.optimization_barrier((values,) + others)[0]


class Grid:
    def __init__(self):
        dp = lax.axis_index("dp")
        seq = lax.axis_index("seq")
        self.z, self.x, self.y, self.c = dp // 2, dp % 2, seq // 2, seq % 2

    def swap(self, values, axis, bit):
        count = lax.axis_size(axis)
        return lax.ppermute(values, axis, [(i, i ^ bit) for i in range(count)])

    def swap_x(self, values):
        return self.swap(values, "dp", 1)

    def swap_y(self, values):
        return self.swap(values, "seq", 2)

    def swap_c(self, values):
        return self.swap(values, "seq", 1)

    def send_z(self, values, steps):
        pairs = [(i, (i // 2 + steps) % lines * 2 + i % 2) for i in range(2 * lines)]
        return lax.ppermute(values, "dp", pairs)


MESH = pl.DeviceIdType.MESH


def place_of():
    dp = lax.axis_index("dp")
    seq = lax.axis_index("seq")
    return dp // 2, lax.rem(dp, 2), seq // 2, lax.rem(seq, 2)


def greet(peers):
    barrier = pltpu.get_barrier_semaphore()
    for peer in peers:
        pl.semaphore_signal(barrier, inc=1, device_id=peer, device_id_type=MESH)
    pl.semaphore_wait(barrier, len(peers))


class Plain:
    def gather_attention(self, shard):
        blocks = lax.all_gather(shard, ("dp", "seq"), axis=0)
        split = blocks.reshape(lax.axis_size("dp"), lax.axis_size("seq"), *shard.shape)
        return jnp.swapaxes(split, 0, 1).reshape(lax.axis_size("seq"), -1, shard.shape[1])

    def reduce_attention(self, gradient):
        owners, wide, width = gradient.shape
        blocks = gradient.reshape(owners, lax.axis_size("dp"), -1, width)
        blocks = jnp.swapaxes(blocks, 0, 1).reshape(-1, width)
        return lax.psum_scatter(blocks, ("dp", "seq"), scatter_dimension=0, tiled=True).astype(f32)


def spec(space=pltpu.VMEM):
    return pl.BlockSpec(memory_space=space)


def local_call(kernel, name, outs, *args, flops=0, smem=0):
    moved = sum(a.size * a.dtype.itemsize for a in args) + sum(
        math.prod(s) * jnp.dtype(k).itemsize for s, k in outs
    )
    return pl.pallas_call(
        kernel,
        out_shape=[jax.ShapeDtypeStruct(s, k) for s, k in outs],
        in_specs=[spec()] * (len(args) - smem) + [spec(pltpu.SMEM)] * smem,
        out_specs=[spec()] * len(outs),
        compiler_params=pltpu.CompilerParams(vmem_limit_bytes=60 * 2**20),
        cost_estimate=pl.CostEstimate(flops=flops, bytes_accessed=moved, transcendentals=0),
        name=name,
    )(*args)


def dot(left, right, left_axis=1, right_axis=0, **how):
    return lax.dot_general(
        left, right, (((left_axis,), (right_axis,)), ((), ())), preferred_element_type=f32, **how
    )


def rotate(chunk, cosine, sine):
    lane = lax.broadcasted_iota(jnp.int32, chunk.shape, 1)
    swapped = jnp.where(lane % 64 < 32, pltpu.roll(chunk, 96, 1), pltpu.roll(chunk, 32, 1))
    return chunk * cosine + swapped * sine


def project(tokens, gain, weights, cosine, sine, attn_input, queries, pairs):
    x = tokens[...].astype(f32)
    scale = lax.rsqrt(jnp.mean(x * x, axis=-1, keepdims=True) + eps_norm)
    normed = (x * scale * gain[...]).astype(bf16)
    attn_input[...] = normed
    projected = jnp.concatenate([dot(normed, block) for block in weights], axis=1)
    first = lax.broadcasted_iota(jnp.int32, (x.shape[0], 128), 1) < 64
    for chunk in (*range(QUERY_WIDTH // 128, QKV // 128), *range(QUERY_WIDTH // 128)):
        u = projected[:, chunk * 128 : chunk * 128 + 128]
        at = chunk * 128 - QUERY_WIDTH
        if at < 0:
            turned = rotate(u, cosine[...], sine[...]) * HEAD_SIZE ** (-0.5)
            queries[:, chunk * 128 : chunk * 128 + 128] = turned.astype(bf16)
        elif at + 128 <= PAIR_WIDTH:
            pairs[:, at : at + 128] = rotate(u, cosine[...], sine[...]).astype(bf16)
        elif at < PAIR_WIDTH:
            turned = jnp.where(first, rotate(u, cosine[...], sine[...]), u)
            pairs[:, at : at + 128] = turned.astype(bf16)
        else:
            pairs[:, at : at + 128] = u.astype(bf16)


def project_kernel(tokens, gain, weight, *refs):
    project(tokens, gain, [weight[j] for j in range(4)], *refs)


def head(values, index):
    return values[:, index * HEAD_SIZE : (index + 1) * HEAD_SIZE]


def attend_group(group, seen, queries, pairs, exact, logs):
    keys = head(pairs, group)
    values = head(pairs, KEY_VALUE_HEADS + group)
    for member in range(GROUP):
        at = group * GROUP + member
        scores = jnp.where(seen, dot(head(queries, at), keys, 1, 1), score_after_mask)
        top = jnp.max(scores, axis=-1, keepdims=True)
        powers = jnp.exp(scores - top)
        total = jnp.sum(powers, axis=-1, keepdims=True)
        exact[:, at * 64 : at * 64 + 64] = dot(powers.astype(bf16), values) / total
        logs[:, at : at + 1] = top + jnp.log(total)


def close_attention(tokens, weights, gain, mixed, exact, resid, mlp_input):
    mixed[...] = exact[...].astype(bf16)
    branch = jnp.concatenate([dot(mixed[...], block) for block in weights], axis=1)
    total = tokens[...].astype(f32) + branch
    resid[...] = total
    scale = lax.rsqrt(jnp.mean(total * total, axis=-1, keepdims=True) + eps_norm)
    mlp_input[...] = (total * scale * gain[...]).astype(bf16)


def attend_kernel(
    queries, pairs, tokens, weight, gain, query_at, key_at, prefix, mixed, exact, logs, resid, mlp_input
):
    seen = (key_at[...] <= query_at[...]) | (key_at[...] < prefix[0])
    for group in range(KEY_VALUE_HEADS):
        attend_group(group, seen, queries, pairs, exact, logs)
    close_attention(tokens, [weight[j] for j in range(4)], gain, mixed, exact, resid, mlp_input)


def back_norm(grad_out, source, gain):
    scale = lax.rsqrt(jnp.mean(source * source, axis=-1, keepdims=True) + eps_norm)
    normed = source * scale
    scaled = grad_out * gain
    inner = jnp.mean(scaled * normed, axis=-1, keepdims=True)
    return jnp.sum(grad_out * normed, axis=0, keepdims=True), scale * (scaled - normed * inner)


def branch_back(
    d_mlp, resid, cotangent, gain, weight, mixed, exact, d_resid, d_mixed, out_grad, gain_grad, deltas
):
    gain_sum, d_normed = back_norm(d_mlp, resid[...], gain[...])
    gain_grad[...] = gain_sum
    total = cotangent[...].astype(f32) + d_normed
    d_resid[...] = total
    width = weight.shape[2]
    d_branch = total.astype(bf16)
    back = None
    for j in range(4):
        part = d_branch[:, j * width : (j + 1) * width]
        out_grad[j] = dot(mixed[...], part, 0, 0).astype(bf16)
        term = dot(part, weight[j], 1, 1)
        back = term if back is None else back + term
    d_mixed[...] = back.astype(bf16)
    product = d_mixed[...].astype(f32) * exact[...]
    which = lax.broadcasted_iota(jnp.int32, (32, QUERY_WIDTH), 1) // HEAD_SIZE
    ones = (which == lax.broadcasted_iota(jnp.int32, (32, QUERY_WIDTH), 0)).astype(f32)
    deltas[...] = dot(ones, product, 1, 1, precision=lax.Precision.HIGHEST)


def branch_back_kernel(d_mlp, *refs):
    branch_back(d_mlp[...], *refs)


def attend_back_group(group, seen, queries, pairs, d_mixed, logs, deltas, d_queries, d_pairs):
    keys = head(pairs, group)
    values = head(pairs, KEY_VALUE_HEADS + group)
    turned_keys = keys.T
    d_keys = d_values = None
    for member in range(GROUP):
        at = group * GROUP + member
        mine = head(queries, at)
        back = head(d_mixed, at)
        scores = jnp.where(seen, dot(keys, mine, 1, 1), score_after_mask)
        probs = jnp.exp(scores - logs[at : at + 1, :])
        d_probs = dot(values, back, 1, 1)
        d_scores = (probs * (d_probs - deltas[at : at + 1, :])).astype(bf16)
        turned = dot(turned_keys, d_scores) * HEAD_SIZE ** (-0.5)
        d_queries[:, at * 64 : at * 64 + 64] = turned.T
        key_term = dot(d_scores, mine)
        value_term = dot(probs.astype(bf16), back)
        d_keys = key_term if d_keys is None else d_keys + key_term
        d_values = value_term if d_values is None else d_values + value_term
    at = group * 64
    d_pairs[:, at : at + 64] = d_keys.astype(bf16)
    at += PAIR_WIDTH
    d_pairs[:, at : at + 64] = d_values.astype(bf16)


def attend_back_kernel(
    queries, pairs, d_mixed, logs, deltas, query_at, key_at, prefix, d_queries, d_pairs
):
    seen = (key_at[...] <= query_at[...]) | (key_at[...] < prefix[0])
    for group in range(KEY_VALUE_HEADS):
        attend_back_group(group, seen, queries, pairs, d_mixed, logs, deltas, d_queries, d_pairs)


def unproject(d_queries, d_pairs, cosine, sine):
    rows = d_queries.shape[0]
    first = lax.broadcasted_iota(jnp.int32, (rows, 128), 1) < 64
    chunks = []
    for chunk in range(QKV // 128):
        at = chunk * 128 - QUERY_WIDTH
        if at < 0:
            chunks.append(rotate(d_queries[:, chunk * 128 : chunk * 128 + 128], cosine[...], -sine[...]))
            continue
        u = d_pairs[:, at : at + 128]
        if at + 128 <= PAIR_WIDTH:
            u = rotate(u, cosine[...], -sine[...])
        elif at < PAIR_WIDTH:
            u = jnp.where(first, rotate(u, cosine[...], -sine[...]), u)
        chunks.append(u)
    return jnp.concatenate([u.astype(bf16) for u in chunks], axis=1)


def project_back_kernel(
    d_queries, d_pairs, attn_input, tokens, d_resid, gain, weight, cosine, sine, tokens_grad, qkv_grad, gain_grad
):
    d_projected = unproject(d_queries, d_pairs, cosine, sine)
    width = weight.shape[2]
    back = None
    for j in range(4):
        part = d_projected[:, j * width : (j + 1) * width]
        qkv_grad[j] = dot(attn_input[...], part, 0, 0).astype(bf16)
        term = dot(part, weight[j], 1, 1)
        back = term if back is None else back + term
    gain_sum, d_normed = back_norm(back, tokens[...].astype(f32), gain[...])
    gain_grad[...] = gain_sum
    tokens_grad[...] = d_resid[...] + d_normed


class Links:
    def __init__(self, sent, got):
        self.sent, self.got, self.copies = sent, got, []

    def send(self, source, target, peer):
        slot = len(self.copies)
        copy = pltpu.make_async_remote_copy(
            src_ref=source,
            dst_ref=target,
            send_sem=self.sent.at[slot],
            recv_sem=self.got.at[slot],
            device_id=peer,
            device_id_type=MESH,
        )
        copy.start()
        self.copies.append(copy)
        return copy

    def finish(self):
        for copy in self.copies:
            copy.wait_send()


class Moves:
    def __init__(self, sems):
        self.sems, self.copies, self.seen = sems, [], set()

    def start(self, source, target):
        slot = len(self.copies)
        copy = pltpu.make_async_copy(source, target, self.sems.at[slot])
        copy.start()
        self.copies.append(copy)
        return slot

    def wait(self, *slots):
        for slot in slots:
            if slot not in self.seen:
                self.seen.add(slot)
                self.copies[slot].wait()

    def finish(self):
        self.wait(*range(len(self.copies)))


class Peers:
    def __init__(self):
        z, x, y, c = place_of()
        self.z, self.x, self.y, self.c = z, x, y, c
        dp, seq = 2 * z + x, 2 * y + c
        self.by_x = (2 * z + 1 - x, seq)
        self.by_y = (dp, 2 * (1 - y) + c)
        self.by_c = (dp, 2 * y + 1 - c)
        self.by_z = {k: (2 * self.line(k) + x, seq) for k in range(1, lines)}

    def line(self, steps):
        return lax.rem(self.z + steps, lines)

    def greet(self):
        greet([self.by_x, self.by_y, self.by_c] + [self.by_z[k] for k in range(1, lines)])


STEPS = (1, 3, 2, 0)


class RowSum:
    def __init__(self, peers, links, partial, arrived, passed, last):
        self.peers, self.links, self.partial = peers, links, partial
        self.arrived, self.passed, self.last = arrived, passed, last
        self.rows = partial.shape[0] // 4
        rows = self.rows
        self.far = links.send(
            partial.at[pl.ds(3 * rows, rows)], arrived.at[pl.ds(rows, rows)], peers.by_c
        )
        self.near = links.send(
            partial.at[pl.ds(2 * rows, rows)], arrived.at[pl.ds(0, rows)], peers.by_c
        )

    def cross(self, across):
        rows = self.rows
        self.far.wait_recv()
        total = across[...].astype(f32) + self.arrived[rows:, :].astype(f32)
        self.passed[...] = total.astype(bf16)
        self.over = self.links.send(self.passed, self.last, self.peers.by_y)

    def total(self, own):
        self.near.wait_recv()
        self.over.wait_recv()
        return (
            own[...].astype(f32)
            + self.arrived[: self.rows, :].astype(f32)
            + self.last[...].astype(f32)
        )


class BlockSum:
    def __init__(self, peers, links, moves, gradient, own, x_in, z_out, z_in):
        self.peers, self.links, self.moves = peers, links, moves
        self.gradient, self.own, self.x_in, self.z_out, self.z_in = gradient, own, x_in, z_out, z_in
        self.arriving, self.slots, self.final, self.kept = {}, {}, {}, None
        for at, k in enumerate(STEPS):
            block = 2 * peers.line(k) + peers.x
            self.slots[k] = [moves.start(gradient.at[block], own.at[at])]

    def taken(self, arrived):
        for at, k in enumerate(STEPS):
            self.slots[k].append(self.moves.start(arrived.at[self.peers.line(k)], self.x_in.at[at]))

    def open(self, k):
        at = STEPS.index(k)
        theirs = 2 * self.peers.line(k) + 1 - self.peers.x
        self.arriving[k] = self.links.send(
            self.gradient.at[theirs], self.x_in.at[at], self.peers.by_x
        )

    def sum_x(self, k):
        at = STEPS.index(k)
        self.moves.wait(*self.slots[k])
        if k in self.arriving:
            self.arriving[k].wait_recv()
        return self.own[at].astype(f32) + self.x_in[at].astype(f32)

    def step(self, k):
        at = STEPS.index(k)
        total = self.sum_x(k)
        if k:
            self.z_out[at] = total.astype(bf16)
            self.final[k] = self.links.send(self.z_out.at[at], self.z_in.at[at], self.peers.by_z[k])
        else:
            self.kept = total

    def total(self):
        total = self.kept
        for at, k in enumerate(STEPS[:-1]):
            self.final[k].wait_recv()
            total = total + self.z_in[at].astype(f32)
        return total


class OwnerSum:
    def __init__(self, peers, links, buffers, own):
        self.peers, self.links, self.own = peers, links, own
        (self.c_in, self.sums, self.y_in, self.x_in, self.x_out, self.y_out) = buffers[:6]
        (self.x_last, self.y_last, self.keep, self.z_out, self.z_in) = buffers[6:]
        self.half = self.sums.shape[3] // 2
        self.over, self.one, self.two, self.final = {}, {}, {}, {}

    def hand(self, source, y_side):
        self.over[y_side] = self.links.send(source, self.c_in.at[y_side], self.peers.by_c)

    def chip(self, y_side):
        self.over[y_side].wait_recv()
        for line in range(lines):
            for side in range(2):
                self.sums[y_side, line, side] = (
                    self.own(y_side, line, side).astype(f32)
                    + self.c_in[y_side, line, side].astype(f32)
                ).astype(bf16)

    def open(self, k):
        p, half = self.peers, self.half
        line, at = p.line(k), STEPS.index(k)
        self.one[k] = (
            self.links.send(
                self.sums.at[1 - p.y, line, :, pl.ds(0, half)], self.y_in.at[at], p.by_y
            ),
            self.links.send(
                self.sums.at[:, line, 1 - p.x, pl.ds(half, half)], self.x_in.at[at], p.by_x
            ),
        )

    def pass_on(self, k):
        p, half = self.peers, self.half
        line, at = p.line(k), STEPS.index(k)
        by_y, by_x = self.one[k]

        def add_up(mine, arrived):
            return mine.astype(f32) + arrived.astype(f32)

        by_y.wait_recv()
        theirs = add_up(self.sums[p.y, line, 1 - p.x, pl.ds(0, half)], self.y_in[at, 1 - p.x])
        self.x_out[at] = theirs.astype(bf16)
        first = self.links.send(self.x_out.at[at], self.x_last.at[at], p.by_x)
        mine = add_up(self.sums[p.y, line, p.x, pl.ds(0, half)], self.y_in[at, p.x])
        self.keep[at, 0:half] = mine
        by_x.wait_recv()
        theirs = add_up(self.sums[1 - p.y, line, p.x, pl.ds(half, half)], self.x_in[at, 1 - p.y])
        self.y_out[at] = theirs.astype(bf16)
        second = self.links.send(self.y_out.at[at], self.y_last.at[at], p.by_y)
        mine = add_up(self.sums[p.y, line, p.x, pl.ds(half, half)], self.x_in[at, p.y])
        self.keep[at, half : 2 * half] = mine
        self.two[k] = first, second

    def close(self, k):
        at, half = STEPS.index(k), self.half
        for copy in self.two[k]:
            copy.wait_recv()
        self.keep[at, 0:half] = self.keep[at, 0:half] + self.x_last[at].astype(f32)
        self.keep[at, half : 2 * half] = self.keep[at, half : 2 * half] + self.y_last[at].astype(f32)
        if k:
            self.z_out[at] = self.keep[at].astype(bf16)
            self.final[k] = self.links.send(self.z_out.at[at], self.z_in.at[at], self.peers.by_z[k])

    def total(self):
        total = self.keep[STEPS.index(0)]
        for at, k in enumerate(STEPS[:-1]):
            self.final[k].wait_recv()
            total = total + self.z_in[at].astype(f32)
        return total


def owner_buffers(rows, width):
    half = rows // 2
    return [
        pltpu.VMEM(shape, kind)
        for shape, kind in (
            ((2, lines, 2, rows, width), bf16),
            ((2, lines, 2, rows, width), bf16),
            ((lines, 2, half, width), bf16),
            ((lines, 2, half, width), bf16),
            ((lines, half, width), bf16),
            ((lines, half, width), bf16),
            ((lines, half, width), bf16),
            ((lines, half, width), bf16),
            ((lines, rows, width), f32),
            ((lines, rows, width), bf16),
            ((lines, rows, width), bf16),
        )
    ]


def front_kernel(
    qkv_shard, out_shard, gu_shard, down_shard, cotangent, tokens, attn_gain, mlp_gain, cosine, sine,
    query_at, key_at, prefix,
    qkv_far, out_far, gu_far, down_far, attn_input, queries, pairs_far, mixed, exact, logs, resid, mlp_rows, cot_rows,
    qkv_full, out_full, pairs, mlp_input, local_sem, sent, got,
):
    peers = Peers()
    links, moves = Links(sent, got), Moves(local_sem)
    z, x, y, c = peers.z, peers.x, peers.y, peers.c
    mine, other = 2 * y + c, 2 * (1 - y) + c
    rows = tokens.shape[0]
    half = qkv_shard.shape[0] // 2
    shards, wholes = (qkv_shard, out_shard), (qkv_full, out_full)
    ffn_shards, ffn_wholes = (gu_shard, down_shard), (gu_far, down_far)
    own = 2 * z + x
    local = [moves.start(s, w.at[mine, own]) for s, w in zip(shards, wholes)]
    local += [moves.start(s, w.at[own]) for s, w in zip(ffn_shards, ffn_wholes)]
    local.append(moves.start(cotangent, cot_rows.at[pl.ds(0, rows)]))
    peers.greet()
    order = (0, 1, 3, 2)
    came = {}
    for array in range(2):
        for k in order[1:]:
            came[array, "z", k] = links.send(
                shards[array], wholes[array].at[mine, own], peers.by_z[k]
            )
    for k in order[1:]:
        for array in range(2):
            came["ffn", array, "z", k] = links.send(
                ffn_shards[array], ffn_wholes[array].at[own], peers.by_z[k]
            )

    def source_line(k):
        return lax.rem(z - k + lines, lines)

    def first(array, k):
        block = 2 * source_line(k) + x
        if k:
            came[array, "z", k].wait_recv()
        view = wholes[array].at[mine, block]
        origin = view if k else shards[array]
        came[array, "x", k] = links.send(origin, view, peers.by_x)
        came[array, "y", k] = links.send(origin, view, peers.by_y)
        came[array, "c", k, 0] = links.send(origin, view, peers.by_c)

    def second(array, k):
        side, line = 2 * source_line(k) + 1 - x, 2 * source_line(k) + x
        came[array, "x", k].wait_recv()
        view = wholes[array].at[mine, side]
        upper = view if array else view.at[pl.ds(0, half)]
        came[array, "xy", k] = links.send(upper, upper, peers.by_y)
        came[array, "c", k, 1] = links.send(view, view, peers.by_c)
        came[array, "y", k].wait_recv()
        view = wholes[array].at[other, line]
        if not array:
            lower = view.at[pl.ds(half, half)]
            came[array, "yx", k] = links.send(lower, lower, peers.by_x)
        came[array, "c", k, 2] = links.send(view, view, peers.by_c)

    def third(array, k):
        view = wholes[array].at[other, 2 * source_line(k) + 1 - x]
        came[array, "xy", k].wait_recv()
        if not array:
            came[array, "yx", k].wait_recv()
        came[array, "c", k, 3] = links.send(view, view, peers.by_c)

    def ffn(k):
        for array in range(2):
            if k:
                came["ffn", array, "z", k].wait_recv()
            view = ffn_wholes[array].at[2 * source_line(k) + x]
            origin = view if k else ffn_shards[array]
            came["ffn", array, "x", k] = links.send(origin, view, peers.by_x)

    def complete(array):
        for k in order:
            for part in range(4):
                came[array, "c", k, part].wait_recv()
        moves.wait(local[array])

    for at in range(6):
        if at < 4:
            first(0, order[at])
        if 1 <= at <= 4:
            second(0, order[at - 1])
        if at >= 2:
            third(0, order[at - 2])
    ffn(0)
    complete(0)
    flat_qkv = [qkv_full[j].reshape(-1, qkv_full.shape[3]) for j in range(4)]
    project(
        tokens, attn_gain, flat_qkv, cosine, sine, attn_input, queries, pairs.at[pl.ds(0, rows)]
    )
    pair_y = links.send(pairs.at[pl.ds(0, rows)], pairs.at[pl.ds(rows, rows)], peers.by_y)
    pair_c = links.send(pairs.at[pl.ds(0, rows)], pairs.at[pl.ds(2 * rows, rows)], peers.by_c)
    moves.start(qkv_full, qkv_far)
    for k in order:
        first(1, k)
    ffn(1)
    pair_y.wait_recv()
    pair_yc = links.send(pairs.at[pl.ds(rows, rows)], pairs.at[pl.ds(3 * rows, rows)], peers.by_c)
    pair_c.wait_recv()
    pair_yc.wait_recv()
    moves.start(pairs, pairs_far)
    seen = (key_at[...] <= query_at[...]) | (key_at[...] < prefix[0])
    attend_group(0, seen, queries, pairs, exact, logs)
    for k in order:
        second(1, k)
    cot_y = links.send(cotangent, cot_rows.at[pl.ds(rows, rows)], peers.by_y)
    cot_c = links.send(cotangent, cot_rows.at[pl.ds(2 * rows, rows)], peers.by_c)
    attend_group(1, seen, queries, pairs, exact, logs)
    attend_group(2, seen, queries, pairs, exact, logs)
    ffn(3)
    for k in order:
        third(1, k)
    attend_group(3, seen, queries, pairs, exact, logs)
    attend_group(4, seen, queries, pairs, exact, logs)
    complete(1)
    moves.start(out_full, out_far)
    flat_out = [out_full[j].reshape(-1, out_full.shape[3]) for j in range(4)]
    close_attention(tokens, flat_out, mlp_gain, mixed, exact, resid, mlp_input)
    mlp_y = links.send(mlp_input, mlp_rows.at[pl.ds(rows, rows)], peers.by_y)
    mlp_c = links.send(mlp_input, mlp_rows.at[pl.ds(2 * rows, rows)], peers.by_c)
    moves.start(mlp_input, mlp_rows.at[pl.ds(0, rows)])
    cot_y.wait_recv()
    view = cot_rows.at[pl.ds(rows, rows)]
    cot_yc = links.send(view, cot_rows.at[pl.ds(3 * rows, rows)], peers.by_c)
    ffn(2)
    mlp_y.wait_recv()
    view = mlp_rows.at[pl.ds(rows, rows)]
    mlp_yc = links.send(view, mlp_rows.at[pl.ds(3 * rows, rows)], peers.by_c)
    for copy in (cot_c, cot_yc, mlp_c, mlp_yc):
        copy.wait_recv()
    for k in order:
        for array in range(2):
            came["ffn", array, "x", k].wait_recv()
    links.finish()
    moves.finish()


def back_one_kernel(
    d_mlp_part, branch_part, down, down_taken, gate, up, resid_far, cotangent_far, weight_far, mixed_far, exact_far,
    queries_far, pairs_far, gain, logs, query_at, key_at, prefix,
    layer_out, d_resid, out_grad_far, gain_grad, d_queries, d_kv, down_sum, gate_sum, up_lines,
    d_mlp_own, branch_own, resid, cotangent, weight, mixed, exact, queries, pairs,
    rows_in, rows_out, rows_last, branch_in, branch_out, branch_last, pair_in, pair_out, pair_last,
    d_mixed, deltas, d_pairs, out_grad, own_blocks, x_in, z_out, z_in, local_sem, sent, got,
):
    peers = Peers()
    links, moves = Links(sent, got), Moves(local_sem)
    rows = resid.shape[0]
    own_d_mlp = moves.start(d_mlp_part.at[pl.ds(0, 2 * rows)], d_mlp_own)
    own_branch = moves.start(branch_part.at[pl.ds(0, 2 * rows)], branch_own)
    ready = {}
    for name, source, target in (
        ("resid", resid_far, resid),
        ("cotangent", cotangent_far, cotangent),
        ("weight", weight_far, weight),
        ("mixed", mixed_far, mixed),
        ("exact", exact_far, exact),
        ("queries", queries_far, queries),
        ("pairs", pairs_far, pairs),
    ):
        ready[name] = moves.start(source, target)
    peers.greet()
    d_mlp_sum = RowSum(peers, links, d_mlp_part, rows_in, rows_out, rows_last)
    sums = [
        BlockSum(peers, links, moves, gradient, *(b.at[i] for b in (own_blocks, x_in, z_out, z_in)))
        for i, gradient in enumerate((down, gate, up))
    ]
    sums[0].taken(down_taken)
    for block in sums[1:]:
        for k in STEPS:
            block.open(k)
    branch_sum = RowSum(peers, links, branch_part, branch_in, branch_out, branch_last)
    pending = [(i, k) for i in (1, 2) for k in STEPS]

    def pump(count):
        for _ in range(count):
            if pending:
                i, k = pending.pop(0)
                if i == 1:
                    sums[i].step(k)
                    continue
                at = STEPS.index(k)
                z_out[2, at] = sums[i].sum_x(k).astype(bf16)
                moves.start(z_out.at[2, at], up_lines.at[at])

    moves.wait(own_d_mlp, own_branch)
    d_mlp_sum.cross(d_mlp_own.at[pl.ds(rows, rows)])
    branch_sum.cross(branch_own.at[pl.ds(rows, rows)])
    for k in STEPS:
        sums[0].step(k)
    pump(2)
    moves.wait(*(ready[n] for n in ("resid", "cotangent", "weight", "mixed", "exact")))
    d_mlp = d_mlp_sum.total(d_mlp_own.at[pl.ds(0, rows)])
    branch_back(
        d_mlp, resid, cotangent, gain, weight, mixed, exact, d_resid, d_mixed, out_grad, gain_grad, deltas
    )
    flush = moves.start(out_grad, out_grad_far)
    pump(2)
    moves.wait(ready["queries"], ready["pairs"])
    seen = (key_at[...] <= query_at[...]) | (key_at[...] < prefix[0])
    for group in range(KEY_VALUE_HEADS):
        attend_back_group(group, seen, queries, pairs, d_mixed, logs, deltas, d_queries, d_pairs)
        if group in (0, 2, 4):
            pump(1)
    pair_sum = RowSum(peers, links, d_pairs, pair_in, pair_out, pair_last)
    pair_sum.cross(d_pairs.at[pl.ds(rows, rows)])
    layer_out[...] = (
        resid[...] + branch_sum.total(branch_own.at[pl.ds(0, rows)]).astype(bf16).astype(f32)
    ).astype(bf16)
    pump(8)
    d_kv[...] = pair_sum.total(d_pairs.at[pl.ds(0, rows)])
    down_sum[...] = sums[0].total()
    gate_sum[...] = sums[1].total()
    links.finish()
    moves.finish()


def back_two_kernel(
    up_lines, out_grad, weight_far, d_queries, d_kv, attn_input, tokens, d_resid, gain, cosine, sine, gain_mlp,
    tokens_grad, gains_sum, up_sum, out_sum, qkv_sum,
    weight, out_own, qkv_grad, up_own, z_in,
    gain_own, gain_c, gain_one, gain_y, gain_two, gain_x, gain_z, local_sem, sent, got, *buffers,
):
    peers = Peers()
    links, moves = Links(sent, got), Moves(local_sem)
    own_out = [moves.start(out_grad.at[2 * side + peers.c], out_own.at[side]) for side in range(2)]
    own_up = moves.start(up_lines.at[STEPS.index(0)], up_own)
    weight_in = moves.start(weight_far, weight)
    out_total = OwnerSum(peers, links, buffers[:11], lambda s, line, side: out_own[s, line, side])
    qkv_total = OwnerSum(
        peers, links, buffers[11:], lambda s, line, side: qkv_grad[2 * s + peers.c, line, side]
    )
    peers.greet()
    for side in range(2):
        out_total.hand(out_grad.at[2 * side + 1 - peers.c], side)
    up_copies = [
        links.send(up_lines.at[at], z_in.at[at], peers.by_z[k]) for at, k in enumerate(STEPS[:-1])
    ]
    d_projected = unproject(d_queries, d_kv, cosine, sine)
    moves.wait(*own_out)
    width = weight.shape[2]
    for j in range(4):
        part = d_projected[:, j * width : (j + 1) * width]
        outer = dot(attn_input[...], part, 0, 0).astype(bf16)
        qkv_grad[j] = outer.reshape(qkv_grad.shape[1:])
        if j % 2:
            qkv_total.hand(qkv_grad.at[j - peers.c], j // 2)
        else:
            out_total.chip(j // 2)
        if j == 2:
            for k in STEPS:
                out_total.open(k)
    for side in range(2):
        qkv_total.chip(side)
    for k in STEPS:
        qkv_total.open(k)
    moves.wait(weight_in)
    back = None
    for j in range(4):
        part = d_projected[:, j * width : (j + 1) * width]
        term = dot(part, weight[j], 1, 1)
        back = term if back is None else back + term
    gain_sum, d_normed = back_norm(back, tokens[...].astype(f32), gain[...])
    gain_own[...] = jnp.concatenate([gain_sum, gain_mlp[...]], axis=0)
    gain_copy = links.send(gain_own, gain_c, peers.by_c)
    for k in STEPS:
        out_total.pass_on(k)
    tokens_grad[...] = d_resid[...] + d_normed
    gain_copy.wait_recv()
    gain_one[...] = gain_own[...] + gain_c[...]
    gain_copy = links.send(gain_one, gain_y, peers.by_y)
    for k in STEPS:
        qkv_total.pass_on(k)
    gain_copy.wait_recv()
    gain_two[...] = gain_one[...] + gain_y[...]
    gain_copy = links.send(gain_two, gain_x, peers.by_x)
    for k in STEPS:
        out_total.close(k)
    gain_copy.wait_recv()
    gain_z[peers.z] = gain_two[...] + gain_x[...]
    gain_copies = [
        links.send(gain_z.at[peers.z], gain_z.at[peers.z], peers.by_z[k]) for k in range(1, lines)
    ]
    for k in STEPS:
        qkv_total.close(k)
    moves.wait(own_up)
    up_total = up_own[...].astype(f32)
    for at, copy in enumerate(up_copies):
        copy.wait_recv()
        up_total = up_total + z_in[at].astype(f32)
    up_sum[...] = up_total
    out_sum[...] = out_total.total()
    for copy in gain_copies:
        copy.wait_recv()
    gains_sum[...] = ((gain_z[0] + gain_z[1]) + gain_z[2]) + gain_z[3]
    qkv_sum[...] = qkv_total.total()
    links.finish()
    moves.finish()


def remote_call(kernel, name, number, outs, scratch, *args, local=16, remote=64, smem=0, flops=0):
    places = {False: spec(), True: spec(pl.ANY)}
    return pl.pallas_call(
        kernel,
        out_shape=[jax.ShapeDtypeStruct(s, k) for s, k, _ in outs],
        in_specs=[places[far] for _, far in args[: len(args) - smem]] + [spec(pltpu.SMEM)] * smem,
        out_specs=[places[far] for _, _, far in outs],
        scratch_shapes=scratch[0]
        + [
            pltpu.SemaphoreType.DMA((local,)),
            pltpu.SemaphoreType.DMA((remote,)),
            pltpu.SemaphoreType.DMA((remote,)),
        ]
        + scratch[1],
        compiler_params=pltpu.CompilerParams(
            collective_id=number, has_side_effects=True, vmem_limit_bytes=62 * 2**20
        ),
        cost_estimate=pl.CostEstimate(flops=flops, bytes_accessed=2**24, transcendentals=0),
        name=name,
    )(*(array for array, _ in args))


def vmem_like(array):
    return pltpu.VMEM(array.shape, array.dtype)


def adam_update(master, moment, square, gradient, step_rate, decay):
    moment_next = beta_one * moment + (1.0 - beta_one) * gradient
    square_next = beta_two * square + (1.0 - beta_two) * gradient * gradient
    master_next = master - step_rate * (
        moment_next / (jnp.sqrt(square_next) + eps_adam) + decay * master
    )
    return (master_next, moment_next, square_next)


def on_device(
    tokens,
    cotangent,
    prefix_len,
    gains_master,
    gains_moment,
    gains_square,
    qkv_master,
    qkv_moment,
    qkv_square,
    out_master,
    out_moment,
    out_square,
    gu_master,
    gu_moment,
    gu_square,
    down_master,
    down_moment,
    down_square,
):
    seq_count = lax.axis_size("seq")
    dp_count = lax.axis_size("dp")
    seq_place = lax.axis_index("seq")
    near = dp_count == 2 * lines and seq_count == 4
    grid = Grid() if near else None
    plain = Plain()
    token_rows = tokens.shape[0]
    quarter = FF // seq_count
    shard_rows = gu_master.shape[0]
    qkv_b = qkv_master.astype(bf16)
    out_b = out_master.astype(bf16)
    gu_b = gu_master.astype(bf16).reshape(shard_rows, 2 * quarter)
    down_b = down_master.astype(bf16).T
    if near:
        key_places = [seq_place ^ step for step in (0, 2, 1, 3)]
    else:
        key_places = list(range(seq_count))
    within = jnp.arange(token_rows, dtype=jnp.int32)
    positions = seq_place * token_rows + within
    key_positions = jnp.concatenate([spot * token_rows + within for spot in key_places])

    cosine_half, sine_half = rope_tables(positions, HEAD_SIZE)
    cosine = jnp.concatenate([cosine_half] * 4, axis=1)
    sine = jnp.concatenate([-sine_half, sine_half] * 2, axis=1)
    shape = (token_rows, D)
    attn_gain, mlp_gain = gains_master[0:1], gains_master[1:2]
    key_count = seq_count * token_rows
    score_flops = 2 * token_rows * key_count * QUERY_WIDTH
    out_flops = 2 * token_rows * D * D
    pair = (token_rows, 2 * PAIR_WIDTH)
    all_pairs = (key_count, 2 * PAIR_WIDTH)
    if near:
        wide = (seq_count, 2 * lines)
        outs = [
            (wide + qkv_b.shape, bf16, True),
            (wide + out_b.shape, bf16, True),
            (wide[1:] + gu_b.shape, bf16, True),
            (wide[1:] + down_b.shape, bf16, True),
            (shape, bf16, False),
            (shape, bf16, False),
            (all_pairs, bf16, True),
            (shape, bf16, False),
            (shape, f32, False),
            ((token_rows, 128), f32, False),
            (shape, f32, False),
            ((key_count, D), bf16, True),
            ((key_count, D), bf16, True),
        ]
        front = remote_call(
            front_kernel,
            "front",
            0,
            outs,
            (
                [pltpu.VMEM(s, k) for s, k, _ in outs[:2]]
                + [pltpu.VMEM(all_pairs, bf16), pltpu.VMEM(shape, bf16)],
                [],
            ),
            *((a, True) for a in (qkv_b, out_b, gu_b, down_b, cotangent)),
            *((a, False) for a in (tokens, attn_gain, mlp_gain, cosine, sine)),
            *((a, False) for a in (positions[:, None], key_positions[None, :], prefix_len)),
            remote=96,
            smem=1,
            flops=2 * token_rows * D * QKV + 2 * score_flops + out_flops,
        )
        qkv_full, out_full, gu_part, down_part, attn_input, queries, kv_rows = front[:7]
        mixed, mixed_exact, logs, resid, mlp_rows, cot_rows = front[7:]
        qkv_full = qkv_full.reshape(seq_count, D, -1)
        out_full = out_full.reshape(seq_count, D, -1)
        gu_part, down_part = gu_part.reshape(D, -1), down_part.reshape(D, -1)
    else:
        qkv_full = plain.gather_attention(qkv_b)
        out_full = plain.gather_attention(out_b)
        gu_part = lax.all_gather(gu_b, "dp", axis=0, tiled=True)
        down_part = lax.all_gather(down_b, "dp", axis=0, tiled=True)
        cot_rows = lax.all_gather(cotangent, "seq", axis=0, tiled=True)
        attn_input, queries, kv_local = local_call(
            project_kernel,
            "project",
            [(shape, bf16), (shape, bf16), (pair, bf16)],
            *(tokens, attn_gain, qkv_full, cosine, sine),
            flops=2 * token_rows * D * QKV,
        )
        kv_rows = lax.all_gather(kv_local, "seq", axis=0, tiled=True)
        mixed, mixed_exact, logs, resid, mlp_input = local_call(
            attend_kernel,
            "attend",
            [(shape, bf16), (shape, f32), ((token_rows, 128), f32), (shape, f32), (shape, bf16)],
            *(queries, kv_rows, tokens, out_full, mlp_gain),
            *(positions[:, None], key_positions[None, :], prefix_len),
            flops=2 * score_flops + out_flops,
            smem=1,
        )
        mlp_rows = lax.all_gather(mlp_input, "seq", axis=0, tiled=True)
    gateup = jnp.dot(mlp_rows, gu_part, preferred_element_type=f32)
    gate = gateup[:, :quarter]
    up_part = gateup[:, quarter:]
    sigmoid_gate = jax.nn.sigmoid(gate)
    silu_gate = gate * sigmoid_gate
    hidden = (silu_gate * up_part).astype(bf16)
    d_hidden = jnp.dot(cot_rows, down_part, preferred_element_type=f32)
    d_gate_b = (d_hidden * up_part * sigmoid_gate * (1.0 + gate * (1.0 - sigmoid_gate))).astype(bf16)
    d_up_b = (d_hidden * silu_gate).astype(bf16)
    d_gateup = jnp.concatenate([d_gate_b, d_up_b], axis=1)

    def contract(left, right, left_axis, right_axis):
        return lax.dot_general(
            left, right, (((left_axis,), (right_axis,)), ((), ())), preferred_element_type=f32
        )

    down_local = contract(cot_rows, hidden, 0, 0).astype(bf16)
    pair_shape = (seq_count, D, out_full.shape[2])
    if near:
        blocks = (2 * lines, shard_rows, quarter)
        lined = (3, lines, shard_rows, quarter)
        down_local = down_local.reshape(blocks)
        down_theirs = pick(down_local.reshape(lines, 2, shard_rows, quarter), 1 - grid.x, 1)
        down_taken = grid.swap_x(down_theirs)
        d_gateup, d_gate_b, d_up_b, hidden = lax.optimization_barrier(
            (d_gateup, d_gate_b, d_up_b, hidden, down_theirs)
        )[:4]
        d_mlp_part = contract(d_gateup, gu_part, 1, 1).astype(bf16)
        branch_part = contract(hidden, down_part, 1, 1).astype(bf16)
        gate_local = contract(mlp_rows, d_gate_b, 0, 0).astype(bf16)
        up_local = contract(mlp_rows, d_up_b, 0, 0).astype(bf16)
        gate_local, up_local = gate_local.reshape(blocks), up_local.reshape(blocks)
        rows_of = [((2 * token_rows, D), bf16), (shape, bf16), (shape, bf16)]
        pairs_of = [((2 * token_rows, 2 * PAIR_WIDTH), bf16), (pair, bf16), (pair, bf16)]
        far = [resid, cotangent, out_full, mixed, mixed_exact, queries, kv_rows]
        layer_out, d_resid, out_local, gain_mlp, d_queries, d_kv, down_owned, gate_owned, up_lines = remote_call(
            back_one_kernel,
            "back_one",
            1,
            [
                (shape, bf16, False),
                (shape, f32, False),
                (pair_shape, bf16, True),
                ((1, D), f32, False),
                (shape, f32, False),
                (pair, f32, False),
                ((shard_rows, quarter), f32, False),
                ((shard_rows, quarter), f32, False),
                (lined[1:], bf16, True),
            ],
            (
                [pltpu.VMEM((2 * token_rows, D), bf16)] * 2
                + [vmem_like(a) for a in far]
                + [pltpu.VMEM(*s) for s in rows_of + rows_of + pairs_of]
                + [
                    pltpu.VMEM(shape, bf16),
                    pltpu.VMEM((32, token_rows), f32),
                    pltpu.VMEM(kv_rows.shape, bf16),
                    pltpu.VMEM(pair_shape, bf16),
                ]
                + [pltpu.VMEM(lined, bf16)] * 4,
                [],
            ),
            *((a, True) for a in (d_mlp_part, branch_part)),
            *((a, True) for a in (down_local, down_taken, gate_local, up_local, *far)),
            *((a, False) for a in (mlp_gain, logs.T, positions[None, :], key_positions[:, None])),
            (prefix_len, False),
            local=40,
            smem=1,
            flops=5 * score_flops + 2 * out_flops,
        )
        line_shape = (seq_count, lines, 2, shard_rows)
        qkv_width, out_width = qkv_full.shape[2], out_full.shape[2]
        tokens_grad, gains_grad, up_owned, out_owned, qkv_owned = remote_call(
            back_two_kernel,
            "back_two",
            2,
            [
                (shape, f32, False),
                ((2, D), f32, False),
                ((shard_rows, quarter), f32, False),
                ((shard_rows, out_width), f32, False),
                ((shard_rows, qkv_width), f32, False),
            ],
            (
                [
                    vmem_like(qkv_full),
                    pltpu.VMEM((2,) + line_shape[1:] + (out_width,), bf16),
                    pltpu.VMEM(line_shape + (qkv_width,), bf16),
                ]
                + [pltpu.VMEM(blocks[1:], bf16), pltpu.VMEM((3,) + blocks[1:], bf16)]
                + [pltpu.VMEM((2, D), f32)] * 6
                + [pltpu.VMEM((lines, 2, D), f32)],
                owner_buffers(shard_rows, out_width) + owner_buffers(shard_rows, qkv_width),
            ),
            *((a, True) for a in (up_lines, out_local.reshape(line_shape + (-1,)), qkv_full)),
            *((a, False) for a in (d_queries, d_kv, attn_input, tokens, d_resid, attn_gain)),
            *((a, False) for a in (cosine, sine, gain_mlp)),
            flops=4 * token_rows * D * QKV,
        )
        gu_owned = jnp.stack([gate_owned, up_owned], axis=1)
    else:
        d_mlp_part = contract(d_gateup, gu_part, 1, 1).astype(bf16)
        branch_part = contract(hidden, down_part, 1, 1).astype(bf16)
        gu_local = contract(mlp_rows, d_gateup, 0, 0).astype(bf16)

        def scatter(values, axis):
            return lax.psum_scatter(values, axis, scatter_dimension=0, tiled=True).astype(f32)

        d_mlp_input = scatter(d_mlp_part, "seq")
        layer_out = (resid + scatter(branch_part, "seq")).astype(bf16)
        down_owned = scatter(down_local, "dp")
        gu_owned = scatter(gu_local, "dp").reshape(shard_rows, 2, quarter)
        d_resid, d_mixed, out_local, gain_mlp, deltas = local_call(
            branch_back_kernel,
            "branch_back",
            [(shape, f32), (shape, bf16), (pair_shape, bf16), ((1, D), f32), ((32, token_rows), f32)],
            *(d_mlp_input, resid, cotangent, mlp_gain, out_full, mixed, mixed_exact),
            flops=2 * out_flops,
        )
        out_owned = plain.reduce_attention(out_local)
        d_queries, d_pairs = local_call(
            attend_back_kernel,
            "attend_back",
            [(shape, f32), (kv_rows.shape, bf16)],
            *(queries, kv_rows, d_mixed, logs.T, deltas),
            *(positions[None, :], key_positions[:, None], prefix_len),
            flops=5 * score_flops,
            smem=1,
        )
        d_kv = scatter(d_pairs, "seq")
        tokens_grad, qkv_local, gain_attn = local_call(
            project_back_kernel,
            "project_back",
            [(shape, f32), (qkv_full.shape, bf16), ((1, D), f32)],
            *(d_queries, d_kv, attn_input, tokens, d_resid, attn_gain, qkv_full, cosine, sine),
            flops=4 * token_rows * D * QKV,
        )
        qkv_owned = plain.reduce_attention(qkv_local)
        gains_grad = lax.psum(jnp.concatenate([gain_attn, gain_mlp], axis=0), ("dp", "seq"))
    down_owned = down_owned.T
    owned = (qkv_owned, out_owned, gu_owned, down_owned)
    rate_wide = 0.5 * D ** (-0.5)
    rate_out = 0.5 * max(QUERY_WIDTH // 256, 1) ** (-0.5)
    rate_down = 0.5 * FF ** (-0.5)
    gains_new = adam_update(gains_master, gains_moment, gains_square, gains_grad, gain_rate, 0.0)
    qkv_new = adam_update(qkv_master, qkv_moment, qkv_square, owned[0], rate_wide, weight_decay)
    out_new = adam_update(out_master, out_moment, out_square, owned[1], rate_out, weight_decay)
    gu_new = adam_update(gu_master, gu_moment, gu_square, owned[2], rate_wide, weight_decay)
    down_new = adam_update(down_master, down_moment, down_square, owned[3], rate_down, weight_decay)
    return (
        layer_out,
        tokens_grad,
        gains_grad,
        owned[0],
        owned[1],
        owned[2],
        owned[3],
        gains_new[0],
        gains_new[1],
        gains_new[2],
        qkv_new[0],
        qkv_new[1],
        qkv_new[2],
        qkv_new[0].astype(jnp.bfloat16),
        out_new[0],
        out_new[1],
        out_new[2],
        out_new[0].astype(jnp.bfloat16),
        gu_new[0],
        gu_new[1],
        gu_new[2],
        gu_new[0].astype(jnp.bfloat16),
        down_new[0],
        down_new[1],
        down_new[2],
        down_new[0].astype(jnp.bfloat16),
    )


def solution(mesh):
    in_specs = (
        P(("dp", "seq"), None),
        P(("dp", "seq"), None),
        P("dp"),
        P(),
        P(),
        P(),
        P("dp", "seq"),
        P("dp", "seq"),
        P("dp", "seq"),
        P("dp", "seq"),
        P("dp", "seq"),
        P("dp", "seq"),
        P("dp", None, "seq"),
        P("dp", None, "seq"),
        P("dp", None, "seq"),
        P("seq", "dp"),
        P("seq", "dp"),
        P("seq", "dp"),
    )
    out_specs = (
        P(("dp", "seq"), None),
        P(("dp", "seq"), None),
        P(),
        P("dp", "seq"),
        P("dp", "seq"),
        P("dp", None, "seq"),
        P("seq", "dp"),
        P(),
        P(),
        P(),
        P("dp", "seq"),
        P("dp", "seq"),
        P("dp", "seq"),
        P("dp", "seq"),
        P("dp", "seq"),
        P("dp", "seq"),
        P("dp", "seq"),
        P("dp", "seq"),
        P("dp", None, "seq"),
        P("dp", None, "seq"),
        P("dp", None, "seq"),
        P("dp", None, "seq"),
        P("seq", "dp"),
        P("seq", "dp"),
        P("seq", "dp"),
        P("seq", "dp"),
    )
    return jax.shard_map(
        on_device, mesh=mesh, in_specs=in_specs, out_specs=out_specs, check_vma=False
    )
```

```python
import functools
import math

import jax
import jax.numpy as jnp
from jax import lax
from jax.experimental import pallas as pl
from jax.experimental.layout import Layout, with_layout_constraint
from jax.experimental.pallas import tpu as pltpu
from jax.sharding import PartitionSpec as P

D = 1280
QUERY_HEADS = 20
KEY_VALUE_HEADS = 5
HEAD_SIZE = 64
FF = 3584
QUERY_WIDTH = 1280
PAIR_WIDTH = KEY_VALUE_HEADS * HEAD_SIZE
QKV = QUERY_WIDTH + 2 * PAIR_WIDTH
GROUP = QUERY_HEADS // KEY_VALUE_HEADS


eps_norm = 1e-05
eps_adam = 1e-08
rope_base = 10000.0
beta_one = 0.5
beta_two = 0.5
weight_decay = 0.1
score_after_mask = -1e30
gain_rate = 0.3
lines = 4
half_rows = 2


bf16 = jnp.bfloat16
f32 = jnp.float32


def rope_tables(positions, head_width):
    half_width = head_width // 2
    frequency = rope_base ** (-2.0 * jnp.arange(half_width, dtype=jnp.float32) / head_width)
    angles = positions.astype(jnp.float32)[:, None] * frequency[None, :]
    return (jnp.cos(angles), jnp.sin(angles))


def pick(values, index, axis):
    return lax.dynamic_index_in_dim(values, index, axis, keepdims=False)


def add(left, right, kind=jnp.bfloat16):
    return (left.astype(f32) + right.astype(f32)).astype(kind)


def after(values, *others):
    return lax.optimization_barrier((values,) + others)[0]


class Grid:
    def __init__(self):
        dp = lax.axis_index("dp")
        seq = lax.axis_index("seq")
        self.z, self.x, self.y, self.c = dp // 2, dp % 2, seq // 2, seq % 2

    def swap(self, values, axis, bit):
        count = lax.axis_size(axis)
        return lax.ppermute(values, axis, [(i, i ^ bit) for i in range(count)])

    def swap_x(self, values):
        return self.swap(values, "dp", 1)

    def swap_y(self, values):
        return self.swap(values, "seq", 2)

    def swap_c(self, values):
        return self.swap(values, "seq", 1)

    def send_z(self, values, steps):
        pairs = [(i, (i // 2 + steps) % lines * 2 + i % 2) for i in range(2 * lines)]
        return lax.ppermute(values, "dp", pairs)


MESH = pl.DeviceIdType.MESH


def place_of():
    dp = lax.axis_index("dp")
    seq = lax.axis_index("seq")
    return dp // 2, lax.rem(dp, 2), seq // 2, lax.rem(seq, 2)


def greet(peers):
    barrier = pltpu.get_barrier_semaphore()
    for peer in peers:
        pl.semaphore_signal(barrier, inc=1, device_id=peer, device_id_type=MESH)
    pl.semaphore_wait(barrier, len(peers))


class Plain:
    def gather_attention(self, shard):
        blocks = lax.all_gather(shard, ("dp", "seq"), axis=0)
        split = blocks.reshape(lax.axis_size("dp"), lax.axis_size("seq"), *shard.shape)
        return jnp.swapaxes(split, 0, 1).reshape(lax.axis_size("seq"), -1, shard.shape[1])

    def reduce_attention(self, gradient):
        owners, wide, width = gradient.shape
        blocks = gradient.reshape(owners, lax.axis_size("dp"), -1, width)
        blocks = jnp.swapaxes(blocks, 0, 1).reshape(-1, width)
        return lax.psum_scatter(blocks, ("dp", "seq"), scatter_dimension=0, tiled=True).astype(f32)


def spec(space=pltpu.VMEM):
    return pl.BlockSpec(memory_space=space)


def local_call(kernel, name, outs, *args, flops=0, smem=0):
    moved = sum(a.size * a.dtype.itemsize for a in args) + sum(
        math.prod(s) * jnp.dtype(k).itemsize for s, k in outs
    )
    return pl.pallas_call(
        kernel,
        out_shape=[jax.ShapeDtypeStruct(s, k) for s, k in outs],
        in_specs=[spec()] * (len(args) - smem) + [spec(pltpu.SMEM)] * smem,
        out_specs=[spec()] * len(outs),
        compiler_params=pltpu.CompilerParams(vmem_limit_bytes=60 * 2**20),
        cost_estimate=pl.CostEstimate(flops=flops, bytes_accessed=moved, transcendentals=0),
        name=name,
    )(*args)


def dot(left, right, left_axis=1, right_axis=0, **how):
    return lax.dot_general(
        left, right, (((left_axis,), (right_axis,)), ((), ())), preferred_element_type=f32, **how
    )


def rotate(chunk, cosine, sine):
    lane = lax.broadcasted_iota(jnp.int32, chunk.shape, 1)
    swapped = jnp.where(lane % 64 < 32, pltpu.roll(chunk, 96, 1), pltpu.roll(chunk, 32, 1))
    return chunk * cosine + swapped * sine


def project(tokens, gain, weights, cosine, sine, attn_input, queries, pairs):
    x = tokens[...].astype(f32)
    scale = lax.rsqrt(jnp.mean(x * x, axis=-1, keepdims=True) + eps_norm)
    normed = (x * scale * gain[...]).astype(bf16)
    attn_input[...] = normed
    projected = jnp.concatenate([dot(normed, block) for block in weights], axis=1)
    first = lax.broadcasted_iota(jnp.int32, (x.shape[0], 128), 1) < 64
    for chunk in (*range(QUERY_WIDTH // 128, QKV // 128), *range(QUERY_WIDTH // 128)):
        u = projected[:, chunk * 128 : chunk * 128 + 128]
        at = chunk * 128 - QUERY_WIDTH
        if at < 0:
            turned = rotate(u, cosine[...], sine[...]) * HEAD_SIZE ** (-0.5)
            queries[:, chunk * 128 : chunk * 128 + 128] = turned.astype(bf16)
        elif at + 128 <= PAIR_WIDTH:
            pairs[:, at : at + 128] = rotate(u, cosine[...], sine[...]).astype(bf16)
        elif at < PAIR_WIDTH:
            turned = jnp.where(first, rotate(u, cosine[...], sine[...]), u)
            pairs[:, at : at + 128] = turned.astype(bf16)
        else:
            pairs[:, at : at + 128] = u.astype(bf16)


def project_kernel(tokens, gain, weight, *refs):
    project(tokens, gain, [weight[j] for j in range(4)], *refs)


def head(values, index):
    return values[:, index * HEAD_SIZE : (index + 1) * HEAD_SIZE]


def attend_group(group, seen, queries, pairs, exact, logs):
    keys = head(pairs, group)
    values = head(pairs, KEY_VALUE_HEADS + group)
    for member in range(GROUP):
        at = group * GROUP + member
        scores = jnp.where(seen, dot(head(queries, at), keys, 1, 1), score_after_mask)
        top = jnp.max(scores, axis=-1, keepdims=True)
        powers = jnp.exp(scores - top)
        total = jnp.sum(powers, axis=-1, keepdims=True)
        exact[:, at * 64 : at * 64 + 64] = dot(powers.astype(bf16), values) / total
        logs[:, at : at + 1] = top + jnp.log(total)


def close_attention(tokens, weights, gain, mixed, exact, resid, mlp_input):
    mixed[...] = exact[...].astype(bf16)
    branch = jnp.concatenate([dot(mixed[...], block) for block in weights], axis=1)
    total = tokens[...].astype(f32) + branch
    resid[...] = total
    scale = lax.rsqrt(jnp.mean(total * total, axis=-1, keepdims=True) + eps_norm)
    mlp_input[...] = (total * scale * gain[...]).astype(bf16)


def attend_kernel(
    queries, pairs, tokens, weight, gain, query_at, key_at, prefix, mixed, exact, logs, resid, mlp_input
):
    seen = (key_at[...] <= query_at[...]) | (key_at[...] < prefix[0])
    for group in range(KEY_VALUE_HEADS):
        attend_group(group, seen, queries, pairs, exact, logs)
    close_attention(tokens, [weight[j] for j in range(4)], gain, mixed, exact, resid, mlp_input)


def back_norm(grad_out, source, gain):
    scale = lax.rsqrt(jnp.mean(source * source, axis=-1, keepdims=True) + eps_norm)
    normed = source * scale
    scaled = grad_out * gain
    inner = jnp.mean(scaled * normed, axis=-1, keepdims=True)
    return jnp.sum(grad_out * normed, axis=0, keepdims=True), scale * (scaled - normed * inner)


def branch_back(
    d_mlp, resid, cotangent, gain, weight, mixed, exact, d_resid, d_mixed, out_grad, gain_grad, deltas
):
    gain_sum, d_normed = back_norm(d_mlp, resid[...], gain[...])
    gain_grad[...] = gain_sum
    total = cotangent[...].astype(f32) + d_normed
    d_resid[...] = total
    width = weight.shape[2]
    d_branch = total.astype(bf16)
    back = None
    for j in range(4):
        part = d_branch[:, j * width : (j + 1) * width]
        out_grad[j] = dot(mixed[...], part, 0, 0).astype(bf16)
        term = dot(part, weight[j], 1, 1)
        back = term if back is None else back + term
    d_mixed[...] = back.astype(bf16)
    product = d_mixed[...].astype(f32) * exact[...]
    which = lax.broadcasted_iota(jnp.int32, (32, QUERY_WIDTH), 1) // HEAD_SIZE
    ones = (which == lax.broadcasted_iota(jnp.int32, (32, QUERY_WIDTH), 0)).astype(f32)
    deltas[...] = dot(ones, product, 1, 1, precision=lax.Precision.HIGHEST)


def branch_back_kernel(d_mlp, *refs):
    branch_back(d_mlp[...], *refs)


def attend_back_group(group, seen, queries, pairs, d_mixed, logs, deltas, d_queries, d_pairs):
    keys = head(pairs, group)
    values = head(pairs, KEY_VALUE_HEADS + group)
    turned_keys = keys.T
    d_keys = d_values = None
    for member in range(GROUP):
        at = group * GROUP + member
        mine = head(queries, at)
        back = head(d_mixed, at)
        scores = jnp.where(seen, dot(keys, mine, 1, 1), score_after_mask)
        probs = jnp.exp(scores - logs[at : at + 1, :])
        d_probs = dot(values, back, 1, 1)
        d_scores = (probs * (d_probs - deltas[at : at + 1, :])).astype(bf16)
        turned = dot(turned_keys, d_scores) * HEAD_SIZE ** (-0.5)
        d_queries[:, at * 64 : at * 64 + 64] = turned.T
        key_term = dot(d_scores, mine)
        value_term = dot(probs.astype(bf16), back)
        d_keys = key_term if d_keys is None else d_keys + key_term
        d_values = value_term if d_values is None else d_values + value_term
    at = group * 64
    d_pairs[:, at : at + 64] = d_keys.astype(bf16)
    at += PAIR_WIDTH
    d_pairs[:, at : at + 64] = d_values.astype(bf16)


def attend_back_kernel(
    queries, pairs, d_mixed, logs, deltas, query_at, key_at, prefix, d_queries, d_pairs
):
    seen = (key_at[...] <= query_at[...]) | (key_at[...] < prefix[0])
    for group in range(KEY_VALUE_HEADS):
        attend_back_group(group, seen, queries, pairs, d_mixed, logs, deltas, d_queries, d_pairs)


def unproject(d_queries, d_pairs, cosine, sine):
    rows = d_queries.shape[0]
    first = lax.broadcasted_iota(jnp.int32, (rows, 128), 1) < 64
    chunks = []
    for chunk in range(QKV // 128):
        at = chunk * 128 - QUERY_WIDTH
        if at < 0:
            chunks.append(rotate(d_queries[:, chunk * 128 : chunk * 128 + 128], cosine[...], -sine[...]))
            continue
        u = d_pairs[:, at : at + 128]
        if at + 128 <= PAIR_WIDTH:
            u = rotate(u, cosine[...], -sine[...])
        elif at < PAIR_WIDTH:
            u = jnp.where(first, rotate(u, cosine[...], -sine[...]), u)
        chunks.append(u)
    return jnp.concatenate([u.astype(bf16) for u in chunks], axis=1)


def project_back_kernel(
    d_queries, d_pairs, attn_input, tokens, d_resid, gain, weight, cosine, sine, tokens_grad, qkv_grad, gain_grad
):
    d_projected = unproject(d_queries, d_pairs, cosine, sine)
    width = weight.shape[2]
    back = None
    for j in range(4):
        part = d_projected[:, j * width : (j + 1) * width]
        qkv_grad[j] = dot(attn_input[...], part, 0, 0).astype(bf16)
        term = dot(part, weight[j], 1, 1)
        back = term if back is None else back + term
    gain_sum, d_normed = back_norm(back, tokens[...].astype(f32), gain[...])
    gain_grad[...] = gain_sum
    tokens_grad[...] = d_resid[...] + d_normed


class Links:
    def __init__(self, sent, got):
        self.sent, self.got, self.copies = sent, got, []

    def send(self, source, target, peer):
        slot = len(self.copies)
        copy = pltpu.make_async_remote_copy(
            src_ref=source,
            dst_ref=target,
            send_sem=self.sent.at[slot],
            recv_sem=self.got.at[slot],
            device_id=peer,
            device_id_type=MESH,
        )
        copy.start()
        self.copies.append(copy)
        return copy

    def finish(self):
        for copy in self.copies:
            copy.wait_send()


class Moves:
    def __init__(self, sems):
        self.sems, self.copies, self.seen = sems, [], set()

    def start(self, source, target):
        slot = len(self.copies)
        copy = pltpu.make_async_copy(source, target, self.sems.at[slot])
        copy.start()
        self.copies.append(copy)
        return slot

    def wait(self, *slots):
        for slot in slots:
            if slot not in self.seen:
                self.seen.add(slot)
                self.copies[slot].wait()

    def finish(self):
        self.wait(*range(len(self.copies)))


class Peers:
    def __init__(self):
        z, x, y, c = place_of()
        self.z, self.x, self.y, self.c = z, x, y, c
        dp, seq = 2 * z + x, 2 * y + c
        self.by_x = (2 * z + 1 - x, seq)
        self.by_y = (dp, 2 * (1 - y) + c)
        self.by_c = (dp, 2 * y + 1 - c)
        self.by_z = {k: (2 * self.line(k) + x, seq) for k in range(1, lines)}

    def line(self, steps):
        return lax.rem(self.z + steps, lines)

    def greet(self):
        greet([self.by_x, self.by_y, self.by_c] + [self.by_z[k] for k in range(1, lines)])


STEPS = (1, 3, 2, 0)


class RowSum:
    def __init__(self, peers, links, partial, arrived, passed, last):
        self.peers, self.links, self.partial = peers, links, partial
        self.arrived, self.passed, self.last = arrived, passed, last
        self.rows = partial.shape[0] // 4
        rows = self.rows
        self.far = links.send(
            partial.at[pl.ds(3 * rows, rows)], arrived.at[pl.ds(rows, rows)], peers.by_c
        )
        self.near = links.send(
            partial.at[pl.ds(2 * rows, rows)], arrived.at[pl.ds(0, rows)], peers.by_c
        )

    def cross(self, across):
        rows = self.rows
        self.far.wait_recv()
        total = across[...].astype(f32) + self.arrived[rows:, :].astype(f32)
        self.passed[...] = total.astype(bf16)
        self.over = self.links.send(self.passed, self.last, self.peers.by_y)

    def total(self, own):
        self.near.wait_recv()
        self.over.wait_recv()
        return (
            own[...].astype(f32)
            + self.arrived[: self.rows, :].astype(f32)
            + self.last[...].astype(f32)
        )


class BlockSum:
    def __init__(self, peers, links, moves, gradient, own, x_in, z_out, z_in):
        self.peers, self.links, self.moves = peers, links, moves
        self.gradient, self.own, self.x_in, self.z_out, self.z_in = gradient, own, x_in, z_out, z_in
        self.arriving, self.slots, self.final, self.kept = {}, {}, {}, None
        for at, k in enumerate(STEPS):
            block = 2 * peers.line(k) + peers.x
            self.slots[k] = [moves.start(gradient(block), own.at[at])]

    def taken(self, arrived):
        for at, k in enumerate(STEPS):
            self.slots[k].append(self.moves.start(arrived.at[self.peers.line(k)], self.x_in.at[at]))

    def open(self, k):
        at = STEPS.index(k)
        theirs = 2 * self.peers.line(k) + 1 - self.peers.x
        self.arriving[k] = self.links.send(
            self.gradient(theirs), self.x_in.at[at], self.peers.by_x
        )

    def sum_x(self, k):
        at = STEPS.index(k)
        self.moves.wait(*self.slots[k])
        if k in self.arriving:
            self.arriving[k].wait_recv()
        return self.own[at].astype(f32) + self.x_in[at].astype(f32)

    def step(self, k):
        at = STEPS.index(k)
        total = self.sum_x(k)
        if k:
            self.z_out[at] = total.astype(bf16)
            self.final[k] = self.links.send(self.z_out.at[at], self.z_in.at[at], self.peers.by_z[k])
        else:
            self.kept = total

    def total(self):
        total = self.kept
        for at, k in enumerate(STEPS[:-1]):
            self.final[k].wait_recv()
            total = total + self.z_in[at].astype(f32)
        return total


class OwnerSum:
    def __init__(self, peers, links, buffers, own):
        self.peers, self.links, self.own = peers, links, own
        (self.c_in, self.sums, self.y_in, self.x_in, self.x_out, self.y_out) = buffers[:6]
        (self.x_last, self.y_last, self.keep, self.z_out, self.z_in) = buffers[6:]
        self.half = self.sums.shape[3] // 2
        self.over, self.one, self.two, self.final = {}, {}, {}, {}

    def hand(self, source, y_side):
        self.over[y_side] = self.links.send(source, self.c_in.at[y_side], self.peers.by_c)

    def chip(self, y_side):
        self.over[y_side].wait_recv()
        for line in range(lines):
            for side in range(2):
                self.sums[y_side, line, side] = (
                    self.own(y_side, line, side).astype(f32)
                    + self.c_in[y_side, line, side].astype(f32)
                ).astype(bf16)

    def open(self, k):
        p, half = self.peers, self.half
        line, at = p.line(k), STEPS.index(k)
        self.one[k] = (
            self.links.send(
                self.sums.at[1 - p.y, line, :, pl.ds(0, half)], self.y_in.at[at], p.by_y
            ),
            self.links.send(
                self.sums.at[:, line, 1 - p.x, pl.ds(half, half)], self.x_in.at[at], p.by_x
            ),
        )

    def pass_on(self, k):
        p, half = self.peers, self.half
        line, at = p.line(k), STEPS.index(k)
        by_y, by_x = self.one[k]

        def add_up(mine, arrived):
            return mine.astype(f32) + arrived.astype(f32)

        by_y.wait_recv()
        theirs = add_up(self.sums[p.y, line, 1 - p.x, pl.ds(0, half)], self.y_in[at, 1 - p.x])
        self.x_out[at] = theirs.astype(bf16)
        first = self.links.send(self.x_out.at[at], self.x_last.at[at], p.by_x)
        mine = add_up(self.sums[p.y, line, p.x, pl.ds(0, half)], self.y_in[at, p.x])
        self.keep[at, 0:half] = mine
        by_x.wait_recv()
        theirs = add_up(self.sums[1 - p.y, line, p.x, pl.ds(half, half)], self.x_in[at, 1 - p.y])
        self.y_out[at] = theirs.astype(bf16)
        second = self.links.send(self.y_out.at[at], self.y_last.at[at], p.by_y)
        mine = add_up(self.sums[p.y, line, p.x, pl.ds(half, half)], self.x_in[at, p.y])
        self.keep[at, half : 2 * half] = mine
        self.two[k] = first, second

    def close(self, k):
        at, half = STEPS.index(k), self.half
        for copy in self.two[k]:
            copy.wait_recv()
        self.keep[at, 0:half] = self.keep[at, 0:half] + self.x_last[at].astype(f32)
        self.keep[at, half : 2 * half] = self.keep[at, half : 2 * half] + self.y_last[at].astype(f32)
        if k:
            self.z_out[at] = self.keep[at].astype(bf16)
            self.final[k] = self.links.send(self.z_out.at[at], self.z_in.at[at], self.peers.by_z[k])

    def total(self):
        total = self.keep[STEPS.index(0)]
        for at, k in enumerate(STEPS[:-1]):
            self.final[k].wait_recv()
            total = total + self.z_in[at].astype(f32)
        return total


def owner_buffers(rows, width):
    half = rows // 2
    return [
        pltpu.VMEM(shape, kind)
        for shape, kind in (
            ((2, lines, 2, rows, width), bf16),
            ((2, lines, 2, rows, width), bf16),
            ((lines, 2, half, width), bf16),
            ((lines, 2, half, width), bf16),
            ((lines, half, width), bf16),
            ((lines, half, width), bf16),
            ((lines, half, width), bf16),
            ((lines, half, width), bf16),
            ((lines, rows, width), f32),
            ((lines, rows, width), bf16),
            ((lines, rows, width), bf16),
        )
    ]


def front_kernel(
    qkv_shard, out_shard, gu_shard, down_shard, cotangent, tokens, attn_gain, mlp_gain, cosine, sine,
    query_at, key_at, prefix,
    qkv_far, out_far, gu_far, down_far, attn_input, queries, pairs_far, mixed, exact, logs, resid, mlp_rows, cot_rows,
    qkv_full, out_full, pairs, mlp_input, local_sem, sent, got,
):
    peers = Peers()
    links, moves = Links(sent, got), Moves(local_sem)
    z, x, y, c = peers.z, peers.x, peers.y, peers.c
    mine, other = 2 * y + c, 2 * (1 - y) + c
    rows = tokens.shape[0]
    half = qkv_shard.shape[0] // 2
    shards, wholes = (qkv_shard, out_shard), (qkv_full, out_full)
    ffn_shards, ffn_wholes = (gu_shard, down_shard), (gu_far, down_far)
    own = 2 * z + x
    local = [moves.start(s, w.at[mine, own]) for s, w in zip(shards, wholes)]
    local += [moves.start(s, w.at[own]) for s, w in zip(ffn_shards, ffn_wholes)]
    local.append(moves.start(cotangent, cot_rows.at[pl.ds(0, rows)]))
    peers.greet()
    order = (0, 1, 3, 2)
    came = {}
    for array in range(2):
        for k in order[1:]:
            came[array, "z", k] = links.send(
                shards[array], wholes[array].at[mine, own], peers.by_z[k]
            )
    for k in order[1:]:
        for array in range(2):
            came["ffn", array, "z", k] = links.send(
                ffn_shards[array], ffn_wholes[array].at[own], peers.by_z[k]
            )

    def source_line(k):
        return lax.rem(z - k + lines, lines)

    def first(array, k):
        block = 2 * source_line(k) + x
        if k:
            came[array, "z", k].wait_recv()
        view = wholes[array].at[mine, block]
        origin = view if k else shards[array]
        came[array, "x", k] = links.send(origin, view, peers.by_x)
        came[array, "y", k] = links.send(origin, view, peers.by_y)
        came[array, "c", k, 0] = links.send(origin, view, peers.by_c)

    def second(array, k):
        side, line = 2 * source_line(k) + 1 - x, 2 * source_line(k) + x
        came[array, "x", k].wait_recv()
        view = wholes[array].at[mine, side]
        upper = view if array else view.at[pl.ds(0, half)]
        came[array, "xy", k] = links.send(upper, upper, peers.by_y)
        came[array, "c", k, 1] = links.send(view, view, peers.by_c)
        came[array, "y", k].wait_recv()
        view = wholes[array].at[other, line]
        if not array:
            lower = view.at[pl.ds(half, half)]
            came[array, "yx", k] = links.send(lower, lower, peers.by_x)
        came[array, "c", k, 2] = links.send(view, view, peers.by_c)

    def third(array, k):
        view = wholes[array].at[other, 2 * source_line(k) + 1 - x]
        came[array, "xy", k].wait_recv()
        if not array:
            came[array, "yx", k].wait_recv()
        came[array, "c", k, 3] = links.send(view, view, peers.by_c)

    def ffn(k):
        for array in range(2):
            if k:
                came["ffn", array, "z", k].wait_recv()
            view = ffn_wholes[array].at[2 * source_line(k) + x]
            origin = view if k else ffn_shards[array]
            came["ffn", array, "x", k] = links.send(origin, view, peers.by_x)

    def complete(array):
        for k in order:
            for part in range(4):
                came[array, "c", k, part].wait_recv()
        moves.wait(local[array])

    for at in range(6):
        if at < 4:
            first(0, order[at])
        if 1 <= at <= 4:
            second(0, order[at - 1])
        if at >= 2:
            third(0, order[at - 2])
    ffn(0)
    complete(0)
    flat_qkv = [qkv_full[j].reshape(-1, qkv_full.shape[3]) for j in range(4)]
    project(
        tokens, attn_gain, flat_qkv, cosine, sine, attn_input, queries, pairs.at[pl.ds(0, rows)]
    )
    pair_y = links.send(pairs.at[pl.ds(0, rows)], pairs.at[pl.ds(rows, rows)], peers.by_y)
    pair_c = links.send(pairs.at[pl.ds(0, rows)], pairs.at[pl.ds(2 * rows, rows)], peers.by_c)
    moves.start(qkv_full, qkv_far)
    for k in order:
        first(1, k)
    ffn(1)
    pair_y.wait_recv()
    pair_yc = links.send(pairs.at[pl.ds(rows, rows)], pairs.at[pl.ds(3 * rows, rows)], peers.by_c)
    pair_c.wait_recv()
    pair_yc.wait_recv()
    moves.start(pairs, pairs_far)
    seen = (key_at[...] <= query_at[...]) | (key_at[...] < prefix[0])
    attend_group(0, seen, queries, pairs, exact, logs)
    for k in order:
        second(1, k)
    cot_y = links.send(cotangent, cot_rows.at[pl.ds(rows, rows)], peers.by_y)
    cot_c = links.send(cotangent, cot_rows.at[pl.ds(2 * rows, rows)], peers.by_c)
    attend_group(1, seen, queries, pairs, exact, logs)
    attend_group(2, seen, queries, pairs, exact, logs)
    ffn(3)
    for k in order:
        third(1, k)
    attend_group(3, seen, queries, pairs, exact, logs)
    attend_group(4, seen, queries, pairs, exact, logs)
    complete(1)
    moves.start(out_full, out_far)
    flat_out = [out_full[j].reshape(-1, out_full.shape[3]) for j in range(4)]
    close_attention(tokens, flat_out, mlp_gain, mixed, exact, resid, mlp_input)
    mlp_y = links.send(mlp_input, mlp_rows.at[pl.ds(rows, rows)], peers.by_y)
    mlp_c = links.send(mlp_input, mlp_rows.at[pl.ds(2 * rows, rows)], peers.by_c)
    moves.start(mlp_input, mlp_rows.at[pl.ds(0, rows)])
    cot_y.wait_recv()
    view = cot_rows.at[pl.ds(rows, rows)]
    cot_yc = links.send(view, cot_rows.at[pl.ds(3 * rows, rows)], peers.by_c)
    ffn(2)
    mlp_y.wait_recv()
    view = mlp_rows.at[pl.ds(rows, rows)]
    mlp_yc = links.send(view, mlp_rows.at[pl.ds(3 * rows, rows)], peers.by_c)
    for copy in (cot_c, cot_yc, mlp_c, mlp_yc):
        copy.wait_recv()
    for k in order:
        for array in range(2):
            came["ffn", array, "x", k].wait_recv()
    links.finish()
    moves.finish()


def back_one_kernel(
    branch_part, down, down_taken, gate_up, resid_far, cotangent_far, weight_far, mixed_far, exact_far,
    queries_far, pairs_far, d_mlp, gain, logs, query_at, key_at, prefix,
    layer_out, d_resid, out_grad_far, gain_grad, d_queries, d_kv, down_sum, gate_sum, up_lines,
    branch_own, resid, cotangent, weight, mixed, exact, queries, pairs,
    branch_in, branch_out, branch_last, pair_in, pair_out, pair_last,
    d_mixed, deltas, d_pairs, out_grad, own_blocks, x_in, z_out, z_in, local_sem, sent, got,
):
    peers = Peers()
    links, moves = Links(sent, got), Moves(local_sem)
    rows, quarter = resid.shape[0], down.shape[2]
    own_branch = moves.start(branch_part.at[pl.ds(0, 2 * rows)], branch_own)
    ready = {}
    for name, source, target in (
        ("resid", resid_far, resid),
        ("cotangent", cotangent_far, cotangent),
        ("weight", weight_far, weight),
        ("mixed", mixed_far, mixed),
        ("exact", exact_far, exact),
        ("queries", queries_far, queries),
        ("pairs", pairs_far, pairs),
    ):
        ready[name] = moves.start(source, target)
    peers.greet()
    sums = [
        BlockSum(peers, links, moves, gradient, *(b.at[i] for b in (own_blocks, x_in, z_out, z_in)))
        for i, gradient in enumerate(
            (
                lambda block: down.at[block],
                lambda block: gate_up.at[block, :, pl.ds(0, quarter)],
                lambda block: gate_up.at[block, :, pl.ds(quarter, quarter)],
            )
        )
    ]
    sums[0].taken(down_taken)
    for block in sums[1:]:
        for k in STEPS:
            block.open(k)
    branch_sum = RowSum(peers, links, branch_part, branch_in, branch_out, branch_last)
    pending = [(i, k) for i in (1, 2) for k in STEPS]

    def pump(count):
        for _ in range(count):
            if pending:
                i, k = pending.pop(0)
                if i == 1:
                    sums[i].step(k)
                    continue
                at = STEPS.index(k)
                z_out[2, at] = sums[i].sum_x(k).astype(bf16)
                moves.start(z_out.at[2, at], up_lines.at[at])

    moves.wait(own_branch)
    branch_sum.cross(branch_own.at[pl.ds(rows, rows)])
    for k in STEPS:
        sums[0].step(k)
    moves.wait(*(ready[n] for n in ("resid", "cotangent", "weight", "mixed", "exact")))
    branch_back(
        d_mlp[...], resid, cotangent, gain, weight, mixed, exact, d_resid, d_mixed, out_grad, gain_grad, deltas
    )
    flush = moves.start(out_grad, out_grad_far)
    pump(2)
    moves.wait(ready["queries"], ready["pairs"])
    seen = (key_at[...] <= query_at[...]) | (key_at[...] < prefix[0])
    for group in range(KEY_VALUE_HEADS):
        attend_back_group(group, seen, queries, pairs, d_mixed, logs, deltas, d_queries, d_pairs)
        if group in (0, 2, 4):
            pump(1)
    pair_sum = RowSum(peers, links, d_pairs, pair_in, pair_out, pair_last)
    pair_sum.cross(d_pairs.at[pl.ds(rows, rows)])
    layer_out[...] = (
        resid[...] + branch_sum.total(branch_own.at[pl.ds(0, rows)]).astype(bf16).astype(f32)
    ).astype(bf16)
    pump(8)
    d_kv[...] = pair_sum.total(d_pairs.at[pl.ds(0, rows)])
    down_sum[...] = sums[0].total()
    gate_sum[...] = sums[1].total()
    links.finish()
    moves.finish()


def back_two_kernel(
    up_lines, out_grad, weight_far, d_queries, d_kv, attn_input, tokens, d_resid, gain, cosine, sine, gain_mlp,
    tokens_grad, gains_sum, up_sum, out_sum, qkv_sum,
    weight, out_own, qkv_grad, up_own, z_in,
    gain_own, gain_c, gain_one, gain_y, gain_two, gain_x, gain_z, local_sem, sent, got, *buffers,
):
    peers = Peers()
    links, moves = Links(sent, got), Moves(local_sem)
    own_out = [moves.start(out_grad.at[2 * side + peers.c], out_own.at[side]) for side in range(2)]
    own_up = moves.start(up_lines.at[STEPS.index(0)], up_own)
    weight_in = moves.start(weight_far, weight)
    out_total = OwnerSum(peers, links, buffers[:11], lambda s, line, side: out_own[s, line, side])
    qkv_total = OwnerSum(
        peers, links, buffers[11:], lambda s, line, side: qkv_grad[2 * s + peers.c, line, side]
    )
    peers.greet()
    for side in range(2):
        out_total.hand(out_grad.at[2 * side + 1 - peers.c], side)
    up_copies = [
        links.send(up_lines.at[at], z_in.at[at], peers.by_z[k]) for at, k in enumerate(STEPS[:-1])
    ]
    d_projected = unproject(d_queries, d_kv, cosine, sine)
    moves.wait(*own_out)
    width = weight.shape[2]
    for j in range(4):
        part = d_projected[:, j * width : (j + 1) * width]
        outer = dot(attn_input[...], part, 0, 0).astype(bf16)
        qkv_grad[j] = outer.reshape(qkv_grad.shape[1:])
        if j % 2:
            qkv_total.hand(qkv_grad.at[j - peers.c], j // 2)
        else:
            out_total.chip(j // 2)
        if j == 2:
            for k in STEPS:
                out_total.open(k)
    for side in range(2):
        qkv_total.chip(side)
    for k in STEPS:
        qkv_total.open(k)
    moves.wait(weight_in)
    back = None
    for j in range(4):
        part = d_projected[:, j * width : (j + 1) * width]
        term = dot(part, weight[j], 1, 1)
        back = term if back is None else back + term
    gain_sum, d_normed = back_norm(back, tokens[...].astype(f32), gain[...])
    gain_own[...] = jnp.concatenate([gain_sum, gain_mlp[...]], axis=0)
    gain_copy = links.send(gain_own, gain_c, peers.by_c)
    for k in STEPS:
        out_total.pass_on(k)
    tokens_grad[...] = d_resid[...] + d_normed
    gain_copy.wait_recv()
    gain_one[...] = gain_own[...] + gain_c[...]
    gain_copy = links.send(gain_one, gain_y, peers.by_y)
    for k in STEPS:
        qkv_total.pass_on(k)
    gain_copy.wait_recv()
    gain_two[...] = gain_one[...] + gain_y[...]
    gain_copy = links.send(gain_two, gain_x, peers.by_x)
    for k in STEPS:
        out_total.close(k)
    gain_copy.wait_recv()
    gain_z[peers.z] = gain_two[...] + gain_x[...]
    gain_copies = [
        links.send(gain_z.at[peers.z], gain_z.at[peers.z], peers.by_z[k]) for k in range(1, lines)
    ]
    for k in STEPS:
        qkv_total.close(k)
    moves.wait(own_up)
    up_total = up_own[...].astype(f32)
    for at, copy in enumerate(up_copies):
        copy.wait_recv()
        up_total = up_total + z_in[at].astype(f32)
    up_sum[...] = up_total
    out_sum[...] = out_total.total()
    for copy in gain_copies:
        copy.wait_recv()
    gains_sum[...] = ((gain_z[0] + gain_z[1]) + gain_z[2]) + gain_z[3]
    qkv_sum[...] = qkv_total.total()
    links.finish()
    moves.finish()


def remote_call(kernel, name, number, outs, scratch, *args, local=16, remote=64, smem=0, flops=0):
    places = {False: spec(), True: spec(pl.ANY)}
    return pl.pallas_call(
        kernel,
        out_shape=[jax.ShapeDtypeStruct(s, k) for s, k, _ in outs],
        in_specs=[places[far] for _, far in args[: len(args) - smem]] + [spec(pltpu.SMEM)] * smem,
        out_specs=[places[far] for _, _, far in outs],
        scratch_shapes=scratch[0]
        + [
            pltpu.SemaphoreType.DMA((local,)),
            pltpu.SemaphoreType.DMA((remote,)),
            pltpu.SemaphoreType.DMA((remote,)),
        ]
        + scratch[1],
        compiler_params=pltpu.CompilerParams(
            collective_id=number, has_side_effects=True, vmem_limit_bytes=62 * 2**20
        ),
        cost_estimate=pl.CostEstimate(flops=flops, bytes_accessed=2**24, transcendentals=0),
        name=name,
    )(*(array for array, _ in args))


def vmem_like(array):
    return pltpu.VMEM(array.shape, array.dtype)


def adam_update(master, moment, square, gradient, step_rate, decay):
    moment_next = beta_one * moment + (1.0 - beta_one) * gradient
    square_next = beta_two * square + (1.0 - beta_two) * gradient * gradient
    master_next = master - step_rate * (
        moment_next / (jnp.sqrt(square_next) + eps_adam) + decay * master
    )
    return (master_next, moment_next, square_next)


def on_device(
    tokens,
    cotangent,
    prefix_len,
    gains_master,
    gains_moment,
    gains_square,
    qkv_master,
    qkv_moment,
    qkv_square,
    out_master,
    out_moment,
    out_square,
    gu_master,
    gu_moment,
    gu_square,
    down_master,
    down_moment,
    down_square,
):
    seq_count = lax.axis_size("seq")
    dp_count = lax.axis_size("dp")
    seq_place = lax.axis_index("seq")
    near = dp_count == 2 * lines and seq_count == 4
    grid = Grid() if near else None
    plain = Plain()
    token_rows = tokens.shape[0]
    quarter = FF // seq_count
    shard_rows = gu_master.shape[0]
    qkv_b = qkv_master.astype(bf16)
    out_b = out_master.astype(bf16)
    gu_b = gu_master.astype(bf16).reshape(shard_rows, 2 * quarter)
    down_b = down_master.astype(bf16).T
    if near:
        key_places = [seq_place ^ step for step in (0, 2, 1, 3)]
    else:
        key_places = list(range(seq_count))
    within = jnp.arange(token_rows, dtype=jnp.int32)
    positions = seq_place * token_rows + within
    key_positions = jnp.concatenate([spot * token_rows + within for spot in key_places])

    cosine_half, sine_half = rope_tables(positions, HEAD_SIZE)
    cosine = jnp.concatenate([cosine_half] * 4, axis=1)
    sine = jnp.concatenate([-sine_half, sine_half] * 2, axis=1)
    shape = (token_rows, D)
    attn_gain, mlp_gain = gains_master[0:1], gains_master[1:2]
    key_count = seq_count * token_rows
    score_flops = 2 * token_rows * key_count * QUERY_WIDTH
    out_flops = 2 * token_rows * D * D
    pair = (token_rows, 2 * PAIR_WIDTH)
    all_pairs = (key_count, 2 * PAIR_WIDTH)
    if near:
        wide = (seq_count, 2 * lines)
        outs = [
            (wide + qkv_b.shape, bf16, True),
            (wide + out_b.shape, bf16, True),
            (wide[1:] + gu_b.shape, bf16, True),
            (wide[1:] + down_b.shape, bf16, True),
            (shape, bf16, False),
            (shape, bf16, False),
            (all_pairs, bf16, True),
            (shape, bf16, False),
            (shape, f32, False),
            ((token_rows, 128), f32, False),
            (shape, f32, False),
            ((key_count, D), bf16, True),
            ((key_count, D), bf16, True),
        ]
        front = remote_call(
            front_kernel,
            "front",
            0,
            outs,
            (
                [pltpu.VMEM(s, k) for s, k, _ in outs[:2]]
                + [pltpu.VMEM(all_pairs, bf16), pltpu.VMEM(shape, bf16)],
                [],
            ),
            *((a, True) for a in (qkv_b, out_b, gu_b, down_b, cotangent)),
            *((a, False) for a in (tokens, attn_gain, mlp_gain, cosine, sine)),
            *((a, False) for a in (positions[:, None], key_positions[None, :], prefix_len)),
            remote=96,
            smem=1,
            flops=2 * token_rows * D * QKV + 2 * score_flops + out_flops,
        )
        qkv_full, out_full, gu_part, down_part, attn_input, queries, kv_rows = front[:7]
        mixed, mixed_exact, logs, resid, mlp_rows, cot_rows = front[7:]
        qkv_full = qkv_full.reshape(seq_count, D, -1)
        out_full = out_full.reshape(seq_count, D, -1)
        gu_part, down_part = gu_part.reshape(D, -1), down_part.reshape(D, -1)
    else:
        qkv_full = plain.gather_attention(qkv_b)
        out_full = plain.gather_attention(out_b)
        gu_part = lax.all_gather(gu_b, "dp", axis=0, tiled=True)
        down_part = lax.all_gather(down_b, "dp", axis=0, tiled=True)
        cot_rows = lax.all_gather(cotangent, "seq", axis=0, tiled=True)
        attn_input, queries, kv_local = local_call(
            project_kernel,
            "project",
            [(shape, bf16), (shape, bf16), (pair, bf16)],
            *(tokens, attn_gain, qkv_full, cosine, sine),
            flops=2 * token_rows * D * QKV,
        )
        kv_rows = lax.all_gather(kv_local, "seq", axis=0, tiled=True)
        mixed, mixed_exact, logs, resid, mlp_input = local_call(
            attend_kernel,
            "attend",
            [(shape, bf16), (shape, f32), ((token_rows, 128), f32), (shape, f32), (shape, bf16)],
            *(queries, kv_rows, tokens, out_full, mlp_gain),
            *(positions[:, None], key_positions[None, :], prefix_len),
            flops=2 * score_flops + out_flops,
            smem=1,
        )
        mlp_rows = lax.all_gather(mlp_input, "seq", axis=0, tiled=True)
    gateup = jnp.dot(mlp_rows, gu_part, preferred_element_type=f32)
    gate = gateup[:, :quarter]
    up_part = gateup[:, quarter:]
    sigmoid_gate = jax.nn.sigmoid(gate)
    silu_gate = gate * sigmoid_gate
    hidden = (silu_gate * up_part).astype(bf16)
    d_hidden = jnp.dot(cot_rows, down_part, preferred_element_type=f32)
    d_gate_b = (d_hidden * up_part * sigmoid_gate * (1.0 + gate * (1.0 - sigmoid_gate))).astype(bf16)
    d_up_b = (d_hidden * silu_gate).astype(bf16)
    d_gateup = jnp.concatenate([d_gate_b, d_up_b], axis=1)

    def contract(left, right, left_axis, right_axis):
        return lax.dot_general(
            left, right, (((left_axis,), (right_axis,)), ((), ())), preferred_element_type=f32
        )

    down_local = contract(cot_rows, hidden, 0, 0).astype(bf16)
    pair_shape = (seq_count, D, out_full.shape[2])
    if near:
        blocks = (2 * lines, shard_rows, quarter)
        lined = (3, lines, shard_rows, quarter)
        down_local = down_local.reshape(blocks)
        down_theirs = pick(down_local.reshape(lines, 2, shard_rows, quarter), 1 - grid.x, 1)
        down_taken = grid.swap_x(down_theirs)
        d_mlp_part = contract(d_gateup, gu_part, 1, 1).astype(bf16)
        half = 2 * token_rows
        d_mlp_chip = d_mlp_part[:half].astype(f32) + grid.swap_c(d_mlp_part[half:]).astype(f32)
        d_mlp_sent = d_mlp_chip[token_rows:].astype(bf16)
        d_mlp_over = grid.swap_y(d_mlp_sent)
        d_mlp_input = d_mlp_chip[:token_rows] + d_mlp_over.astype(f32)
        branch_part = contract(hidden, down_part, 1, 1).astype(bf16)
        gu_local = contract(after(mlp_rows, d_mlp_sent), d_gateup, 0, 0).astype(bf16)
        gu_local = gu_local.reshape(blocks[:2] + (2 * quarter,))
        rows_of = [((2 * token_rows, D), bf16), (shape, bf16), (shape, bf16)]
        pairs_of = [((2 * token_rows, 2 * PAIR_WIDTH), bf16), (pair, bf16), (pair, bf16)]
        far = [resid, cotangent, out_full, mixed, mixed_exact, queries, kv_rows]
        layer_out, d_resid, out_local, gain_mlp, d_queries, d_kv, down_owned, gate_owned, up_lines = remote_call(
            back_one_kernel,
            "back_one",
            1,
            [
                (shape, bf16, False),
                (shape, f32, False),
                (pair_shape, bf16, True),
                ((1, D), f32, False),
                (shape, f32, False),
                (pair, f32, False),
                ((shard_rows, quarter), f32, False),
                ((shard_rows, quarter), f32, False),
                (lined[1:], bf16, True),
            ],
            (
                [pltpu.VMEM((2 * token_rows, D), bf16)]
                + [vmem_like(a) for a in far]
                + [pltpu.VMEM(*s) for s in rows_of + pairs_of]
                + [
                    pltpu.VMEM(shape, bf16),
                    pltpu.VMEM((32, token_rows), f32),
                    pltpu.VMEM(kv_rows.shape, bf16),
                    pltpu.VMEM(pair_shape, bf16),
                ]
                + [pltpu.VMEM(lined, bf16)] * 4,
                [],
            ),
            *((a, True) for a in (branch_part, down_local, down_taken, gu_local, *far)),
            *((a, False) for a in (d_mlp_input, mlp_gain, logs.T, positions[None, :], key_positions[:, None])),
            (prefix_len, False),
            local=40,
            smem=1,
            flops=5 * score_flops + 2 * out_flops,
        )
        line_shape = (seq_count, lines, 2, shard_rows)
        qkv_width, out_width = qkv_full.shape[2], out_full.shape[2]
        tokens_grad, gains_grad, up_owned, out_owned, qkv_owned = remote_call(
            back_two_kernel,
            "back_two",
            2,
            [
                (shape, f32, False),
                ((2, D), f32, False),
                ((shard_rows, quarter), f32, False),
                ((shard_rows, out_width), f32, False),
                ((shard_rows, qkv_width), f32, False),
            ],
            (
                [
                    vmem_like(qkv_full),
                    pltpu.VMEM((2,) + line_shape[1:] + (out_width,), bf16),
                    pltpu.VMEM(line_shape + (qkv_width,), bf16),
                ]
                + [pltpu.VMEM(blocks[1:], bf16), pltpu.VMEM((3,) + blocks[1:], bf16)]
                + [pltpu.VMEM((2, D), f32)] * 6
                + [pltpu.VMEM((lines, 2, D), f32)],
                owner_buffers(shard_rows, out_width) + owner_buffers(shard_rows, qkv_width),
            ),
            *((a, True) for a in (up_lines, out_local.reshape(line_shape + (-1,)), qkv_full)),
            *((a, False) for a in (d_queries, d_kv, attn_input, tokens, d_resid, attn_gain)),
            *((a, False) for a in (cosine, sine, gain_mlp)),
            flops=4 * token_rows * D * QKV,
        )
        gu_owned = with_layout_constraint(
            jnp.stack([gate_owned, up_owned], axis=1), Layout(major_to_minor=(0, 1, 2))
        )
    else:
        d_mlp_part = contract(d_gateup, gu_part, 1, 1).astype(bf16)
        branch_part = contract(hidden, down_part, 1, 1).astype(bf16)
        gu_local = contract(mlp_rows, d_gateup, 0, 0).astype(bf16)

        def scatter(values, axis):
            return lax.psum_scatter(values, axis, scatter_dimension=0, tiled=True).astype(f32)

        d_mlp_input = scatter(d_mlp_part, "seq")
        layer_out = (resid + scatter(branch_part, "seq")).astype(bf16)
        down_owned = scatter(down_local, "dp")
        gu_owned = scatter(gu_local, "dp").reshape(shard_rows, 2, quarter)
        d_resid, d_mixed, out_local, gain_mlp, deltas = local_call(
            branch_back_kernel,
            "branch_back",
            [(shape, f32), (shape, bf16), (pair_shape, bf16), ((1, D), f32), ((32, token_rows), f32)],
            *(d_mlp_input, resid, cotangent, mlp_gain, out_full, mixed, mixed_exact),
            flops=2 * out_flops,
        )
        out_owned = plain.reduce_attention(out_local)
        d_queries, d_pairs = local_call(
            attend_back_kernel,
            "attend_back",
            [(shape, f32), (kv_rows.shape, bf16)],
            *(queries, kv_rows, d_mixed, logs.T, deltas),
            *(positions[None, :], key_positions[:, None], prefix_len),
            flops=5 * score_flops,
            smem=1,
        )
        d_kv = scatter(d_pairs, "seq")
        tokens_grad, qkv_local, gain_attn = local_call(
            project_back_kernel,
            "project_back",
            [(shape, f32), (qkv_full.shape, bf16), ((1, D), f32)],
            *(d_queries, d_kv, attn_input, tokens, d_resid, attn_gain, qkv_full, cosine, sine),
            flops=4 * token_rows * D * QKV,
        )
        qkv_owned = plain.reduce_attention(qkv_local)
        gains_grad = lax.psum(jnp.concatenate([gain_attn, gain_mlp], axis=0), ("dp", "seq"))
    down_owned = down_owned.T
    owned = (qkv_owned, out_owned, gu_owned, down_owned)
    rate_wide = 0.5 * D ** (-0.5)
    rate_out = 0.5 * max(QUERY_WIDTH // 256, 1) ** (-0.5)
    rate_down = 0.5 * FF ** (-0.5)
    gains_new = adam_update(gains_master, gains_moment, gains_square, gains_grad, gain_rate, 0.0)
    qkv_new = adam_update(qkv_master, qkv_moment, qkv_square, owned[0], rate_wide, weight_decay)
    out_new = adam_update(out_master, out_moment, out_square, owned[1], rate_out, weight_decay)
    gu_new = adam_update(gu_master, gu_moment, gu_square, owned[2], rate_wide, weight_decay)
    down_new = adam_update(down_master, down_moment, down_square, owned[3], rate_down, weight_decay)
    return (
        layer_out,
        tokens_grad,
        gains_grad,
        owned[0],
        owned[1],
        owned[2],
        owned[3],
        gains_new[0],
        gains_new[1],
        gains_new[2],
        qkv_new[0],
        qkv_new[1],
        qkv_new[2],
        qkv_new[0].astype(jnp.bfloat16),
        out_new[0],
        out_new[1],
        out_new[2],
        out_new[0].astype(jnp.bfloat16),
        gu_new[0],
        gu_new[1],
        gu_new[2],
        gu_new[0].astype(jnp.bfloat16),
        down_new[0],
        down_new[1],
        down_new[2],
        down_new[0].astype(jnp.bfloat16),
    )


def solution(mesh):
    in_specs = (
        P(("dp", "seq"), None),
        P(("dp", "seq"), None),
        P("dp"),
        P(),
        P(),
        P(),
        P("dp", "seq"),
        P("dp", "seq"),
        P("dp", "seq"),
        P("dp", "seq"),
        P("dp", "seq"),
        P("dp", "seq"),
        P("dp", None, "seq"),
        P("dp", None, "seq"),
        P("dp", None, "seq"),
        P("seq", "dp"),
        P("seq", "dp"),
        P("seq", "dp"),
    )
    out_specs = (
        P(("dp", "seq"), None),
        P(("dp", "seq"), None),
        P(),
        P("dp", "seq"),
        P("dp", "seq"),
        P("dp", None, "seq"),
        P("seq", "dp"),
        P(),
        P(),
        P(),
        P("dp", "seq"),
        P("dp", "seq"),
        P("dp", "seq"),
        P("dp", "seq"),
        P("dp", "seq"),
        P("dp", "seq"),
        P("dp", "seq"),
        P("dp", "seq"),
        P("dp", None, "seq"),
        P("dp", None, "seq"),
        P("dp", None, "seq"),
        P("dp", None, "seq"),
        P("seq", "dp"),
        P("seq", "dp"),
        P("seq", "dp"),
        P("seq", "dp"),
    )
    return jax.shard_map(
        on_device, mesh=mesh, in_specs=in_specs, out_specs=out_specs, check_vma=False
    )
```

```python
import functools
import math

import jax
import jax.numpy as jnp
from jax import lax
from jax.experimental import pallas as pl
from jax.experimental.layout import Layout, with_layout_constraint
from jax.experimental.pallas import tpu as pltpu
from jax.sharding import PartitionSpec as P

D = 1280
QUERY_HEADS = 20
KEY_VALUE_HEADS = 5
HEAD_SIZE = 64
FF = 3584
QUERY_WIDTH = 1280
PAIR_WIDTH = KEY_VALUE_HEADS * HEAD_SIZE
QKV = QUERY_WIDTH + 2 * PAIR_WIDTH
GROUP = QUERY_HEADS // KEY_VALUE_HEADS


eps_norm = 1e-05
eps_adam = 1e-08
rope_base = 10000.0
beta_one = 0.5
beta_two = 0.5
weight_decay = 0.1
score_after_mask = -1e30
gain_rate = 0.3
lines = 4
half_rows = 2


bf16 = jnp.bfloat16
f32 = jnp.float32


def rope_tables(positions, head_width):
    half_width = head_width // 2
    frequency = rope_base ** (-2.0 * jnp.arange(half_width, dtype=jnp.float32) / head_width)
    angles = positions.astype(jnp.float32)[:, None] * frequency[None, :]
    return (jnp.cos(angles), jnp.sin(angles))


def pick(values, index, axis):
    return lax.dynamic_index_in_dim(values, index, axis, keepdims=False)


def add(left, right, kind=jnp.bfloat16):
    return (left.astype(f32) + right.astype(f32)).astype(kind)


def after(values, *others):
    return lax.optimization_barrier((values,) + others)[0]


class Grid:
    def __init__(self):
        dp = lax.axis_index("dp")
        seq = lax.axis_index("seq")
        self.z, self.x, self.y, self.c = dp // 2, dp % 2, seq // 2, seq % 2

    def swap(self, values, axis, bit):
        count = lax.axis_size(axis)
        return lax.ppermute(values, axis, [(i, i ^ bit) for i in range(count)])

    def swap_x(self, values):
        return self.swap(values, "dp", 1)

    def swap_y(self, values):
        return self.swap(values, "seq", 2)

    def swap_c(self, values):
        return self.swap(values, "seq", 1)

    def send_z(self, values, steps):
        pairs = [(i, (i // 2 + steps) % lines * 2 + i % 2) for i in range(2 * lines)]
        return lax.ppermute(values, "dp", pairs)


MESH = pl.DeviceIdType.MESH


def place_of():
    dp = lax.axis_index("dp")
    seq = lax.axis_index("seq")
    return dp // 2, lax.rem(dp, 2), seq // 2, lax.rem(seq, 2)


def greet(peers):
    barrier = pltpu.get_barrier_semaphore()
    for peer in peers:
        pl.semaphore_signal(barrier, inc=1, device_id=peer, device_id_type=MESH)
    pl.semaphore_wait(barrier, len(peers))


class Plain:
    def gather_attention(self, shard):
        blocks = lax.all_gather(shard, ("dp", "seq"), axis=0)
        split = blocks.reshape(lax.axis_size("dp"), lax.axis_size("seq"), *shard.shape)
        return jnp.swapaxes(split, 0, 1).reshape(lax.axis_size("seq"), -1, shard.shape[1])

    def reduce_attention(self, gradient):
        owners, wide, width = gradient.shape
        blocks = gradient.reshape(owners, lax.axis_size("dp"), -1, width)
        blocks = jnp.swapaxes(blocks, 0, 1).reshape(-1, width)
        return lax.psum_scatter(blocks, ("dp", "seq"), scatter_dimension=0, tiled=True).astype(f32)


def spec(space=pltpu.VMEM):
    return pl.BlockSpec(memory_space=space)


def local_call(kernel, name, outs, *args, flops=0, smem=0):
    moved = sum(a.size * a.dtype.itemsize for a in args) + sum(
        math.prod(s) * jnp.dtype(k).itemsize for s, k in outs
    )
    return pl.pallas_call(
        kernel,
        out_shape=[jax.ShapeDtypeStruct(s, k) for s, k in outs],
        in_specs=[spec()] * (len(args) - smem) + [spec(pltpu.SMEM)] * smem,
        out_specs=[spec()] * len(outs),
        compiler_params=pltpu.CompilerParams(vmem_limit_bytes=60 * 2**20),
        cost_estimate=pl.CostEstimate(flops=flops, bytes_accessed=moved, transcendentals=0),
        name=name,
    )(*args)


def dot(left, right, left_axis=1, right_axis=0, **how):
    return lax.dot_general(
        left, right, (((left_axis,), (right_axis,)), ((), ())), preferred_element_type=f32, **how
    )


def rotate(chunk, cosine, sine):
    lane = lax.broadcasted_iota(jnp.int32, chunk.shape, 1)
    swapped = jnp.where(lane % 64 < 32, pltpu.roll(chunk, 96, 1), pltpu.roll(chunk, 32, 1))
    return chunk * cosine + swapped * sine


def project(tokens, gain, weights, cosine, sine, attn_input, queries, pairs):
    x = tokens[...].astype(f32)
    scale = lax.rsqrt(jnp.mean(x * x, axis=-1, keepdims=True) + eps_norm)
    normed = (x * scale * gain[...]).astype(bf16)
    attn_input[...] = normed
    projected = jnp.concatenate([dot(normed, block) for block in weights], axis=1)
    first = lax.broadcasted_iota(jnp.int32, (x.shape[0], 128), 1) < 64
    for chunk in (*range(QUERY_WIDTH // 128, QKV // 128), *range(QUERY_WIDTH // 128)):
        u = projected[:, chunk * 128 : chunk * 128 + 128]
        at = chunk * 128 - QUERY_WIDTH
        if at < 0:
            turned = rotate(u, cosine[...], sine[...]) * HEAD_SIZE ** (-0.5)
            queries[:, chunk * 128 : chunk * 128 + 128] = turned.astype(bf16)
        elif at + 128 <= PAIR_WIDTH:
            pairs[:, at : at + 128] = rotate(u, cosine[...], sine[...]).astype(bf16)
        elif at < PAIR_WIDTH:
            turned = jnp.where(first, rotate(u, cosine[...], sine[...]), u)
            pairs[:, at : at + 128] = turned.astype(bf16)
        else:
            pairs[:, at : at + 128] = u.astype(bf16)


def project_kernel(tokens, gain, weight, *refs):
    project(tokens, gain, [weight[j] for j in range(4)], *refs)


def head(values, index):
    return values[:, index * HEAD_SIZE : (index + 1) * HEAD_SIZE]


def attend_group(group, seen, queries, pairs, exact, logs):
    keys = head(pairs, group)
    values = head(pairs, KEY_VALUE_HEADS + group)
    for member in range(GROUP):
        at = group * GROUP + member
        scores = jnp.where(seen, dot(head(queries, at), keys, 1, 1), score_after_mask)
        top = jnp.max(scores, axis=-1, keepdims=True)
        powers = jnp.exp(scores - top)
        total = jnp.sum(powers, axis=-1, keepdims=True)
        exact[:, at * 64 : at * 64 + 64] = dot(powers.astype(bf16), values) / total
        logs[:, at : at + 1] = top + jnp.log(total)


def close_attention(tokens, weights, gain, mixed, exact, resid, mlp_input):
    mixed[...] = exact[...].astype(bf16)
    branch = jnp.concatenate([dot(mixed[...], block) for block in weights], axis=1)
    total = tokens[...].astype(f32) + branch
    resid[...] = total
    scale = lax.rsqrt(jnp.mean(total * total, axis=-1, keepdims=True) + eps_norm)
    mlp_input[...] = (total * scale * gain[...]).astype(bf16)


def attend_kernel(
    queries, pairs, tokens, weight, gain, query_at, key_at, prefix, mixed, exact, logs, resid, mlp_input
):
    seen = (key_at[...] <= query_at[...]) | (key_at[...] < prefix[0])
    for group in range(KEY_VALUE_HEADS):
        attend_group(group, seen, queries, pairs, exact, logs)
    close_attention(tokens, [weight[j] for j in range(4)], gain, mixed, exact, resid, mlp_input)


def back_norm(grad_out, source, gain):
    scale = lax.rsqrt(jnp.mean(source * source, axis=-1, keepdims=True) + eps_norm)
    normed = source * scale
    scaled = grad_out * gain
    inner = jnp.mean(scaled * normed, axis=-1, keepdims=True)
    return jnp.sum(grad_out * normed, axis=0, keepdims=True), scale * (scaled - normed * inner)


def branch_back(
    d_mlp, resid, cotangent, gain, weight, mixed, exact, d_resid, d_mixed, out_grad, gain_grad, deltas
):
    gain_sum, d_normed = back_norm(d_mlp, resid[...], gain[...])
    gain_grad[...] = gain_sum
    total = cotangent[...].astype(f32) + d_normed
    d_resid[...] = total
    width = weight.shape[2]
    d_branch = total.astype(bf16)
    back = None
    for j in range(4):
        part = d_branch[:, j * width : (j + 1) * width]
        out_grad[j] = dot(mixed[...], part, 0, 0).astype(bf16)
        term = dot(part, weight[j], 1, 1)
        back = term if back is None else back + term
    d_mixed[...] = back.astype(bf16)
    product = d_mixed[...].astype(f32) * exact[...]
    which = lax.broadcasted_iota(jnp.int32, (32, QUERY_WIDTH), 1) // HEAD_SIZE
    ones = (which == lax.broadcasted_iota(jnp.int32, (32, QUERY_WIDTH), 0)).astype(f32)
    deltas[...] = dot(ones, product, 1, 1, precision=lax.Precision.HIGHEST)


def branch_back_kernel(d_mlp, *refs):
    branch_back(d_mlp[...], *refs)


def attend_back_group(group, seen, queries, pairs, d_mixed, logs, deltas, d_queries, d_pairs):
    keys = head(pairs, group)
    values = head(pairs, KEY_VALUE_HEADS + group)
    turned_keys = keys.T
    d_keys = d_values = None
    for member in range(GROUP):
        at = group * GROUP + member
        mine = head(queries, at)
        back = head(d_mixed, at)
        scores = jnp.where(seen, dot(keys, mine, 1, 1), score_after_mask)
        probs = jnp.exp(scores - logs[at : at + 1, :])
        d_probs = dot(values, back, 1, 1)
        d_scores = (probs * (d_probs - deltas[at : at + 1, :])).astype(bf16)
        turned = dot(turned_keys, d_scores) * HEAD_SIZE ** (-0.5)
        d_queries[:, at * 64 : at * 64 + 64] = turned.T
        key_term = dot(d_scores, mine)
        value_term = dot(probs.astype(bf16), back)
        d_keys = key_term if d_keys is None else d_keys + key_term
        d_values = value_term if d_values is None else d_values + value_term
    at = group * 64
    d_pairs[:, at : at + 64] = d_keys.astype(bf16)
    at += PAIR_WIDTH
    d_pairs[:, at : at + 64] = d_values.astype(bf16)


def attend_back_kernel(
    queries, pairs, d_mixed, logs, deltas, query_at, key_at, prefix, d_queries, d_pairs
):
    seen = (key_at[...] <= query_at[...]) | (key_at[...] < prefix[0])
    for group in range(KEY_VALUE_HEADS):
        attend_back_group(group, seen, queries, pairs, d_mixed, logs, deltas, d_queries, d_pairs)


def unproject(d_queries, d_pairs, cosine, sine):
    rows = d_queries.shape[0]
    first = lax.broadcasted_iota(jnp.int32, (rows, 128), 1) < 64
    chunks = []
    for chunk in range(QKV // 128):
        at = chunk * 128 - QUERY_WIDTH
        if at < 0:
            chunks.append(rotate(d_queries[:, chunk * 128 : chunk * 128 + 128], cosine[...], -sine[...]))
            continue
        u = d_pairs[:, at : at + 128]
        if at + 128 <= PAIR_WIDTH:
            u = rotate(u, cosine[...], -sine[...])
        elif at < PAIR_WIDTH:
            u = jnp.where(first, rotate(u, cosine[...], -sine[...]), u)
        chunks.append(u)
    return jnp.concatenate([u.astype(bf16) for u in chunks], axis=1)


def project_back_kernel(
    d_queries, d_pairs, attn_input, tokens, d_resid, gain, weight, cosine, sine, tokens_grad, qkv_grad, gain_grad
):
    d_projected = unproject(d_queries, d_pairs, cosine, sine)
    width = weight.shape[2]
    back = None
    for j in range(4):
        part = d_projected[:, j * width : (j + 1) * width]
        qkv_grad[j] = dot(attn_input[...], part, 0, 0).astype(bf16)
        term = dot(part, weight[j], 1, 1)
        back = term if back is None else back + term
    gain_sum, d_normed = back_norm(back, tokens[...].astype(f32), gain[...])
    gain_grad[...] = gain_sum
    tokens_grad[...] = d_resid[...] + d_normed


class Links:
    def __init__(self, sent, got):
        self.sent, self.got, self.copies, self.some = sent, got, [], []

    def send(self, source, target, peer):
        slot = len(self.copies)
        copy = pltpu.make_async_remote_copy(
            src_ref=source,
            dst_ref=target,
            send_sem=self.sent.at[slot],
            recv_sem=self.got.at[slot],
            device_id=peer,
            device_id_type=MESH,
        )
        copy.start()
        self.copies.append(copy)
        return copy

    def send_if(self, started, source, target, peer):
        slot = len(self.copies)
        copy = pltpu.make_async_remote_copy(
            src_ref=source,
            dst_ref=target,
            send_sem=self.sent.at[slot],
            recv_sem=self.got.at[slot],
            device_id=peer,
            device_id_type=MESH,
        )
        self.copies.append(None)
        self.some.append((started, copy))
        pl.when(started)(copy.start)
        return copy

    def finish(self):
        for copy in self.copies:
            if copy is not None:
                copy.wait_send()
        for started, copy in self.some:
            pl.when(started)(copy.wait_send)


class Moves:
    def __init__(self, sems):
        self.sems, self.copies, self.seen = sems, [], set()

    def start(self, source, target):
        slot = len(self.copies)
        copy = pltpu.make_async_copy(source, target, self.sems.at[slot])
        copy.start()
        self.copies.append(copy)
        return slot

    def wait(self, *slots):
        for slot in slots:
            if slot not in self.seen:
                self.seen.add(slot)
                self.copies[slot].wait()

    def finish(self):
        self.wait(*range(len(self.copies)))


class Peers:
    def __init__(self):
        z, x, y, c = place_of()
        self.z, self.x, self.y, self.c = z, x, y, c
        dp, seq = 2 * z + x, 2 * y + c
        self.by_x = (2 * z + 1 - x, seq)
        self.by_y = (dp, 2 * (1 - y) + c)
        self.by_c = (dp, 2 * y + 1 - c)
        self.by_z = {k: (2 * self.line(k) + x, seq) for k in range(1, lines)}

    def line(self, steps):
        return lax.rem(self.z + steps, lines)

    def greet(self):
        greet([self.by_x, self.by_y, self.by_c] + [self.by_z[k] for k in range(1, lines)])


STEPS = (1, 3, 2, 0)


class RowSum:
    def __init__(self, peers, links, partial, arrived, passed, last):
        self.peers, self.links, self.partial = peers, links, partial
        self.arrived, self.passed, self.last = arrived, passed, last
        self.rows = partial.shape[0] // 4
        rows = self.rows
        self.far = links.send(
            partial.at[pl.ds(3 * rows, rows)], arrived.at[pl.ds(rows, rows)], peers.by_c
        )
        self.near = links.send(
            partial.at[pl.ds(2 * rows, rows)], arrived.at[pl.ds(0, rows)], peers.by_c
        )

    def cross(self, across):
        rows = self.rows
        self.far.wait_recv()
        total = across[...].astype(f32) + self.arrived[rows:, :].astype(f32)
        self.passed[...] = total.astype(bf16)
        self.over = self.links.send(self.passed, self.last, self.peers.by_y)

    def total(self, own):
        self.near.wait_recv()
        self.over.wait_recv()
        return (
            own[...].astype(f32)
            + self.arrived[: self.rows, :].astype(f32)
            + self.last[...].astype(f32)
        )


class BlockSum:
    def __init__(self, peers, links, moves, gradient, own, x_in, z_out, z_in):
        self.peers, self.links, self.moves = peers, links, moves
        self.gradient, self.own, self.x_in, self.z_out, self.z_in = gradient, own, x_in, z_out, z_in
        self.arriving, self.slots, self.final, self.kept = {}, {}, {}, None
        for at, k in enumerate(STEPS):
            block = 2 * peers.line(k) + peers.x
            self.slots[k] = [moves.start(gradient(block), own.at[at])]

    def taken(self, arrived):
        for at, k in enumerate(STEPS):
            self.slots[k].append(self.moves.start(arrived.at[self.peers.line(k)], self.x_in.at[at]))

    def open(self, k):
        at = STEPS.index(k)
        theirs = 2 * self.peers.line(k) + 1 - self.peers.x
        self.arriving[k] = self.links.send(
            self.gradient(theirs), self.x_in.at[at], self.peers.by_x
        )

    def sum_x(self, k):
        at = STEPS.index(k)
        self.moves.wait(*self.slots[k])
        if k in self.arriving:
            self.arriving[k].wait_recv()
        return self.own[at].astype(f32) + self.x_in[at].astype(f32)

    def step(self, k):
        at = STEPS.index(k)
        total = self.sum_x(k)
        if k:
            self.z_out[at] = total.astype(bf16)
            self.final[k] = self.links.send(self.z_out.at[at], self.z_in.at[at], self.peers.by_z[k])
        else:
            self.kept = total

    def total(self):
        total = self.kept
        for at, k in enumerate(STEPS[:-1]):
            self.final[k].wait_recv()
            total = total + self.z_in[at].astype(f32)
        return total


class OwnerSum:
    def __init__(self, peers, links, buffers, own):
        self.peers, self.links, self.own = peers, links, own
        (self.c_in, self.sums, self.y_in, self.x_in, self.x_out, self.y_out) = buffers[:6]
        (self.x_last, self.y_last, self.keep, self.z_out, self.z_in) = buffers[6:]
        self.half = self.sums.shape[3] // 2
        self.over, self.one, self.two, self.final = {}, {}, {}, {}

    def hand(self, source, y_side):
        self.over[y_side] = self.links.send(source, self.c_in.at[y_side], self.peers.by_c)

    def chip(self, y_side):
        self.over[y_side].wait_recv()
        for line in range(lines):
            for side in range(2):
                self.sums[y_side, line, side] = (
                    self.own(y_side, line, side).astype(f32)
                    + self.c_in[y_side, line, side].astype(f32)
                ).astype(bf16)

    def open(self, k):
        p, half = self.peers, self.half
        line, at = p.line(k), STEPS.index(k)
        self.one[k] = (
            self.links.send(
                self.sums.at[1 - p.y, line, :, pl.ds(0, half)], self.y_in.at[at], p.by_y
            ),
            self.links.send(
                self.sums.at[:, line, 1 - p.x, pl.ds(half, half)], self.x_in.at[at], p.by_x
            ),
        )

    def pass_on(self, k):
        p, half = self.peers, self.half
        line, at = p.line(k), STEPS.index(k)
        by_y, by_x = self.one[k]

        def add_up(mine, arrived):
            return mine.astype(f32) + arrived.astype(f32)

        by_y.wait_recv()
        theirs = add_up(self.sums[p.y, line, 1 - p.x, pl.ds(0, half)], self.y_in[at, 1 - p.x])
        self.x_out[at] = theirs.astype(bf16)
        first = self.links.send(self.x_out.at[at], self.x_last.at[at], p.by_x)
        mine = add_up(self.sums[p.y, line, p.x, pl.ds(0, half)], self.y_in[at, p.x])
        self.keep[at, 0:half] = mine
        by_x.wait_recv()
        theirs = add_up(self.sums[1 - p.y, line, p.x, pl.ds(half, half)], self.x_in[at, 1 - p.y])
        self.y_out[at] = theirs.astype(bf16)
        second = self.links.send(self.y_out.at[at], self.y_last.at[at], p.by_y)
        mine = add_up(self.sums[p.y, line, p.x, pl.ds(half, half)], self.x_in[at, p.y])
        self.keep[at, half : 2 * half] = mine
        self.two[k] = first, second

    def close(self, k):
        at, half = STEPS.index(k), self.half
        for copy in self.two[k]:
            copy.wait_recv()
        self.keep[at, 0:half] = self.keep[at, 0:half] + self.x_last[at].astype(f32)
        self.keep[at, half : 2 * half] = self.keep[at, half : 2 * half] + self.y_last[at].astype(f32)
        if k:
            self.z_out[at] = self.keep[at].astype(bf16)
            self.final[k] = self.links.send(self.z_out.at[at], self.z_in.at[at], self.peers.by_z[k])

    def total(self):
        total = self.keep[STEPS.index(0)]
        for at, k in enumerate(STEPS[:-1]):
            self.final[k].wait_recv()
            total = total + self.z_in[at].astype(f32)
        return total


def owner_buffers(rows, width):
    half = rows // 2
    return [
        pltpu.VMEM(shape, kind)
        for shape, kind in (
            ((2, lines, 2, rows, width), bf16),
            ((2, lines, 2, rows, width), bf16),
            ((lines, 2, half, width), bf16),
            ((lines, 2, half, width), bf16),
            ((lines, half, width), bf16),
            ((lines, half, width), bf16),
            ((lines, half, width), bf16),
            ((lines, half, width), bf16),
            ((lines, rows, width), f32),
            ((lines, rows, width), bf16),
            ((lines, rows, width), bf16),
        )
    ]


def front_kernel(
    qkv_shard, out_shard, gu_shard, down_shard, cotangent, tokens, attn_gain, mlp_gain, cosine, sine,
    query_at, key_at, prefix,
    qkv_far, out_far, gu_far, down_far, attn_input, queries, pairs_far, mixed, exact, logs, resid, mlp_rows, cot_rows,
    qkv_full, out_full, pairs, mlp_input, local_sem, sent, got,
):
    peers = Peers()
    links, moves = Links(sent, got), Moves(local_sem)
    z, x, y, c = peers.z, peers.x, peers.y, peers.c
    mine, other = 2 * y + c, 2 * (1 - y) + c
    rows = tokens.shape[0]
    half = qkv_shard.shape[0] // 2
    shards, wholes = (qkv_shard, out_shard), (qkv_full, out_full)
    ffn_shards, ffn_wholes = (gu_shard, down_shard), (gu_far, down_far)
    own = 2 * z + x
    local = [moves.start(s, w.at[mine, own]) for s, w in zip(shards, wholes)]
    local += [moves.start(s, w.at[own]) for s, w in zip(ffn_shards, ffn_wholes)]
    local.append(moves.start(cotangent, cot_rows.at[pl.ds(0, rows)]))
    peers.greet()
    order = (0, 1, 3, 2)
    came = {}

    def relay(steps, way):
        line, beyond = z - way * steps, z + way
        held = (line >= 0) & (line < lines)
        goes = held & (beyond >= 0) & (beyond < lines)
        line = lax.clamp(0, line, lines - 1)
        beyond = lax.clamp(0, beyond, lines - 1)
        beyond = jnp.where(beyond == z, z - way, beyond)
        for array in range(2):
            view = ffn_wholes[array].at[2 * line + x]
            origin = view if steps else ffn_shards[array]
            came["ffn", array, way, steps + 1] = links.send_if(
                goes, origin, view, (2 * beyond + x, mine)
            )

    def relayed(steps, way):
        line = z - way * steps
        held = (line >= 0) & (line < lines)
        line = lax.clamp(0, line, lines - 1)
        for array in range(2):
            pl.when(held)(came["ffn", array, way, steps].wait_recv)
        if steps < lines - 1:
            relay(steps, way)
        for array in range(2):
            view = ffn_wholes[array].at[2 * line + x]
            came["ffn", array, way, steps, "x"] = held, links.send_if(held, view, view, peers.by_x)

    for array in range(2):
        for k in order[1:]:
            came[array, "z", k] = links.send(
                shards[array], wholes[array].at[mine, own], peers.by_z[k]
            )
    for way in (1, -1):
        relay(0, way)

    def source_line(k):
        return lax.rem(z - k + lines, lines)

    def first(array, k):
        block = 2 * source_line(k) + x
        if k:
            came[array, "z", k].wait_recv()
        view = wholes[array].at[mine, block]
        origin = view if k else shards[array]
        came[array, "x", k] = links.send(origin, view, peers.by_x)
        came[array, "y", k] = links.send(origin, view, peers.by_y)
        came[array, "c", k, 0] = links.send(origin, view, peers.by_c)

    def second(array, k):
        side, line = 2 * source_line(k) + 1 - x, 2 * source_line(k) + x
        came[array, "x", k].wait_recv()
        view = wholes[array].at[mine, side]
        upper = view if array else view.at[pl.ds(0, half)]
        came[array, "xy", k] = links.send(upper, upper, peers.by_y)
        came[array, "c", k, 1] = links.send(view, view, peers.by_c)
        came[array, "y", k].wait_recv()
        view = wholes[array].at[other, line]
        if not array:
            lower = view.at[pl.ds(half, half)]
            came[array, "yx", k] = links.send(lower, lower, peers.by_x)
        came[array, "c", k, 2] = links.send(view, view, peers.by_c)

    def third(array, k):
        view = wholes[array].at[other, 2 * source_line(k) + 1 - x]
        came[array, "xy", k].wait_recv()
        if not array:
            came[array, "yx", k].wait_recv()
        came[array, "c", k, 3] = links.send(view, view, peers.by_c)

    def ffn(steps):
        if steps:
            for way in (1, -1):
                relayed(steps, way)
            return
        for array in range(2):
            view = ffn_wholes[array].at[own]
            came["ffn", array, "x"] = links.send(ffn_shards[array], view, peers.by_x)

    def complete(array):
        for k in order:
            for part in range(4):
                came[array, "c", k, part].wait_recv()
        moves.wait(local[array])

    for at in range(6):
        if at < 4:
            first(0, order[at])
        if 1 <= at <= 4:
            second(0, order[at - 1])
        if at >= 2:
            third(0, order[at - 2])
    ffn(0)
    complete(0)
    flat_qkv = [qkv_full[j].reshape(-1, qkv_full.shape[3]) for j in range(4)]
    project(
        tokens, attn_gain, flat_qkv, cosine, sine, attn_input, queries, pairs.at[pl.ds(0, rows)]
    )
    pair_y = links.send(pairs.at[pl.ds(0, rows)], pairs.at[pl.ds(rows, rows)], peers.by_y)
    pair_c = links.send(pairs.at[pl.ds(0, rows)], pairs.at[pl.ds(2 * rows, rows)], peers.by_c)
    moves.start(qkv_full, qkv_far)
    for k in order:
        first(1, k)
    ffn(1)
    pair_y.wait_recv()
    pair_yc = links.send(pairs.at[pl.ds(rows, rows)], pairs.at[pl.ds(3 * rows, rows)], peers.by_c)
    pair_c.wait_recv()
    pair_yc.wait_recv()
    moves.start(pairs, pairs_far)
    seen = (key_at[...] <= query_at[...]) | (key_at[...] < prefix[0])
    attend_group(0, seen, queries, pairs, exact, logs)
    for k in order:
        second(1, k)
    cot_y = links.send(cotangent, cot_rows.at[pl.ds(rows, rows)], peers.by_y)
    cot_c = links.send(cotangent, cot_rows.at[pl.ds(2 * rows, rows)], peers.by_c)
    attend_group(1, seen, queries, pairs, exact, logs)
    attend_group(2, seen, queries, pairs, exact, logs)
    ffn(2)
    for k in order:
        third(1, k)
    attend_group(3, seen, queries, pairs, exact, logs)
    attend_group(4, seen, queries, pairs, exact, logs)
    complete(1)
    moves.start(out_full, out_far)
    flat_out = [out_full[j].reshape(-1, out_full.shape[3]) for j in range(4)]
    close_attention(tokens, flat_out, mlp_gain, mixed, exact, resid, mlp_input)
    mlp_y = links.send(mlp_input, mlp_rows.at[pl.ds(rows, rows)], peers.by_y)
    mlp_c = links.send(mlp_input, mlp_rows.at[pl.ds(2 * rows, rows)], peers.by_c)
    moves.start(mlp_input, mlp_rows.at[pl.ds(0, rows)])
    cot_y.wait_recv()
    view = cot_rows.at[pl.ds(rows, rows)]
    cot_yc = links.send(view, cot_rows.at[pl.ds(3 * rows, rows)], peers.by_c)
    ffn(3)
    mlp_y.wait_recv()
    view = mlp_rows.at[pl.ds(rows, rows)]
    mlp_yc = links.send(view, mlp_rows.at[pl.ds(3 * rows, rows)], peers.by_c)
    for copy in (cot_c, cot_yc, mlp_c, mlp_yc):
        copy.wait_recv()
    for array in range(2):
        came["ffn", array, "x"].wait_recv()
        for steps in range(1, lines):
            for way in (1, -1):
                held, copy = came["ffn", array, way, steps, "x"]
                pl.when(held)(copy.wait_recv)
    links.finish()
    moves.finish()


def back_one_kernel(
    d_mlp_part, branch_part, down, down_taken, gate_up, resid_far, cotangent_far, weight_far, mixed_far, exact_far,
    queries_far, pairs_far, gain, logs, query_at, key_at, prefix,
    layer_out, d_resid, out_grad_far, gain_grad, d_queries, d_kv, down_sum, gate_sum, up_lines,
    d_mlp_own, branch_own, resid, cotangent, weight, mixed, exact, queries, pairs,
    rows_in, rows_out, rows_last, branch_in, branch_out, branch_last, pair_in, pair_out, pair_last,
    d_mixed, deltas, d_pairs, out_grad, own_blocks, x_in, z_out, z_in, local_sem, sent, got,
):
    peers = Peers()
    links, moves = Links(sent, got), Moves(local_sem)
    rows, quarter = resid.shape[0], down.shape[2]
    own_d_mlp = moves.start(d_mlp_part.at[pl.ds(0, 2 * rows)], d_mlp_own)
    own_branch = moves.start(branch_part.at[pl.ds(0, 2 * rows)], branch_own)
    ready = {}
    for name, source, target in (
        ("resid", resid_far, resid),
        ("cotangent", cotangent_far, cotangent),
        ("weight", weight_far, weight),
        ("mixed", mixed_far, mixed),
        ("exact", exact_far, exact),
        ("queries", queries_far, queries),
        ("pairs", pairs_far, pairs),
    ):
        ready[name] = moves.start(source, target)
    peers.greet()
    d_mlp_sum = RowSum(peers, links, d_mlp_part, rows_in, rows_out, rows_last)
    sums = [
        BlockSum(peers, links, moves, gradient, *(b.at[i] for b in (own_blocks, x_in, z_out, z_in)))
        for i, gradient in enumerate(
            (
                lambda block: down.at[block],
                lambda block: gate_up.at[block, :, pl.ds(0, quarter)],
                lambda block: gate_up.at[block, :, pl.ds(quarter, quarter)],
            )
        )
    ]
    sums[0].taken(down_taken)
    for block in sums[1:]:
        for k in STEPS:
            block.open(k)
    branch_sum = RowSum(peers, links, branch_part, branch_in, branch_out, branch_last)
    pending = [(i, k) for i in (1, 2) for k in STEPS]

    def pump(count):
        for _ in range(count):
            if pending:
                i, k = pending.pop(0)
                if i == 1:
                    sums[i].step(k)
                    continue
                at = STEPS.index(k)
                z_out[2, at] = sums[i].sum_x(k).astype(bf16)
                moves.start(z_out.at[2, at], up_lines.at[at])

    moves.wait(own_d_mlp, own_branch)
    d_mlp_sum.cross(d_mlp_own.at[pl.ds(rows, rows)])
    branch_sum.cross(branch_own.at[pl.ds(rows, rows)])
    for k in STEPS:
        sums[0].step(k)
    pump(2)
    moves.wait(*(ready[n] for n in ("resid", "cotangent", "weight", "mixed", "exact")))
    d_mlp = d_mlp_sum.total(d_mlp_own.at[pl.ds(0, rows)])
    branch_back(
        d_mlp, resid, cotangent, gain, weight, mixed, exact, d_resid, d_mixed, out_grad, gain_grad, deltas
    )
    flush = moves.start(out_grad, out_grad_far)
    pump(2)
    moves.wait(ready["queries"], ready["pairs"])
    seen = (key_at[...] <= query_at[...]) | (key_at[...] < prefix[0])
    for group in range(KEY_VALUE_HEADS):
        attend_back_group(group, seen, queries, pairs, d_mixed, logs, deltas, d_queries, d_pairs)
        if group in (0, 2, 4):
            pump(1)
    pair_sum = RowSum(peers, links, d_pairs, pair_in, pair_out, pair_last)
    pair_sum.cross(d_pairs.at[pl.ds(rows, rows)])
    layer_out[...] = (
        resid[...] + branch_sum.total(branch_own.at[pl.ds(0, rows)]).astype(bf16).astype(f32)
    ).astype(bf16)
    pump(8)
    d_kv[...] = pair_sum.total(d_pairs.at[pl.ds(0, rows)])
    down_sum[...] = sums[0].total()
    gate_sum[...] = sums[1].total()
    links.finish()
    moves.finish()


def back_two_kernel(
    up_lines, out_grad, weight_far, d_queries, d_kv, attn_input, tokens, d_resid, gain, cosine, sine, gain_mlp,
    tokens_grad, gains_sum, up_sum, out_sum, qkv_sum,
    weight, out_own, qkv_grad, up_own, z_in,
    gain_own, gain_c, gain_one, gain_y, gain_two, gain_x, gain_z, local_sem, sent, got, *buffers,
):
    peers = Peers()
    links, moves = Links(sent, got), Moves(local_sem)
    own_out = [moves.start(out_grad.at[2 * side + peers.c], out_own.at[side]) for side in range(2)]
    own_up = moves.start(up_lines.at[STEPS.index(0)], up_own)
    weight_in = moves.start(weight_far, weight)
    out_total = OwnerSum(peers, links, buffers[:11], lambda s, line, side: out_own[s, line, side])
    qkv_total = OwnerSum(
        peers, links, buffers[11:], lambda s, line, side: qkv_grad[2 * s + peers.c, line, side]
    )
    peers.greet()
    for side in range(2):
        out_total.hand(out_grad.at[2 * side + 1 - peers.c], side)
    up_copies = [
        links.send(up_lines.at[at], z_in.at[at], peers.by_z[k]) for at, k in enumerate(STEPS[:-1])
    ]
    d_projected = unproject(d_queries, d_kv, cosine, sine)
    moves.wait(*own_out)
    width = weight.shape[2]
    for j in range(4):
        part = d_projected[:, j * width : (j + 1) * width]
        outer = dot(attn_input[...], part, 0, 0).astype(bf16)
        qkv_grad[j] = outer.reshape(qkv_grad.shape[1:])
        if j % 2:
            qkv_total.hand(qkv_grad.at[j - peers.c], j // 2)
        else:
            out_total.chip(j // 2)
        if j == 2:
            for k in STEPS:
                out_total.open(k)
    for side in range(2):
        qkv_total.chip(side)
    for k in STEPS:
        qkv_total.open(k)
    moves.wait(weight_in)
    back = None
    for j in range(4):
        part = d_projected[:, j * width : (j + 1) * width]
        term = dot(part, weight[j], 1, 1)
        back = term if back is None else back + term
    gain_sum, d_normed = back_norm(back, tokens[...].astype(f32), gain[...])
    gain_own[...] = jnp.concatenate([gain_sum, gain_mlp[...]], axis=0)
    gain_copy = links.send(gain_own, gain_c, peers.by_c)
    for k in STEPS:
        out_total.pass_on(k)
    tokens_grad[...] = d_resid[...] + d_normed
    gain_copy.wait_recv()
    gain_one[...] = gain_own[...] + gain_c[...]
    gain_copy = links.send(gain_one, gain_y, peers.by_y)
    for k in STEPS:
        qkv_total.pass_on(k)
    gain_copy.wait_recv()
    gain_two[...] = gain_one[...] + gain_y[...]
    gain_copy = links.send(gain_two, gain_x, peers.by_x)
    for k in STEPS:
        out_total.close(k)
    gain_copy.wait_recv()
    gain_z[peers.z] = gain_two[...] + gain_x[...]
    gain_copies = [
        links.send(gain_z.at[peers.z], gain_z.at[peers.z], peers.by_z[k]) for k in range(1, lines)
    ]
    for k in STEPS:
        qkv_total.close(k)
    moves.wait(own_up)
    up_total = up_own[...].astype(f32)
    for at, copy in enumerate(up_copies):
        copy.wait_recv()
        up_total = up_total + z_in[at].astype(f32)
    up_sum[...] = up_total
    out_sum[...] = out_total.total()
    for copy in gain_copies:
        copy.wait_recv()
    gains_sum[...] = ((gain_z[0] + gain_z[1]) + gain_z[2]) + gain_z[3]
    qkv_sum[...] = qkv_total.total()
    links.finish()
    moves.finish()


def remote_call(kernel, name, number, outs, scratch, *args, local=16, remote=64, smem=0, flops=0):
    places = {False: spec(), True: spec(pl.ANY)}
    return pl.pallas_call(
        kernel,
        out_shape=[jax.ShapeDtypeStruct(s, k) for s, k, _ in outs],
        in_specs=[places[far] for _, far in args[: len(args) - smem]] + [spec(pltpu.SMEM)] * smem,
        out_specs=[places[far] for _, _, far in outs],
        scratch_shapes=scratch[0]
        + [
            pltpu.SemaphoreType.DMA((local,)),
            pltpu.SemaphoreType.DMA((remote,)),
            pltpu.SemaphoreType.DMA((remote,)),
        ]
        + scratch[1],
        compiler_params=pltpu.CompilerParams(
            collective_id=number, has_side_effects=True, vmem_limit_bytes=62 * 2**20
        ),
        cost_estimate=pl.CostEstimate(flops=flops, bytes_accessed=2**24, transcendentals=0),
        name=name,
    )(*(array for array, _ in args))


def vmem_like(array):
    return pltpu.VMEM(array.shape, array.dtype)


def adam_update(master, moment, square, gradient, step_rate, decay):
    moment_next = beta_one * moment + (1.0 - beta_one) * gradient
    square_next = beta_two * square + (1.0 - beta_two) * gradient * gradient
    master_next = master - step_rate * (
        moment_next / (jnp.sqrt(square_next) + eps_adam) + decay * master
    )
    return (master_next, moment_next, square_next)


def on_device(
    tokens,
    cotangent,
    prefix_len,
    gains_master,
    gains_moment,
    gains_square,
    qkv_master,
    qkv_moment,
    qkv_square,
    out_master,
    out_moment,
    out_square,
    gu_master,
    gu_moment,
    gu_square,
    down_master,
    down_moment,
    down_square,
):
    seq_count = lax.axis_size("seq")
    dp_count = lax.axis_size("dp")
    seq_place = lax.axis_index("seq")
    near = dp_count == 2 * lines and seq_count == 4
    grid = Grid() if near else None
    plain = Plain()
    token_rows = tokens.shape[0]
    quarter = FF // seq_count
    shard_rows = gu_master.shape[0]
    qkv_b = qkv_master.astype(bf16)
    out_b = out_master.astype(bf16)
    gu_b = gu_master.astype(bf16).reshape(shard_rows, 2 * quarter)
    down_b = down_master.astype(bf16).T
    if near:
        key_places = [seq_place ^ step for step in (0, 2, 1, 3)]
    else:
        key_places = list(range(seq_count))
    within = jnp.arange(token_rows, dtype=jnp.int32)
    positions = seq_place * token_rows + within
    key_positions = jnp.concatenate([spot * token_rows + within for spot in key_places])

    cosine_half, sine_half = rope_tables(positions, HEAD_SIZE)
    cosine = jnp.concatenate([cosine_half] * 4, axis=1)
    sine = jnp.concatenate([-sine_half, sine_half] * 2, axis=1)
    shape = (token_rows, D)
    attn_gain, mlp_gain = gains_master[0:1], gains_master[1:2]
    key_count = seq_count * token_rows
    score_flops = 2 * token_rows * key_count * QUERY_WIDTH
    out_flops = 2 * token_rows * D * D
    pair = (token_rows, 2 * PAIR_WIDTH)
    all_pairs = (key_count, 2 * PAIR_WIDTH)
    if near:
        wide = (seq_count, 2 * lines)
        outs = [
            (wide + qkv_b.shape, bf16, True),
            (wide + out_b.shape, bf16, True),
            (wide[1:] + gu_b.shape, bf16, True),
            (wide[1:] + down_b.shape, bf16, True),
            (shape, bf16, False),
            (shape, bf16, False),
            (all_pairs, bf16, True),
            (shape, bf16, False),
            (shape, f32, False),
            ((token_rows, 128), f32, False),
            (shape, f32, False),
            ((key_count, D), bf16, True),
            ((key_count, D), bf16, True),
        ]
        front = remote_call(
            front_kernel,
            "front",
            0,
            outs,
            (
                [pltpu.VMEM(s, k) for s, k, _ in outs[:2]]
                + [pltpu.VMEM(all_pairs, bf16), pltpu.VMEM(shape, bf16)],
                [],
            ),
            *((a, True) for a in (qkv_b, out_b, gu_b, down_b, cotangent)),
            *((a, False) for a in (tokens, attn_gain, mlp_gain, cosine, sine)),
            *((a, False) for a in (positions[:, None], key_positions[None, :], prefix_len)),
            remote=112,
            smem=1,
            flops=2 * token_rows * D * QKV + 2 * score_flops + out_flops,
        )
        qkv_full, out_full, gu_part, down_part, attn_input, queries, kv_rows = front[:7]
        mixed, mixed_exact, logs, resid, mlp_rows, cot_rows = front[7:]
        qkv_full = qkv_full.reshape(seq_count, D, -1)
        out_full = out_full.reshape(seq_count, D, -1)
        gu_part, down_part = gu_part.reshape(D, -1), down_part.reshape(D, -1)
    else:
        qkv_full = plain.gather_attention(qkv_b)
        out_full = plain.gather_attention(out_b)
        gu_part = lax.all_gather(gu_b, "dp", axis=0, tiled=True)
        down_part = lax.all_gather(down_b, "dp", axis=0, tiled=True)
        cot_rows = lax.all_gather(cotangent, "seq", axis=0, tiled=True)
        attn_input, queries, kv_local = local_call(
            project_kernel,
            "project",
            [(shape, bf16), (shape, bf16), (pair, bf16)],
            *(tokens, attn_gain, qkv_full, cosine, sine),
            flops=2 * token_rows * D * QKV,
        )
        kv_rows = lax.all_gather(kv_local, "seq", axis=0, tiled=True)
        mixed, mixed_exact, logs, resid, mlp_input = local_call(
            attend_kernel,
            "attend",
            [(shape, bf16), (shape, f32), ((token_rows, 128), f32), (shape, f32), (shape, bf16)],
            *(queries, kv_rows, tokens, out_full, mlp_gain),
            *(positions[:, None], key_positions[None, :], prefix_len),
            flops=2 * score_flops + out_flops,
            smem=1,
        )
        mlp_rows = lax.all_gather(mlp_input, "seq", axis=0, tiled=True)
    gateup = jnp.dot(mlp_rows, gu_part, preferred_element_type=f32)
    gate = gateup[:, :quarter]
    up_part = gateup[:, quarter:]
    sigmoid_gate = jax.nn.sigmoid(gate)
    silu_gate = gate * sigmoid_gate
    hidden = (silu_gate * up_part).astype(bf16)
    d_hidden = jnp.dot(cot_rows, down_part, preferred_element_type=f32)
    d_gate_b = (d_hidden * up_part * sigmoid_gate * (1.0 + gate * (1.0 - sigmoid_gate))).astype(bf16)
    d_up_b = (d_hidden * silu_gate).astype(bf16)
    d_gateup = jnp.concatenate([d_gate_b, d_up_b], axis=1)

    def contract(left, right, left_axis, right_axis):
        return lax.dot_general(
            left, right, (((left_axis,), (right_axis,)), ((), ())), preferred_element_type=f32
        )

    down_local = contract(cot_rows, hidden, 0, 0).astype(bf16)
    pair_shape = (seq_count, D, out_full.shape[2])
    if near:
        blocks = (2 * lines, shard_rows, quarter)
        lined = (3, lines, shard_rows, quarter)
        down_local = down_local.reshape(blocks)
        down_theirs = pick(down_local.reshape(lines, 2, shard_rows, quarter), 1 - grid.x, 1)
        down_taken = grid.swap_x(down_theirs)
        d_mlp_part = contract(d_gateup, gu_part, 1, 1).astype(bf16)
        branch_part = contract(hidden, down_part, 1, 1).astype(bf16)
        gu_local = contract(mlp_rows, d_gateup, 0, 0).astype(bf16)
        gu_local = gu_local.reshape(blocks[:2] + (2 * quarter,))
        rows_of = [((2 * token_rows, D), bf16), (shape, bf16), (shape, bf16)]
        pairs_of = [((2 * token_rows, 2 * PAIR_WIDTH), bf16), (pair, bf16), (pair, bf16)]
        far = [resid, cotangent, out_full, mixed, mixed_exact, queries, kv_rows]
        layer_out, d_resid, out_local, gain_mlp, d_queries, d_kv, down_owned, gate_owned, up_lines = remote_call(
            back_one_kernel,
            "back_one",
            1,
            [
                (shape, bf16, False),
                (shape, f32, False),
                (pair_shape, bf16, True),
                ((1, D), f32, False),
                (shape, f32, False),
                (pair, f32, False),
                ((shard_rows, quarter), f32, False),
                ((shard_rows, quarter), f32, False),
                (lined[1:], bf16, True),
            ],
            (
                [pltpu.VMEM((2 * token_rows, D), bf16)] * 2
                + [vmem_like(a) for a in far]
                + [pltpu.VMEM(*s) for s in rows_of + rows_of + pairs_of]
                + [
                    pltpu.VMEM(shape, bf16),
                    pltpu.VMEM((32, token_rows), f32),
                    pltpu.VMEM(kv_rows.shape, bf16),
                    pltpu.VMEM(pair_shape, bf16),
                ]
                + [pltpu.VMEM(lined, bf16)] * 4,
                [],
            ),
            *((a, True) for a in (d_mlp_part, branch_part)),
            *((a, True) for a in (down_local, down_taken, gu_local, *far)),
            *((a, False) for a in (mlp_gain, logs.T, positions[None, :], key_positions[:, None])),
            (prefix_len, False),
            local=40,
            smem=1,
            flops=5 * score_flops + 2 * out_flops,
        )
        line_shape = (seq_count, lines, 2, shard_rows)
        qkv_width, out_width = qkv_full.shape[2], out_full.shape[2]
        tokens_grad, gains_grad, up_owned, out_owned, qkv_owned = remote_call(
            back_two_kernel,
            "back_two",
            2,
            [
                (shape, f32, False),
                ((2, D), f32, False),
                ((shard_rows, quarter), f32, False),
                ((shard_rows, out_width), f32, False),
                ((shard_rows, qkv_width), f32, False),
            ],
            (
                [
                    vmem_like(qkv_full),
                    pltpu.VMEM((2,) + line_shape[1:] + (out_width,), bf16),
                    pltpu.VMEM(line_shape + (qkv_width,), bf16),
                ]
                + [pltpu.VMEM(blocks[1:], bf16), pltpu.VMEM((3,) + blocks[1:], bf16)]
                + [pltpu.VMEM((2, D), f32)] * 6
                + [pltpu.VMEM((lines, 2, D), f32)],
                owner_buffers(shard_rows, out_width) + owner_buffers(shard_rows, qkv_width),
            ),
            *((a, True) for a in (up_lines, out_local.reshape(line_shape + (-1,)), qkv_full)),
            *((a, False) for a in (d_queries, d_kv, attn_input, tokens, d_resid, attn_gain)),
            *((a, False) for a in (cosine, sine, gain_mlp)),
            flops=4 * token_rows * D * QKV,
        )
        gu_owned = with_layout_constraint(
            jnp.stack([gate_owned, up_owned], axis=1), Layout(major_to_minor=(0, 1, 2))
        )
    else:
        d_mlp_part = contract(d_gateup, gu_part, 1, 1).astype(bf16)
        branch_part = contract(hidden, down_part, 1, 1).astype(bf16)
        gu_local = contract(mlp_rows, d_gateup, 0, 0).astype(bf16)

        def scatter(values, axis):
            return lax.psum_scatter(values, axis, scatter_dimension=0, tiled=True).astype(f32)

        d_mlp_input = scatter(d_mlp_part, "seq")
        layer_out = (resid + scatter(branch_part, "seq")).astype(bf16)
        down_owned = scatter(down_local, "dp")
        gu_owned = scatter(gu_local, "dp").reshape(shard_rows, 2, quarter)
        d_resid, d_mixed, out_local, gain_mlp, deltas = local_call(
            branch_back_kernel,
            "branch_back",
            [(shape, f32), (shape, bf16), (pair_shape, bf16), ((1, D), f32), ((32, token_rows), f32)],
            *(d_mlp_input, resid, cotangent, mlp_gain, out_full, mixed, mixed_exact),
            flops=2 * out_flops,
        )
        out_owned = plain.reduce_attention(out_local)
        d_queries, d_pairs = local_call(
            attend_back_kernel,
            "attend_back",
            [(shape, f32), (kv_rows.shape, bf16)],
            *(queries, kv_rows, d_mixed, logs.T, deltas),
            *(positions[None, :], key_positions[:, None], prefix_len),
            flops=5 * score_flops,
            smem=1,
        )
        d_kv = scatter(d_pairs, "seq")
        tokens_grad, qkv_local, gain_attn = local_call(
            project_back_kernel,
            "project_back",
            [(shape, f32), (qkv_full.shape, bf16), ((1, D), f32)],
            *(d_queries, d_kv, attn_input, tokens, d_resid, attn_gain, qkv_full, cosine, sine),
            flops=4 * token_rows * D * QKV,
        )
        qkv_owned = plain.reduce_attention(qkv_local)
        gains_grad = lax.psum(jnp.concatenate([gain_attn, gain_mlp], axis=0), ("dp", "seq"))
    down_owned = down_owned.T
    owned = (qkv_owned, out_owned, gu_owned, down_owned)
    rate_wide = 0.5 * D ** (-0.5)
    rate_out = 0.5 * max(QUERY_WIDTH // 256, 1) ** (-0.5)
    rate_down = 0.5 * FF ** (-0.5)
    gains_new = adam_update(gains_master, gains_moment, gains_square, gains_grad, gain_rate, 0.0)
    qkv_new = adam_update(qkv_master, qkv_moment, qkv_square, owned[0], rate_wide, weight_decay)
    out_new = adam_update(out_master, out_moment, out_square, owned[1], rate_out, weight_decay)
    gu_new = adam_update(gu_master, gu_moment, gu_square, owned[2], rate_wide, weight_decay)
    down_new = adam_update(down_master, down_moment, down_square, owned[3], rate_down, weight_decay)
    return (
        layer_out,
        tokens_grad,
        gains_grad,
        owned[0],
        owned[1],
        owned[2],
        owned[3],
        gains_new[0],
        gains_new[1],
        gains_new[2],
        qkv_new[0],
        qkv_new[1],
        qkv_new[2],
        qkv_new[0].astype(jnp.bfloat16),
        out_new[0],
        out_new[1],
        out_new[2],
        out_new[0].astype(jnp.bfloat16),
        gu_new[0],
        gu_new[1],
        gu_new[2],
        gu_new[0].astype(jnp.bfloat16),
        down_new[0],
        down_new[1],
        down_new[2],
        down_new[0].astype(jnp.bfloat16),
    )


def solution(mesh):
    in_specs = (
        P(("dp", "seq"), None),
        P(("dp", "seq"), None),
        P("dp"),
        P(),
        P(),
        P(),
        P("dp", "seq"),
        P("dp", "seq"),
        P("dp", "seq"),
        P("dp", "seq"),
        P("dp", "seq"),
        P("dp", "seq"),
        P("dp", None, "seq"),
        P("dp", None, "seq"),
        P("dp", None, "seq"),
        P("seq", "dp"),
        P("seq", "dp"),
        P("seq", "dp"),
    )
    out_specs = (
        P(("dp", "seq"), None),
        P(("dp", "seq"), None),
        P(),
        P("dp", "seq"),
        P("dp", "seq"),
        P("dp", None, "seq"),
        P("seq", "dp"),
        P(),
        P(),
        P(),
        P("dp", "seq"),
        P("dp", "seq"),
        P("dp", "seq"),
        P("dp", "seq"),
        P("dp", "seq"),
        P("dp", "seq"),
        P("dp", "seq"),
        P("dp", "seq"),
        P("dp", None, "seq"),
        P("dp", None, "seq"),
        P("dp", None, "seq"),
        P("dp", None, "seq"),
        P("seq", "dp"),
        P("seq", "dp"),
        P("seq", "dp"),
        P("seq", "dp"),
    )
    return jax.shard_map(
        on_device, mesh=mesh, in_specs=in_specs, out_specs=out_specs, check_vma=False
    )
```

```python
import functools
import math

import jax
import jax.numpy as jnp
from jax import lax
from jax.experimental import pallas as pl
from jax.experimental.layout import Layout, with_layout_constraint
from jax.experimental.pallas import tpu as pltpu
from jax.sharding import PartitionSpec as P

D = 1280
QUERY_HEADS = 20
KEY_VALUE_HEADS = 5
HEAD_SIZE = 64
FF = 3584
QUERY_WIDTH = 1280
PAIR_WIDTH = KEY_VALUE_HEADS * HEAD_SIZE
QKV = QUERY_WIDTH + 2 * PAIR_WIDTH
GROUP = QUERY_HEADS // KEY_VALUE_HEADS


eps_norm = 1e-05
eps_adam = 1e-08
rope_base = 10000.0
beta_one = 0.5
beta_two = 0.5
weight_decay = 0.1
score_after_mask = -1e30
gain_rate = 0.3
lines = 4
half_rows = 2


bf16 = jnp.bfloat16
f32 = jnp.float32


def rope_tables(positions, head_width):
    half_width = head_width // 2
    frequency = rope_base ** (-2.0 * jnp.arange(half_width, dtype=jnp.float32) / head_width)
    angles = positions.astype(jnp.float32)[:, None] * frequency[None, :]
    return (jnp.cos(angles), jnp.sin(angles))


def pick(values, index, axis):
    return lax.dynamic_index_in_dim(values, index, axis, keepdims=False)


def add(left, right, kind=jnp.bfloat16):
    return (left.astype(f32) + right.astype(f32)).astype(kind)


def after(values, *others):
    return lax.optimization_barrier((values,) + others)[0]


class Grid:
    def __init__(self):
        dp = lax.axis_index("dp")
        seq = lax.axis_index("seq")
        self.z, self.x, self.y, self.c = dp // 2, dp % 2, seq // 2, seq % 2

    def swap(self, values, axis, bit):
        count = lax.axis_size(axis)
        return lax.ppermute(values, axis, [(i, i ^ bit) for i in range(count)])

    def swap_x(self, values):
        return self.swap(values, "dp", 1)

    def swap_y(self, values):
        return self.swap(values, "seq", 2)

    def swap_c(self, values):
        return self.swap(values, "seq", 1)

    def send_z(self, values, steps):
        pairs = [(i, (i // 2 + steps) % lines * 2 + i % 2) for i in range(2 * lines)]
        return lax.ppermute(values, "dp", pairs)


MESH = pl.DeviceIdType.MESH


def place_of():
    dp = lax.axis_index("dp")
    seq = lax.axis_index("seq")
    return dp // 2, lax.rem(dp, 2), seq // 2, lax.rem(seq, 2)


def greet(peers):
    barrier = pltpu.get_barrier_semaphore()
    for peer in peers:
        pl.semaphore_signal(barrier, inc=1, device_id=peer, device_id_type=MESH)
    pl.semaphore_wait(barrier, len(peers))


class Plain:
    def gather_attention(self, shard):
        blocks = lax.all_gather(shard, ("dp", "seq"), axis=0)
        split = blocks.reshape(lax.axis_size("dp"), lax.axis_size("seq"), *shard.shape)
        return jnp.swapaxes(split, 0, 1).reshape(lax.axis_size("seq"), -1, shard.shape[1])

    def reduce_attention(self, gradient):
        owners, wide, width = gradient.shape
        blocks = gradient.reshape(owners, lax.axis_size("dp"), -1, width)
        blocks = jnp.swapaxes(blocks, 0, 1).reshape(-1, width)
        return lax.psum_scatter(blocks, ("dp", "seq"), scatter_dimension=0, tiled=True).astype(f32)


def spec(space=pltpu.VMEM):
    return pl.BlockSpec(memory_space=space)


def local_call(kernel, name, outs, *args, flops=0, smem=0):
    moved = sum(a.size * a.dtype.itemsize for a in args) + sum(
        math.prod(s) * jnp.dtype(k).itemsize for s, k in outs
    )
    return pl.pallas_call(
        kernel,
        out_shape=[jax.ShapeDtypeStruct(s, k) for s, k in outs],
        in_specs=[spec()] * (len(args) - smem) + [spec(pltpu.SMEM)] * smem,
        out_specs=[spec()] * len(outs),
        compiler_params=pltpu.CompilerParams(vmem_limit_bytes=60 * 2**20),
        cost_estimate=pl.CostEstimate(flops=flops, bytes_accessed=moved, transcendentals=0),
        name=name,
    )(*args)


def dot(left, right, left_axis=1, right_axis=0, **how):
    return lax.dot_general(
        left, right, (((left_axis,), (right_axis,)), ((), ())), preferred_element_type=f32, **how
    )


def rotate(chunk, cosine, sine):
    lane = lax.broadcasted_iota(jnp.int32, chunk.shape, 1)
    swapped = jnp.where(lane % 64 < 32, pltpu.roll(chunk, 96, 1), pltpu.roll(chunk, 32, 1))
    return chunk * cosine + swapped * sine


def project(tokens, gain, weights, cosine, sine, attn_input, queries, pairs):
    x = tokens[...].astype(f32)
    scale = lax.rsqrt(jnp.mean(x * x, axis=-1, keepdims=True) + eps_norm)
    normed = (x * scale * gain[...]).astype(bf16)
    attn_input[...] = normed
    projected = jnp.concatenate([dot(normed, block) for block in weights], axis=1)
    first = lax.broadcasted_iota(jnp.int32, (x.shape[0], 128), 1) < 64
    for chunk in (*range(QUERY_WIDTH // 128, QKV // 128), *range(QUERY_WIDTH // 128)):
        u = projected[:, chunk * 128 : chunk * 128 + 128]
        at = chunk * 128 - QUERY_WIDTH
        if at < 0:
            turned = rotate(u, cosine[...], sine[...]) * HEAD_SIZE ** (-0.5)
            queries[:, chunk * 128 : chunk * 128 + 128] = turned.astype(bf16)
        elif at + 128 <= PAIR_WIDTH:
            pairs[:, at : at + 128] = rotate(u, cosine[...], sine[...]).astype(bf16)
        elif at < PAIR_WIDTH:
            turned = jnp.where(first, rotate(u, cosine[...], sine[...]), u)
            pairs[:, at : at + 128] = turned.astype(bf16)
        else:
            pairs[:, at : at + 128] = u.astype(bf16)


def project_kernel(tokens, gain, weight, *refs):
    project(tokens, gain, [weight[j] for j in range(4)], *refs)


def head(values, index):
    return values[:, index * HEAD_SIZE : (index + 1) * HEAD_SIZE]


def attend_group(group, seen, queries, pairs, exact, logs):
    keys = head(pairs, group)
    values = head(pairs, KEY_VALUE_HEADS + group)
    for member in range(GROUP):
        at = group * GROUP + member
        scores = jnp.where(seen, dot(head(queries, at), keys, 1, 1), score_after_mask)
        top = jnp.max(scores, axis=-1, keepdims=True)
        powers = jnp.exp(scores - top)
        total = jnp.sum(powers, axis=-1, keepdims=True)
        exact[:, at * 64 : at * 64 + 64] = dot(powers.astype(bf16), values) / total
        logs[:, at : at + 1] = top + jnp.log(total)


def close_attention(tokens, weights, gain, mixed, exact, resid, mlp_input):
    mixed[...] = exact[...].astype(bf16)
    branch = jnp.concatenate([dot(mixed[...], block) for block in weights], axis=1)
    total = tokens[...].astype(f32) + branch
    resid[...] = total
    scale = lax.rsqrt(jnp.mean(total * total, axis=-1, keepdims=True) + eps_norm)
    mlp_input[...] = (total * scale * gain[...]).astype(bf16)


def attend_kernel(
    queries, pairs, tokens, weight, gain, query_at, key_at, prefix, mixed, exact, logs, resid, mlp_input
):
    seen = (key_at[...] <= query_at[...]) | (key_at[...] < prefix[0])
    for group in range(KEY_VALUE_HEADS):
        attend_group(group, seen, queries, pairs, exact, logs)
    close_attention(tokens, [weight[j] for j in range(4)], gain, mixed, exact, resid, mlp_input)


def back_norm(grad_out, source, gain):
    scale = lax.rsqrt(jnp.mean(source * source, axis=-1, keepdims=True) + eps_norm)
    normed = source * scale
    scaled = grad_out * gain
    inner = jnp.mean(scaled * normed, axis=-1, keepdims=True)
    return jnp.sum(grad_out * normed, axis=0, keepdims=True), scale * (scaled - normed * inner)


def branch_back(
    d_mlp, resid, cotangent, gain, weight, mixed, exact, d_resid, d_mixed, out_grad, gain_grad, deltas
):
    gain_sum, d_normed = back_norm(d_mlp, resid[...], gain[...])
    gain_grad[...] = gain_sum
    total = cotangent[...].astype(f32) + d_normed
    d_resid[...] = total
    width = weight.shape[2]
    d_branch = total.astype(bf16)
    back = None
    for j in range(4):
        part = d_branch[:, j * width : (j + 1) * width]
        out_grad[j] = dot(mixed[...], part, 0, 0).astype(bf16)
        term = dot(part, weight[j], 1, 1)
        back = term if back is None else back + term
    d_mixed[...] = back.astype(bf16)
    product = d_mixed[...].astype(f32) * exact[...]
    which = lax.broadcasted_iota(jnp.int32, (32, QUERY_WIDTH), 1) // HEAD_SIZE
    ones = (which == lax.broadcasted_iota(jnp.int32, (32, QUERY_WIDTH), 0)).astype(f32)
    deltas[...] = dot(ones, product, 1, 1, precision=lax.Precision.HIGHEST)


def branch_back_kernel(d_mlp, *refs):
    branch_back(d_mlp[...], *refs)


def attend_back_group(group, seen, queries, pairs, d_mixed, logs, deltas, d_queries, d_pairs):
    keys = head(pairs, group)
    values = head(pairs, KEY_VALUE_HEADS + group)
    turned_keys = keys.T
    d_keys = d_values = None
    for member in range(GROUP):
        at = group * GROUP + member
        mine = head(queries, at)
        back = head(d_mixed, at)
        scores = jnp.where(seen, dot(keys, mine, 1, 1), score_after_mask)
        probs = jnp.exp(scores - logs[at : at + 1, :])
        d_probs = dot(values, back, 1, 1)
        d_scores = (probs * (d_probs - deltas[at : at + 1, :])).astype(bf16)
        turned = dot(turned_keys, d_scores) * HEAD_SIZE ** (-0.5)
        d_queries[:, at * 64 : at * 64 + 64] = turned.T
        key_term = dot(d_scores, mine)
        value_term = dot(probs.astype(bf16), back)
        d_keys = key_term if d_keys is None else d_keys + key_term
        d_values = value_term if d_values is None else d_values + value_term
    at = group * 64
    d_pairs[:, at : at + 64] = d_keys.astype(bf16)
    at += PAIR_WIDTH
    d_pairs[:, at : at + 64] = d_values.astype(bf16)


def attend_back_kernel(
    queries, pairs, d_mixed, logs, deltas, query_at, key_at, prefix, d_queries, d_pairs
):
    seen = (key_at[...] <= query_at[...]) | (key_at[...] < prefix[0])
    for group in range(KEY_VALUE_HEADS):
        attend_back_group(group, seen, queries, pairs, d_mixed, logs, deltas, d_queries, d_pairs)


def unproject(d_queries, d_pairs, cosine, sine):
    rows = d_queries.shape[0]
    first = lax.broadcasted_iota(jnp.int32, (rows, 128), 1) < 64
    chunks = []
    for chunk in range(QKV // 128):
        at = chunk * 128 - QUERY_WIDTH
        if at < 0:
            chunks.append(rotate(d_queries[:, chunk * 128 : chunk * 128 + 128], cosine[...], -sine[...]))
            continue
        u = d_pairs[:, at : at + 128]
        if at + 128 <= PAIR_WIDTH:
            u = rotate(u, cosine[...], -sine[...])
        elif at < PAIR_WIDTH:
            u = jnp.where(first, rotate(u, cosine[...], -sine[...]), u)
        chunks.append(u)
    return jnp.concatenate([u.astype(bf16) for u in chunks], axis=1)


def project_back_kernel(
    d_queries, d_pairs, attn_input, tokens, d_resid, gain, weight, cosine, sine, tokens_grad, qkv_grad, gain_grad
):
    d_projected = unproject(d_queries, d_pairs, cosine, sine)
    width = weight.shape[2]
    back = None
    for j in range(4):
        part = d_projected[:, j * width : (j + 1) * width]
        qkv_grad[j] = dot(attn_input[...], part, 0, 0).astype(bf16)
        term = dot(part, weight[j], 1, 1)
        back = term if back is None else back + term
    gain_sum, d_normed = back_norm(back, tokens[...].astype(f32), gain[...])
    gain_grad[...] = gain_sum
    tokens_grad[...] = d_resid[...] + d_normed


class Links:
    def __init__(self, sent, got):
        self.sent, self.got, self.copies, self.some = sent, got, [], []

    def send(self, source, target, peer):
        slot = len(self.copies)
        copy = pltpu.make_async_remote_copy(
            src_ref=source,
            dst_ref=target,
            send_sem=self.sent.at[slot],
            recv_sem=self.got.at[slot],
            device_id=peer,
            device_id_type=MESH,
        )
        copy.start()
        self.copies.append(copy)
        return copy

    def send_if(self, started, source, target, peer):
        slot = len(self.copies)
        copy = pltpu.make_async_remote_copy(
            src_ref=source,
            dst_ref=target,
            send_sem=self.sent.at[slot],
            recv_sem=self.got.at[slot],
            device_id=peer,
            device_id_type=MESH,
        )
        self.copies.append(None)
        self.some.append((started, copy))
        pl.when(started)(copy.start)
        return copy

    def finish(self):
        for copy in self.copies:
            if copy is not None:
                copy.wait_send()
        for started, copy in self.some:
            pl.when(started)(copy.wait_send)


class Moves:
    def __init__(self, sems):
        self.sems, self.copies, self.seen = sems, [], set()

    def start(self, source, target):
        slot = len(self.copies)
        copy = pltpu.make_async_copy(source, target, self.sems.at[slot])
        copy.start()
        self.copies.append(copy)
        return slot

    def wait(self, *slots):
        for slot in slots:
            if slot not in self.seen:
                self.seen.add(slot)
                self.copies[slot].wait()

    def finish(self):
        self.wait(*range(len(self.copies)))


class Peers:
    def __init__(self):
        z, x, y, c = place_of()
        self.z, self.x, self.y, self.c = z, x, y, c
        dp, seq = 2 * z + x, 2 * y + c
        self.by_x = (2 * z + 1 - x, seq)
        self.by_y = (dp, 2 * (1 - y) + c)
        self.by_c = (dp, 2 * y + 1 - c)
        self.by_z = {k: (2 * self.line(k) + x, seq) for k in range(1, lines)}

    def line(self, steps):
        return lax.rem(self.z + steps, lines)

    def greet(self):
        greet([self.by_x, self.by_y, self.by_c] + [self.by_z[k] for k in range(1, lines)])


STEPS = (1, 3, 2, 0)


class RowSum:
    def __init__(self, peers, links, partial, arrived, passed, last):
        self.peers, self.links, self.partial = peers, links, partial
        self.arrived, self.passed, self.last = arrived, passed, last
        self.rows = partial.shape[0] // 4
        rows = self.rows
        self.far = links.send(
            partial.at[pl.ds(3 * rows, rows)], arrived.at[pl.ds(rows, rows)], peers.by_c
        )
        self.near = links.send(
            partial.at[pl.ds(2 * rows, rows)], arrived.at[pl.ds(0, rows)], peers.by_c
        )

    def cross(self, across):
        rows = self.rows
        self.far.wait_recv()
        total = across[...].astype(f32) + self.arrived[rows:, :].astype(f32)
        self.passed[...] = total.astype(bf16)
        self.over = self.links.send(self.passed, self.last, self.peers.by_y)

    def total(self, own):
        self.near.wait_recv()
        self.over.wait_recv()
        return (
            own[...].astype(f32)
            + self.arrived[: self.rows, :].astype(f32)
            + self.last[...].astype(f32)
        )


class BlockSum:
    def __init__(self, peers, links, moves, gradient, own, x_in, z_out, z_in):
        self.peers, self.links, self.moves = peers, links, moves
        self.gradient, self.own, self.x_in, self.z_out, self.z_in = gradient, own, x_in, z_out, z_in
        self.arriving, self.slots, self.final, self.kept = {}, {}, {}, None
        for at, k in enumerate(STEPS):
            block = 2 * peers.line(k) + peers.x
            self.slots[k] = [moves.start(gradient(block), own.at[at])]

    def taken(self, arrived):
        for at, k in enumerate(STEPS):
            self.slots[k].append(self.moves.start(arrived.at[self.peers.line(k)], self.x_in.at[at]))

    def open(self, k):
        at = STEPS.index(k)
        theirs = 2 * self.peers.line(k) + 1 - self.peers.x
        self.arriving[k] = self.links.send(
            self.gradient(theirs), self.x_in.at[at], self.peers.by_x
        )

    def sum_x(self, k):
        at = STEPS.index(k)
        self.moves.wait(*self.slots[k])
        if k in self.arriving:
            self.arriving[k].wait_recv()
        return self.own[at].astype(f32) + self.x_in[at].astype(f32)

    def step(self, k):
        at = STEPS.index(k)
        total = self.sum_x(k)
        if k:
            self.z_out[at] = total.astype(bf16)
            self.final[k] = self.links.send(self.z_out.at[at], self.z_in.at[at], self.peers.by_z[k])
        else:
            self.kept = total

    def total(self):
        total = self.kept
        for at, k in enumerate(STEPS[:-1]):
            self.final[k].wait_recv()
            total = total + self.z_in[at].astype(f32)
        return total


class OwnerSum:
    def __init__(self, peers, links, buffers, own):
        self.peers, self.links, self.own = peers, links, own
        (self.c_in, self.sums, self.y_in, self.x_in, self.x_out, self.y_out) = buffers[:6]
        (self.x_last, self.y_last, self.keep, self.z_out, self.z_in) = buffers[6:]
        self.half = self.sums.shape[3] // 2
        self.over, self.one, self.two, self.final = {}, {}, {}, {}

    def hand(self, source, y_side):
        self.over[y_side] = self.links.send(source, self.c_in.at[y_side], self.peers.by_c)

    def chip(self, y_side):
        self.over[y_side].wait_recv()
        for line in range(lines):
            for side in range(2):
                self.sums[y_side, line, side] = (
                    self.own(y_side, line, side).astype(f32)
                    + self.c_in[y_side, line, side].astype(f32)
                ).astype(bf16)

    def open(self, k):
        p, half = self.peers, self.half
        line, at = p.line(k), STEPS.index(k)
        self.one[k] = (
            self.links.send(
                self.sums.at[1 - p.y, line, :, pl.ds(0, half)], self.y_in.at[at], p.by_y
            ),
            self.links.send(
                self.sums.at[:, line, 1 - p.x, pl.ds(half, half)], self.x_in.at[at], p.by_x
            ),
        )

    def pass_on(self, k):
        p, half = self.peers, self.half
        line, at = p.line(k), STEPS.index(k)
        by_y, by_x = self.one[k]

        def add_up(mine, arrived):
            return mine.astype(f32) + arrived.astype(f32)

        by_y.wait_recv()
        theirs = add_up(self.sums[p.y, line, 1 - p.x, pl.ds(0, half)], self.y_in[at, 1 - p.x])
        self.x_out[at] = theirs.astype(bf16)
        first = self.links.send(self.x_out.at[at], self.x_last.at[at], p.by_x)
        mine = add_up(self.sums[p.y, line, p.x, pl.ds(0, half)], self.y_in[at, p.x])
        self.keep[at, 0:half] = mine
        by_x.wait_recv()
        theirs = add_up(self.sums[1 - p.y, line, p.x, pl.ds(half, half)], self.x_in[at, 1 - p.y])
        self.y_out[at] = theirs.astype(bf16)
        second = self.links.send(self.y_out.at[at], self.y_last.at[at], p.by_y)
        mine = add_up(self.sums[p.y, line, p.x, pl.ds(half, half)], self.x_in[at, p.y])
        self.keep[at, half : 2 * half] = mine
        self.two[k] = first, second

    def close(self, k):
        at, half = STEPS.index(k), self.half
        for copy in self.two[k]:
            copy.wait_recv()
        self.keep[at, 0:half] = self.keep[at, 0:half] + self.x_last[at].astype(f32)
        self.keep[at, half : 2 * half] = self.keep[at, half : 2 * half] + self.y_last[at].astype(f32)
        if k:
            self.z_out[at] = self.keep[at].astype(bf16)
            self.final[k] = self.links.send(self.z_out.at[at], self.z_in.at[at], self.peers.by_z[k])

    def total(self):
        total = self.keep[STEPS.index(0)]
        for at, k in enumerate(STEPS[:-1]):
            self.final[k].wait_recv()
            total = total + self.z_in[at].astype(f32)
        return total


def owner_buffers(rows, width):
    half = rows // 2
    return [
        pltpu.VMEM(shape, kind)
        for shape, kind in (
            ((2, lines, 2, rows, width), bf16),
            ((2, lines, 2, rows, width), bf16),
            ((lines, 2, half, width), bf16),
            ((lines, 2, half, width), bf16),
            ((lines, half, width), bf16),
            ((lines, half, width), bf16),
            ((lines, half, width), bf16),
            ((lines, half, width), bf16),
            ((lines, rows, width), f32),
            ((lines, rows, width), bf16),
            ((lines, rows, width), bf16),
        )
    ]


def front_kernel(
    qkv_shard, out_shard, gu_shard, down_shard, cotangent, tokens, attn_gain, mlp_gain, cosine, sine,
    query_at, key_at, prefix,
    qkv_far, out_far, gu_far, down_far, attn_input, queries, pairs_far, mixed, exact, log_rows, resid, mlp_rows, cot_rows,
    qkv_full, out_full, pairs, mlp_input, logs, local_sem, sent, got,
):
    peers = Peers()
    links, moves = Links(sent, got), Moves(local_sem)
    z, x, y, c = peers.z, peers.x, peers.y, peers.c
    mine, other = 2 * y + c, 2 * (1 - y) + c
    rows = tokens.shape[0]
    half = qkv_shard.shape[0] // 2
    shards, wholes = (qkv_shard, out_shard), (qkv_full, out_full)
    ffn_shards, ffn_wholes = (gu_shard, down_shard), (gu_far, down_far)
    own = 2 * z + x
    local = [moves.start(s, w.at[mine, own]) for s, w in zip(shards, wholes)]
    local += [moves.start(s, w.at[own]) for s, w in zip(ffn_shards, ffn_wholes)]
    local.append(moves.start(cotangent, cot_rows.at[pl.ds(0, rows)]))
    peers.greet()
    order = (0, 1, 3, 2)
    came = {}

    def relay(steps, way):
        line, beyond = z - way * steps, z + way
        held = (line >= 0) & (line < lines)
        goes = held & (beyond >= 0) & (beyond < lines)
        line = lax.clamp(0, line, lines - 1)
        beyond = lax.clamp(0, beyond, lines - 1)
        beyond = jnp.where(beyond == z, z - way, beyond)
        for array in range(2):
            view = ffn_wholes[array].at[2 * line + x]
            origin = view if steps else ffn_shards[array]
            came["ffn", array, way, steps + 1] = links.send_if(
                goes, origin, view, (2 * beyond + x, mine)
            )

    def relayed(steps, way):
        line = z - way * steps
        held = (line >= 0) & (line < lines)
        line = lax.clamp(0, line, lines - 1)
        for array in range(2):
            pl.when(held)(came["ffn", array, way, steps].wait_recv)
        if steps < lines - 1:
            relay(steps, way)
        for array in range(2):
            view = ffn_wholes[array].at[2 * line + x]
            came["ffn", array, way, steps, "x"] = held, links.send_if(held, view, view, peers.by_x)

    for array in range(2):
        for k in order[1:]:
            came[array, "z", k] = links.send(
                shards[array], wholes[array].at[mine, own], peers.by_z[k]
            )
    for way in (1, -1):
        relay(0, way)

    def source_line(k):
        return lax.rem(z - k + lines, lines)

    def first(array, k):
        block = 2 * source_line(k) + x
        if k:
            came[array, "z", k].wait_recv()
        view = wholes[array].at[mine, block]
        origin = view if k else shards[array]
        came[array, "x", k] = links.send(origin, view, peers.by_x)
        came[array, "y", k] = links.send(origin, view, peers.by_y)
        came[array, "c", k, 0] = links.send(origin, view, peers.by_c)

    def second(array, k):
        side, line = 2 * source_line(k) + 1 - x, 2 * source_line(k) + x
        came[array, "x", k].wait_recv()
        view = wholes[array].at[mine, side]
        upper = view if array else view.at[pl.ds(0, half)]
        came[array, "xy", k] = links.send(upper, upper, peers.by_y)
        came[array, "c", k, 1] = links.send(view, view, peers.by_c)
        came[array, "y", k].wait_recv()
        view = wholes[array].at[other, line]
        if not array:
            lower = view.at[pl.ds(half, half)]
            came[array, "yx", k] = links.send(lower, lower, peers.by_x)
        came[array, "c", k, 2] = links.send(view, view, peers.by_c)

    def third(array, k):
        view = wholes[array].at[other, 2 * source_line(k) + 1 - x]
        came[array, "xy", k].wait_recv()
        if not array:
            came[array, "yx", k].wait_recv()
        came[array, "c", k, 3] = links.send(view, view, peers.by_c)

    def ffn(steps):
        if steps:
            for way in (1, -1):
                relayed(steps, way)
            return
        for array in range(2):
            view = ffn_wholes[array].at[own]
            came["ffn", array, "x"] = links.send(ffn_shards[array], view, peers.by_x)

    def complete(array):
        for k in order:
            for part in range(4):
                came[array, "c", k, part].wait_recv()
        moves.wait(local[array])

    for at in range(6):
        if at < 4:
            first(0, order[at])
        if 1 <= at <= 4:
            second(0, order[at - 1])
        if at >= 2:
            third(0, order[at - 2])
    ffn(0)
    complete(0)
    flat_qkv = [qkv_full[j].reshape(-1, qkv_full.shape[3]) for j in range(4)]
    project(
        tokens, attn_gain, flat_qkv, cosine, sine, attn_input, queries, pairs.at[pl.ds(0, rows)]
    )
    pair_y = links.send(pairs.at[pl.ds(0, rows)], pairs.at[pl.ds(rows, rows)], peers.by_y)
    pair_c = links.send(pairs.at[pl.ds(0, rows)], pairs.at[pl.ds(2 * rows, rows)], peers.by_c)
    moves.start(qkv_full, qkv_far)
    for k in order:
        first(1, k)
    ffn(1)
    pair_y.wait_recv()
    pair_yc = links.send(pairs.at[pl.ds(rows, rows)], pairs.at[pl.ds(3 * rows, rows)], peers.by_c)
    pair_c.wait_recv()
    pair_yc.wait_recv()
    moves.start(pairs, pairs_far)
    seen = (key_at[...] <= query_at[...]) | (key_at[...] < prefix[0])
    attend_group(0, seen, queries, pairs, exact, logs)
    for k in order:
        second(1, k)
    cot_y = links.send(cotangent, cot_rows.at[pl.ds(rows, rows)], peers.by_y)
    cot_c = links.send(cotangent, cot_rows.at[pl.ds(2 * rows, rows)], peers.by_c)
    attend_group(1, seen, queries, pairs, exact, logs)
    attend_group(2, seen, queries, pairs, exact, logs)
    ffn(2)
    for k in order:
        third(1, k)
    attend_group(3, seen, queries, pairs, exact, logs)
    attend_group(4, seen, queries, pairs, exact, logs)
    log_rows[...] = logs[...].T
    complete(1)
    moves.start(out_full, out_far)
    flat_out = [out_full[j].reshape(-1, out_full.shape[3]) for j in range(4)]
    close_attention(tokens, flat_out, mlp_gain, mixed, exact, resid, mlp_input)
    mlp_y = links.send(mlp_input, mlp_rows.at[pl.ds(rows, rows)], peers.by_y)
    mlp_c = links.send(mlp_input, mlp_rows.at[pl.ds(2 * rows, rows)], peers.by_c)
    moves.start(mlp_input, mlp_rows.at[pl.ds(0, rows)])
    cot_y.wait_recv()
    view = cot_rows.at[pl.ds(rows, rows)]
    cot_yc = links.send(view, cot_rows.at[pl.ds(3 * rows, rows)], peers.by_c)
    ffn(3)
    mlp_y.wait_recv()
    view = mlp_rows.at[pl.ds(rows, rows)]
    mlp_yc = links.send(view, mlp_rows.at[pl.ds(3 * rows, rows)], peers.by_c)
    for copy in (cot_c, cot_yc, mlp_c, mlp_yc):
        copy.wait_recv()
    for array in range(2):
        came["ffn", array, "x"].wait_recv()
        for steps in range(1, lines):
            for way in (1, -1):
                held, copy = came["ffn", array, way, steps, "x"]
                pl.when(held)(copy.wait_recv)
    links.finish()
    moves.finish()


def back_one_kernel(
    d_mlp_part, branch_part, down, down_taken, gate_up, resid_far, cotangent_far, weight_far, mixed_far, exact_far,
    queries_far, pairs_far, gain, logs, query_at, key_at, prefix,
    layer_out, d_resid, out_grad_far, gain_grad, d_queries, d_kv, down_sum, gate_sum, up_lines,
    d_mlp_own, branch_own, resid, cotangent, weight, mixed, exact, queries, pairs,
    rows_in, rows_out, rows_last, branch_in, branch_out, branch_last, pair_in, pair_out, pair_last,
    d_mixed, deltas, d_pairs, out_grad, own_blocks, x_in, z_out, z_in, local_sem, sent, got,
):
    peers = Peers()
    links, moves = Links(sent, got), Moves(local_sem)
    rows, quarter = resid.shape[0], down.shape[2]
    own_d_mlp = moves.start(d_mlp_part.at[pl.ds(0, 2 * rows)], d_mlp_own)
    own_branch = moves.start(branch_part.at[pl.ds(0, 2 * rows)], branch_own)
    ready = {}
    for name, source, target in (
        ("resid", resid_far, resid),
        ("cotangent", cotangent_far, cotangent),
        ("weight", weight_far, weight),
        ("mixed", mixed_far, mixed),
        ("exact", exact_far, exact),
        ("queries", queries_far, queries),
        ("pairs", pairs_far, pairs),
    ):
        ready[name] = moves.start(source, target)
    peers.greet()
    d_mlp_sum = RowSum(peers, links, d_mlp_part, rows_in, rows_out, rows_last)
    sums = [
        BlockSum(peers, links, moves, gradient, *(b.at[i] for b in (own_blocks, x_in, z_out, z_in)))
        for i, gradient in enumerate(
            (
                lambda block: down.at[block],
                lambda block: gate_up.at[block, :, pl.ds(0, quarter)],
                lambda block: gate_up.at[block, :, pl.ds(quarter, quarter)],
            )
        )
    ]
    sums[0].taken(down_taken)
    for block in sums[1:]:
        for k in STEPS:
            block.open(k)
    branch_sum = RowSum(peers, links, branch_part, branch_in, branch_out, branch_last)
    pending = [(i, k) for i in (1, 2) for k in STEPS]

    def pump(count):
        for _ in range(count):
            if pending:
                i, k = pending.pop(0)
                if i == 1:
                    sums[i].step(k)
                    continue
                at = STEPS.index(k)
                z_out[2, at] = sums[i].sum_x(k).astype(bf16)
                moves.start(z_out.at[2, at], up_lines.at[at])

    moves.wait(own_d_mlp, own_branch)
    d_mlp_sum.cross(d_mlp_own.at[pl.ds(rows, rows)])
    branch_sum.cross(branch_own.at[pl.ds(rows, rows)])
    for k in STEPS:
        sums[0].step(k)
    pump(2)
    moves.wait(*(ready[n] for n in ("resid", "cotangent", "weight", "mixed", "exact")))
    d_mlp = d_mlp_sum.total(d_mlp_own.at[pl.ds(0, rows)])
    branch_back(
        d_mlp, resid, cotangent, gain, weight, mixed, exact, d_resid, d_mixed, out_grad, gain_grad, deltas
    )
    flush = moves.start(out_grad, out_grad_far)
    pump(2)
    moves.wait(ready["queries"], ready["pairs"])
    seen = (key_at[...] <= query_at[...]) | (key_at[...] < prefix[0])
    for group in range(KEY_VALUE_HEADS):
        attend_back_group(group, seen, queries, pairs, d_mixed, logs, deltas, d_queries, d_pairs)
        if group in (0, 2, 4):
            pump(1)
    pair_sum = RowSum(peers, links, d_pairs, pair_in, pair_out, pair_last)
    pair_sum.cross(d_pairs.at[pl.ds(rows, rows)])
    layer_out[...] = (
        resid[...] + branch_sum.total(branch_own.at[pl.ds(0, rows)]).astype(bf16).astype(f32)
    ).astype(bf16)
    pump(8)
    d_kv[...] = pair_sum.total(d_pairs.at[pl.ds(0, rows)])
    down_sum[...] = sums[0].total()
    gate_sum[...] = sums[1].total()
    links.finish()
    moves.finish()


def back_two_kernel(
    up_lines, out_grad, weight_far, d_queries, d_kv, attn_input, tokens, d_resid, gain, cosine, sine, gain_mlp,
    tokens_grad, gains_sum, up_sum, out_sum, qkv_sum,
    weight, out_own, qkv_grad, up_own, z_in,
    gain_own, gain_c, gain_one, gain_y, gain_two, gain_x, gain_z, local_sem, sent, got, *buffers,
):
    peers = Peers()
    links, moves = Links(sent, got), Moves(local_sem)
    own_out = [moves.start(out_grad.at[2 * side + peers.c], out_own.at[side]) for side in range(2)]
    own_up = moves.start(up_lines.at[STEPS.index(0)], up_own)
    weight_in = moves.start(weight_far, weight)
    out_total = OwnerSum(peers, links, buffers[:11], lambda s, line, side: out_own[s, line, side])
    qkv_total = OwnerSum(
        peers, links, buffers[11:], lambda s, line, side: qkv_grad[2 * s + peers.c, line, side]
    )
    peers.greet()
    for side in range(2):
        out_total.hand(out_grad.at[2 * side + 1 - peers.c], side)
    up_copies = [
        links.send(up_lines.at[at], z_in.at[at], peers.by_z[k]) for at, k in enumerate(STEPS[:-1])
    ]
    d_projected = unproject(d_queries, d_kv, cosine, sine)
    moves.wait(*own_out)
    width = weight.shape[2]
    for j in range(4):
        part = d_projected[:, j * width : (j + 1) * width]
        outer = dot(attn_input[...], part, 0, 0).astype(bf16)
        qkv_grad[j] = outer.reshape(qkv_grad.shape[1:])
        if j % 2:
            qkv_total.hand(qkv_grad.at[j - peers.c], j // 2)
        else:
            out_total.chip(j // 2)
        if j == 2:
            for k in STEPS:
                out_total.open(k)
    qkv_total.chip(0)
    for k in (1, 3):
        out_total.pass_on(k)
    qkv_total.chip(1)
    for k in (2, 0):
        out_total.pass_on(k)
    for k in STEPS:
        qkv_total.open(k)
    moves.wait(weight_in)
    back = None
    for j in range(4):
        part = d_projected[:, j * width : (j + 1) * width]
        term = dot(part, weight[j], 1, 1)
        back = term if back is None else back + term
    gain_sum, d_normed = back_norm(back, tokens[...].astype(f32), gain[...])
    gain_own[...] = jnp.concatenate([gain_sum, gain_mlp[...]], axis=0)
    gain_copy = links.send(gain_own, gain_c, peers.by_c)
    for k in STEPS:
        out_total.close(k)
    gain_copy.wait_recv()
    gain_one[...] = gain_own[...] + gain_c[...]
    gain_copy = links.send(gain_one, gain_y, peers.by_y)
    tokens_grad[...] = d_resid[...] + d_normed
    for k in STEPS:
        qkv_total.pass_on(k)
    gain_copy.wait_recv()
    gain_two[...] = gain_one[...] + gain_y[...]
    gain_copy = links.send(gain_two, gain_x, peers.by_x)
    for k in (1, 3):
        qkv_total.close(k)
    gain_copy.wait_recv()
    gain_z[peers.z] = gain_two[...] + gain_x[...]
    gain_copies = [
        links.send(gain_z.at[peers.z], gain_z.at[peers.z], peers.by_z[k]) for k in range(1, lines)
    ]
    for k in (2, 0):
        qkv_total.close(k)
    moves.wait(own_up)
    up_total = up_own[...].astype(f32)
    for at, copy in enumerate(up_copies):
        copy.wait_recv()
        up_total = up_total + z_in[at].astype(f32)
    up_sum[...] = up_total
    out_sum[...] = out_total.total()
    for copy in gain_copies:
        copy.wait_recv()
    gains_sum[...] = ((gain_z[0] + gain_z[1]) + gain_z[2]) + gain_z[3]
    qkv_sum[...] = qkv_total.total()
    links.finish()
    moves.finish()


def remote_call(kernel, name, number, outs, scratch, *args, local=16, remote=64, smem=0, flops=0):
    places = {False: spec(), True: spec(pl.ANY)}
    return pl.pallas_call(
        kernel,
        out_shape=[jax.ShapeDtypeStruct(s, k) for s, k, _ in outs],
        in_specs=[places[far] for _, far in args[: len(args) - smem]] + [spec(pltpu.SMEM)] * smem,
        out_specs=[places[far] for _, _, far in outs],
        scratch_shapes=scratch[0]
        + [
            pltpu.SemaphoreType.DMA((local,)),
            pltpu.SemaphoreType.DMA((remote,)),
            pltpu.SemaphoreType.DMA((remote,)),
        ]
        + scratch[1],
        compiler_params=pltpu.CompilerParams(
            collective_id=number, has_side_effects=True, vmem_limit_bytes=62 * 2**20
        ),
        cost_estimate=pl.CostEstimate(flops=flops, bytes_accessed=2**24, transcendentals=0),
        name=name,
    )(*(array for array, _ in args))


def vmem_like(array):
    return pltpu.VMEM(array.shape, array.dtype)


def adam_update(master, moment, square, gradient, step_rate, decay):
    moment_next = beta_one * moment + (1.0 - beta_one) * gradient
    square_next = beta_two * square + (1.0 - beta_two) * gradient * gradient
    master_next = master - step_rate * (
        moment_next / (jnp.sqrt(square_next) + eps_adam) + decay * master
    )
    return (master_next, moment_next, square_next)


def on_device(
    tokens,
    cotangent,
    prefix_len,
    gains_master,
    gains_moment,
    gains_square,
    qkv_master,
    qkv_moment,
    qkv_square,
    out_master,
    out_moment,
    out_square,
    gu_master,
    gu_moment,
    gu_square,
    down_master,
    down_moment,
    down_square,
):
    seq_count = lax.axis_size("seq")
    dp_count = lax.axis_size("dp")
    seq_place = lax.axis_index("seq")
    near = dp_count == 2 * lines and seq_count == 4
    grid = Grid() if near else None
    plain = Plain()
    token_rows = tokens.shape[0]
    quarter = FF // seq_count
    shard_rows = gu_master.shape[0]
    qkv_b = qkv_master.astype(bf16)
    out_b = out_master.astype(bf16)
    gu_b = gu_master.astype(bf16).reshape(shard_rows, 2 * quarter)
    down_b = down_master.astype(bf16).T
    if near:
        key_places = [seq_place ^ step for step in (0, 2, 1, 3)]
    else:
        key_places = list(range(seq_count))
    within = jnp.arange(token_rows, dtype=jnp.int32)
    positions = seq_place * token_rows + within
    key_positions = jnp.concatenate([spot * token_rows + within for spot in key_places])

    cosine_half, sine_half = rope_tables(positions, HEAD_SIZE)
    cosine = jnp.concatenate([cosine_half] * 4, axis=1)
    sine = jnp.concatenate([-sine_half, sine_half] * 2, axis=1)
    shape = (token_rows, D)
    attn_gain, mlp_gain = gains_master[0:1], gains_master[1:2]
    key_count = seq_count * token_rows
    score_flops = 2 * token_rows * key_count * QUERY_WIDTH
    out_flops = 2 * token_rows * D * D
    pair = (token_rows, 2 * PAIR_WIDTH)
    all_pairs = (key_count, 2 * PAIR_WIDTH)
    if near:
        wide = (seq_count, 2 * lines)
        outs = [
            (wide + qkv_b.shape, bf16, True),
            (wide + out_b.shape, bf16, True),
            (wide[1:] + gu_b.shape, bf16, True),
            (wide[1:] + down_b.shape, bf16, True),
            (shape, bf16, False),
            (shape, bf16, False),
            (all_pairs, bf16, True),
            (shape, bf16, False),
            (shape, f32, False),
            ((128, token_rows), f32, False),
            (shape, f32, False),
            ((key_count, D), bf16, True),
            ((key_count, D), bf16, True),
        ]
        front = remote_call(
            front_kernel,
            "front",
            0,
            outs,
            (
                [pltpu.VMEM(s, k) for s, k, _ in outs[:2]]
                + [pltpu.VMEM(all_pairs, bf16), pltpu.VMEM(shape, bf16)]
                + [pltpu.VMEM((token_rows, 128), f32)],
                [],
            ),
            *((a, True) for a in (qkv_b, out_b, gu_b, down_b, cotangent)),
            *((a, False) for a in (tokens, attn_gain, mlp_gain, cosine, sine)),
            *((a, False) for a in (positions[:, None], key_positions[None, :], prefix_len)),
            remote=112,
            smem=1,
            flops=2 * token_rows * D * QKV + 2 * score_flops + out_flops,
        )
        qkv_full, out_full, gu_part, down_part, attn_input, queries, kv_rows = front[:7]
        mixed, mixed_exact, log_rows, resid, mlp_rows, cot_rows = front[7:]
        qkv_full = qkv_full.reshape(seq_count, D, -1)
        out_full = out_full.reshape(seq_count, D, -1)
        gu_part, down_part = gu_part.reshape(D, -1), down_part.reshape(D, -1)
    else:
        qkv_full = plain.gather_attention(qkv_b)
        out_full = plain.gather_attention(out_b)
        gu_part = lax.all_gather(gu_b, "dp", axis=0, tiled=True)
        down_part = lax.all_gather(down_b, "dp", axis=0, tiled=True)
        cot_rows = lax.all_gather(cotangent, "seq", axis=0, tiled=True)
        attn_input, queries, kv_local = local_call(
            project_kernel,
            "project",
            [(shape, bf16), (shape, bf16), (pair, bf16)],
            *(tokens, attn_gain, qkv_full, cosine, sine),
            flops=2 * token_rows * D * QKV,
        )
        kv_rows = lax.all_gather(kv_local, "seq", axis=0, tiled=True)
        mixed, mixed_exact, logs, resid, mlp_input = local_call(
            attend_kernel,
            "attend",
            [(shape, bf16), (shape, f32), ((token_rows, 128), f32), (shape, f32), (shape, bf16)],
            *(queries, kv_rows, tokens, out_full, mlp_gain),
            *(positions[:, None], key_positions[None, :], prefix_len),
            flops=2 * score_flops + out_flops,
            smem=1,
        )
        mlp_rows = lax.all_gather(mlp_input, "seq", axis=0, tiled=True)
    gateup = jnp.dot(mlp_rows, gu_part, preferred_element_type=f32)
    gate = gateup[:, :quarter]
    up_part = gateup[:, quarter:]
    sigmoid_gate = jax.nn.sigmoid(gate)
    silu_gate = gate * sigmoid_gate
    hidden = (silu_gate * up_part).astype(bf16)
    d_hidden = jnp.dot(cot_rows, down_part, preferred_element_type=f32)
    d_gate_b = (d_hidden * up_part * sigmoid_gate * (1.0 + gate * (1.0 - sigmoid_gate))).astype(bf16)
    d_up_b = (d_hidden * silu_gate).astype(bf16)
    d_gateup = jnp.concatenate([d_gate_b, d_up_b], axis=1)

    def contract(left, right, left_axis, right_axis):
        return lax.dot_general(
            left, right, (((left_axis,), (right_axis,)), ((), ())), preferred_element_type=f32
        )

    down_local = contract(cot_rows, hidden, 0, 0).astype(bf16)
    pair_shape = (seq_count, D, out_full.shape[2])
    if near:
        blocks = (2 * lines, shard_rows, quarter)
        lined = (3, lines, shard_rows, quarter)
        down_local = down_local.reshape(blocks)
        down_theirs = pick(down_local.reshape(lines, 2, shard_rows, quarter), 1 - grid.x, 1)
        down_taken = grid.swap_x(down_theirs)
        d_mlp_part = contract(d_gateup, gu_part, 1, 1).astype(bf16)
        branch_part = contract(hidden, down_part, 1, 1).astype(bf16)
        gu_local = contract(mlp_rows, d_gateup, 0, 0).astype(bf16)
        gu_local = gu_local.reshape(blocks[:2] + (2 * quarter,))
        rows_of = [((2 * token_rows, D), bf16), (shape, bf16), (shape, bf16)]
        pairs_of = [((2 * token_rows, 2 * PAIR_WIDTH), bf16), (pair, bf16), (pair, bf16)]
        far = [resid, cotangent, out_full, mixed, mixed_exact, queries, kv_rows]
        layer_out, d_resid, out_local, gain_mlp, d_queries, d_kv, down_owned, gate_owned, up_lines = remote_call(
            back_one_kernel,
            "back_one",
            1,
            [
                (shape, bf16, False),
                (shape, f32, False),
                (pair_shape, bf16, True),
                ((1, D), f32, False),
                (shape, f32, False),
                (pair, f32, False),
                ((shard_rows, quarter), f32, False),
                ((shard_rows, quarter), f32, False),
                (lined[1:], bf16, True),
            ],
            (
                [pltpu.VMEM((2 * token_rows, D), bf16)] * 2
                + [vmem_like(a) for a in far]
                + [pltpu.VMEM(*s) for s in rows_of + rows_of + pairs_of]
                + [
                    pltpu.VMEM(shape, bf16),
                    pltpu.VMEM((32, token_rows), f32),
                    pltpu.VMEM(kv_rows.shape, bf16),
                    pltpu.VMEM(pair_shape, bf16),
                ]
                + [pltpu.VMEM(lined, bf16)] * 4,
                [],
            ),
            *((a, True) for a in (d_mlp_part, branch_part)),
            *((a, True) for a in (down_local, down_taken, gu_local, *far)),
            *((a, False) for a in (mlp_gain, log_rows, positions[None, :], key_positions[:, None])),
            (prefix_len, False),
            local=40,
            smem=1,
            flops=5 * score_flops + 2 * out_flops,
        )
        line_shape = (seq_count, lines, 2, shard_rows)
        qkv_width, out_width = qkv_full.shape[2], out_full.shape[2]
        tokens_grad, gains_grad, up_owned, out_owned, qkv_owned = remote_call(
            back_two_kernel,
            "back_two",
            2,
            [
                (shape, f32, False),
                ((2, D), f32, False),
                ((shard_rows, quarter), f32, False),
                ((shard_rows, out_width), f32, False),
                ((shard_rows, qkv_width), f32, False),
            ],
            (
                [
                    vmem_like(qkv_full),
                    pltpu.VMEM((2,) + line_shape[1:] + (out_width,), bf16),
                    pltpu.VMEM(line_shape + (qkv_width,), bf16),
                ]
                + [pltpu.VMEM(blocks[1:], bf16), pltpu.VMEM((3,) + blocks[1:], bf16)]
                + [pltpu.VMEM((2, D), f32)] * 6
                + [pltpu.VMEM((lines, 2, D), f32)],
                owner_buffers(shard_rows, out_width) + owner_buffers(shard_rows, qkv_width),
            ),
            *((a, True) for a in (up_lines, out_local.reshape(line_shape + (-1,)), qkv_full)),
            *((a, False) for a in (d_queries, d_kv, attn_input, tokens, d_resid, attn_gain)),
            *((a, False) for a in (cosine, sine, gain_mlp)),
            flops=4 * token_rows * D * QKV,
        )
        gu_owned = with_layout_constraint(
            jnp.stack([gate_owned, up_owned], axis=1), Layout(major_to_minor=(0, 1, 2))
        )
    else:
        d_mlp_part = contract(d_gateup, gu_part, 1, 1).astype(bf16)
        branch_part = contract(hidden, down_part, 1, 1).astype(bf16)
        gu_local = contract(mlp_rows, d_gateup, 0, 0).astype(bf16)

        def scatter(values, axis):
            return lax.psum_scatter(values, axis, scatter_dimension=0, tiled=True).astype(f32)

        d_mlp_input = scatter(d_mlp_part, "seq")
        layer_out = (resid + scatter(branch_part, "seq")).astype(bf16)
        down_owned = scatter(down_local, "dp")
        gu_owned = scatter(gu_local, "dp").reshape(shard_rows, 2, quarter)
        d_resid, d_mixed, out_local, gain_mlp, deltas = local_call(
            branch_back_kernel,
            "branch_back",
            [(shape, f32), (shape, bf16), (pair_shape, bf16), ((1, D), f32), ((32, token_rows), f32)],
            *(d_mlp_input, resid, cotangent, mlp_gain, out_full, mixed, mixed_exact),
            flops=2 * out_flops,
        )
        out_owned = plain.reduce_attention(out_local)
        d_queries, d_pairs = local_call(
            attend_back_kernel,
            "attend_back",
            [(shape, f32), (kv_rows.shape, bf16)],
            *(queries, kv_rows, d_mixed, logs.T, deltas),
            *(positions[None, :], key_positions[:, None], prefix_len),
            flops=5 * score_flops,
            smem=1,
        )
        d_kv = scatter(d_pairs, "seq")
        tokens_grad, qkv_local, gain_attn = local_call(
            project_back_kernel,
            "project_back",
            [(shape, f32), (qkv_full.shape, bf16), ((1, D), f32)],
            *(d_queries, d_kv, attn_input, tokens, d_resid, attn_gain, qkv_full, cosine, sine),
            flops=4 * token_rows * D * QKV,
        )
        qkv_owned = plain.reduce_attention(qkv_local)
        gains_grad = lax.psum(jnp.concatenate([gain_attn, gain_mlp], axis=0), ("dp", "seq"))
    down_owned = down_owned.T
    owned = (qkv_owned, out_owned, gu_owned, down_owned)
    rate_wide = 0.5 * D ** (-0.5)
    rate_out = 0.5 * max(QUERY_WIDTH // 256, 1) ** (-0.5)
    rate_down = 0.5 * FF ** (-0.5)
    gains_new = adam_update(gains_master, gains_moment, gains_square, gains_grad, gain_rate, 0.0)
    qkv_new = adam_update(qkv_master, qkv_moment, qkv_square, owned[0], rate_wide, weight_decay)
    out_new = adam_update(out_master, out_moment, out_square, owned[1], rate_out, weight_decay)
    gu_new = adam_update(gu_master, gu_moment, gu_square, owned[2], rate_wide, weight_decay)
    down_new = adam_update(down_master, down_moment, down_square, owned[3], rate_down, weight_decay)
    return (
        layer_out,
        tokens_grad,
        gains_grad,
        owned[0],
        owned[1],
        owned[2],
        owned[3],
        gains_new[0],
        gains_new[1],
        gains_new[2],
        qkv_new[0],
        qkv_new[1],
        qkv_new[2],
        qkv_new[0].astype(jnp.bfloat16),
        out_new[0],
        out_new[1],
        out_new[2],
        out_new[0].astype(jnp.bfloat16),
        gu_new[0],
        gu_new[1],
        gu_new[2],
        gu_new[0].astype(jnp.bfloat16),
        down_new[0],
        down_new[1],
        down_new[2],
        down_new[0].astype(jnp.bfloat16),
    )


def solution(mesh):
    in_specs = (
        P(("dp", "seq"), None),
        P(("dp", "seq"), None),
        P("dp"),
        P(),
        P(),
        P(),
        P("dp", "seq"),
        P("dp", "seq"),
        P("dp", "seq"),
        P("dp", "seq"),
        P("dp", "seq"),
        P("dp", "seq"),
        P("dp", None, "seq"),
        P("dp", None, "seq"),
        P("dp", None, "seq"),
        P("seq", "dp"),
        P("seq", "dp"),
        P("seq", "dp"),
    )
    out_specs = (
        P(("dp", "seq"), None),
        P(("dp", "seq"), None),
        P(),
        P("dp", "seq"),
        P("dp", "seq"),
        P("dp", None, "seq"),
        P("seq", "dp"),
        P(),
        P(),
        P(),
        P("dp", "seq"),
        P("dp", "seq"),
        P("dp", "seq"),
        P("dp", "seq"),
        P("dp", "seq"),
        P("dp", "seq"),
        P("dp", "seq"),
        P("dp", "seq"),
        P("dp", None, "seq"),
        P("dp", None, "seq"),
        P("dp", None, "seq"),
        P("dp", None, "seq"),
        P("seq", "dp"),
        P("seq", "dp"),
        P("seq", "dp"),
        P("seq", "dp"),
    )
    return jax.shard_map(
        on_device, mesh=mesh, in_specs=in_specs, out_specs=out_specs, check_vma=False
    )
```
